256 devices in a mesh: gx: 4 (over y), gy: 16 (over z, x_lo), gz: 4 (over x_hi, core).
Axes of the slice: x: 4 (x_hi: 2, x_lo: 2; x = x_hi * 2 + x_lo), y: 4, z: 8, core: 2. Of those that a mesh axis runs over, the one named last changes fastest.
Arguments:
- features: bfloat16 [4, 16, 4, 128, 512], P('gx', 'gy', 'gz'), may hold values from -6 to 6
- positions: int32 [4, 16, 4, 3, 128], P('gx', 'gy', 'gz'), may hold values from 0 to 16383, as said below
- species: int32 [4, 16, 4, 128], P('gx', 'gy', 'gz'), may hold values from 0 to 9
- counts: int32 [4, 16, 4], P('gx', 'gy', 'gz'), may hold values from 64 to 128, as said below
- neighbors: int32 [4, 16, 4, 12, 128], P('gx', 'gy', 'gz'), may hold values from 0 to 3455, as said below
- waves: int32 [3, 2048], replicated, may hold values from -8 to 8, as said below
- radial_in: bfloat16 [8, 64], replicated, may hold values from -2 to 2
- radial_out: bfloat16 [64, 128], replicated, may hold values from -0.75 to 0.75
- species_gain: float32 [10, 128], replicated, may hold values from 0.5 to 1.5
- mix_weight: bfloat16 [128, 128], replicated, may hold values from -0.5 to 0.5
- readout: float32 [128], replicated, may hold values from -0.5 to 0.5
- charge_weight: float32 [128, 8], replicated, may hold values from -0.5 to 0.5
- ref_energy: float32 [10], replicated, may hold values from -4 to 4
Outputs:
- site_energy: float32 [4, 16, 4, 128], P('gx', 'gy', 'gz')
- forces: float32 [4, 16, 4, 3, 128], P('gx', 'gy', 'gz')
The draws below stay inside these ranges and needn't reach their ends.
Inputs may be any that keep to these rules, and one draw needn't show every extreme that they name: The first counts[a, b, c] slots of a cell hold atoms, the others are empty. `positions`: an atom of global cell n has coordinate n * 1024 plus 0 to 1023 along each dimension. `neighbors`: entry ((a * 3 + b) * 3 + c) * 128 + s names slot s of cell (a, b, c) of the device's block extended by one cell on every side, counted from the extended block's corner; it is an occupied slot of one of the 27 cells around the atom's own cell. `waves`: the first component is 1 to 8, the others -8 to 8.
All inputs are finite; a program needn't handle non-finite values.
Results may differ from the reference program's by a relative error of at most 0.004.
Values may be sent and summed in bfloat16 or wider, within the bound.
A program may use at most 64 MiB of HBM per device.

```python
import math
import jax
import jax.numpy as jnp
from jax import lax

CX = 1
CY = 1
CZ = 1
SLOTS = 128
NEIGH = 12
CH = 128
HID = 64
BASIS = 8
WAVES = 2048
CHARGES = 8
SPECIES = 10
TICKS = 1024
MAXM = 8
NX = 4
NY = 16
NZ = 4


def cell_counts(key):
    return jax.random.randint(jax.random.fold_in(key, 11), (NX, NY, NZ), SLOTS // 2, SLOTS + 1, dtype=jnp.int32)


def draw_counts(key, part):
    return cell_counts(key)


def draw_neighbors(key, part):
    counts = cell_counts(key)
    pick, choose = jax.random.split(jax.random.fold_in(key, 23))
    shape = (NX, NY, NZ, NEIGH, SLOTS)
    offset = jax.random.randint(pick, shape + (3,), 0, 3, dtype=jnp.int32)
    xs = jnp.arange(NX, dtype=jnp.int32)[:, None, None, None, None]
    ys = jnp.arange(NY, dtype=jnp.int32)[None, :, None, None, None]
    zs = jnp.arange(NZ, dtype=jnp.int32)[None, None, :, None, None]
    target_x = (xs + offset[..., 0] - 1) % NX
    target_y = (ys + offset[..., 1] - 1) % NY
    target_z = (zs + offset[..., 2] - 1) % NZ
    target = counts[target_x, target_y, target_z]
    raw = jax.random.randint(choose, shape, 0, 1 << 20, dtype=jnp.int32)
    slot = raw % target
    ext_x = xs % CX + offset[..., 0]
    ext_y = ys % CY + offset[..., 1]
    ext_z = zs % CZ + offset[..., 2]
    return (((ext_x * (CY + 2) + ext_y) * (CZ + 2) + ext_z) * SLOTS + slot).astype(jnp.int32)


def draw_positions(key, part):
    xs = jnp.broadcast_to(jnp.arange(NX, dtype=jnp.int32)[:, None, None], (NX, NY, NZ))
    ys = jnp.broadcast_to(jnp.arange(NY, dtype=jnp.int32)[None, :, None], (NX, NY, NZ))
    zs = jnp.broadcast_to(jnp.arange(NZ, dtype=jnp.int32)[None, None, :], (NX, NY, NZ))
    anchor = jnp.stack([xs, ys, zs], axis=3)[..., None] * TICKS
    jitter = jax.random.randint(jax.random.fold_in(key, 31), (NX, NY, NZ, 3, SLOTS), 0, TICKS, dtype=jnp.int32)
    return (anchor + jitter).astype(jnp.int32)


def draw_waves(key, part):
    first_key, rest_key = jax.random.split(jax.random.fold_in(key, 41))
    first = jax.random.randint(first_key, (1, WAVES), 1, MAXM + 1, dtype=jnp.int32)
    rest = jax.random.randint(rest_key, (2, WAVES), -MAXM, MAXM + 1, dtype=jnp.int32)
    return jnp.concatenate([first, rest], axis=0)


def touch_ends(values, own_key, smallest, largest):
    index_at = [jax.random.randint(jax.random.fold_in(own_key, axis), (), 0, length) for axis, length in enumerate(values.shape)]
    main_axis = values.shape.index(max(values.shape))
    neighbour = index_at[:main_axis] + [(index_at[main_axis] + 1) % values.shape[main_axis]] + index_at[main_axis + 1:]
    return values.at[tuple(index_at)].set(smallest).at[tuple(neighbour)].set(largest)


def levels(key, dims, cuts, low, top_value):
    factor_of = 1.0
    for position, blocks in cuts:
        heights = jax.random.uniform(jax.random.fold_in(jax.random.fold_in(key, 6), position), (blocks,), jnp.float32, low / len(cuts), top_value / len(cuts))
        factor_of = factor_of * jnp.repeat(jnp.exp(heights), dims[position] // blocks).reshape((-1,) + (1,) * (len(dims) - 1 - position))
    return factor_of


def normal_values(rng, extent, deviation, most, cuts=(), kind=jnp.bfloat16):
    factor_of = levels(rng, extent, cuts, -0.22, 0.18) if cuts else 1.0
    drawn = jax.random.normal(rng, extent, jnp.float32) * deviation * factor_of
    return jnp.minimum(jnp.maximum(drawn, -most), most).astype(kind)


def setup_inputs(seed: int = 0) -> dict:
    key_of = jax.random.split(jax.random.key(seed), 14)
    return {
        "features": normal_values(key_of[0], (NX, NY, NZ, SLOTS, 4 * CH), 1.0, 6.0, ((0, 4), (1, 16), (2, 4))),
        "positions": draw_positions(jax.random.fold_in(key_of[13], 71), 0),
        "species": touch_ends(jax.random.randint(key_of[2], (NX, NY, NZ, SLOTS), 0, SPECIES), jax.random.fold_in(key_of[2], 1), 0, SPECIES - 1).astype(jnp.int32),
        "counts": draw_counts(jax.random.fold_in(key_of[13], 71), 0),
        "neighbors": draw_neighbors(jax.random.fold_in(key_of[13], 71), 0),
        "waves": draw_waves(jax.random.fold_in(key_of[13], 71), 0),
        "radial_in": normal_values(key_of[6], (BASIS, HID), BASIS ** -0.5, 2.0),
        "radial_out": normal_values(key_of[7], (HID, CH), HID ** -0.5, 0.75),
        "species_gain": jnp.clip(jax.random.uniform(key_of[8], (SPECIES, CH), jnp.float32, 0.5, 1.5), 0.5, 1.5),
        "mix_weight": normal_values(key_of[9], (CH, CH), CH ** -0.5, 0.5),
        "readout": normal_values(key_of[10], (CH,), CH ** -0.5, 0.5, (), jnp.float32),
        "charge_weight": normal_values(key_of[11], (CH, CHARGES), CH ** -0.5, 0.5, (), jnp.float32),
        "ref_energy": normal_values(key_of[12], (SPECIES,), 1.0, 4.0, (), jnp.float32),
    }


def wrap_delta(delta, lengths):
    half = lengths // 2
    return (delta + half) % lengths - half

def phase_angle(pos, waves, lengths):
    frac = jnp.zeros((pos.shape[0], waves.shape[1]), jnp.float32)
    for dim in range(3):
        prod = pos[:, dim:dim + 1] * waves[dim:dim + 1, :] % lengths[dim]
        frac = frac + prod.astype(jnp.float32) / lengths[dim].astype(jnp.float32)
    return 2.0 * math.pi * frac

def wave_terms(waves, cells_dim, norm):
    kvec = 2.0 * math.pi * waves.astype(jnp.float32) / cells_dim[:, None]
    ksq = lax.optimization_barrier(jnp.sum(kvec * kvec, axis=0))
    green = 8.0 * jnp.exp(-ksq / 64.0) / (8.0 + ksq) * norm
    return (kvec, green)

def pair_terms(disp, near, own, gain, radial_in, radial_out, mix_weight, readout, charge_weight):
    rows, neigh = (disp.shape[0], disp.shape[1])
    chans = mix_weight.shape[0]
    count = radial_in.shape[0]
    r2 = lax.optimization_barrier(jnp.sum(disp * disp, axis=-1))
    spread = jnp.sqrt(r2 + 0.25)
    unit = disp / spread[..., None]
    centers = 0.25 + 0.5 * jnp.arange(count, dtype=jnp.float32)
    basis = jnp.exp(-2.0 * (spread[..., None] - centers) ** 2) / (1.0 + r2)[..., None]
    basis = basis.astype(jnp.bfloat16).reshape(rows * neigh, count)
    hidden = jax.nn.silu(jnp.dot(basis, radial_in, preferred_element_type=jnp.float32)).astype(jnp.bfloat16)
    radial = jnp.dot(hidden, radial_out, preferred_element_type=jnp.float32).reshape(rows, neigh, chans) * gain
    parts = near.astype(jnp.float32).reshape(rows, neigh, 4, chans)
    scalar = parts[:, :, 0]
    vector = parts[:, :, 1:]
    along = lax.optimization_barrier(jnp.sum(unit[..., None] * vector, axis=2))
    first = lax.optimization_barrier(jnp.sum(radial * (scalar + along), axis=1))
    rest = lax.optimization_barrier(jnp.sum(radial[:, :, None, :] * (vector + unit[..., None] * scalar[:, :, None, :]), axis=1))
    message = jnp.concatenate([first[:, None, :], rest], axis=1) * neigh ** (-0.5)
    message = message.astype(jnp.bfloat16).reshape(rows * 4, chans)
    mixed = jnp.dot(message, mix_weight, preferred_element_type=jnp.float32).reshape(rows, 4, chans)
    updated = own.astype(jnp.float32).reshape(rows, 4, chans) + mixed
    leading = updated[:, 0]
    energy = jnp.dot(leading, readout, precision=lax.Precision.HIGHEST)
    charges = jnp.dot(leading, charge_weight, precision=lax.Precision.HIGHEST)
    return (energy, charges)

def reference(features, positions, species, counts, neighbors, waves, radial_in, radial_out, species_gain, mix_weight, readout, charge_weight, ref_energy):
    cells = NX * NY * NZ
    total = cells * SLOTS
    width = features.shape[-1]
    flat_feats = features.reshape(total, width)
    flat_pos = jnp.transpose(positions, (0, 1, 2, 4, 3)).reshape(total, 3)
    flat_spec = species.reshape(total)
    live = (jnp.arange(SLOTS, dtype=jnp.int32)[None, None, None, :] < counts[..., None]).astype(jnp.float32).reshape(cells, SLOTS)
    order = jnp.transpose(neighbors, (0, 1, 2, 4, 3))
    slot = order % SLOTS
    cell = order // SLOTS
    along_z = cell % (CZ + 2)
    along_y = cell // (CZ + 2) % (CY + 2)
    along_x = cell // ((CZ + 2) * (CY + 2))
    xs = jnp.arange(NX, dtype=jnp.int32)[:, None, None, None, None]
    ys = jnp.arange(NY, dtype=jnp.int32)[None, :, None, None, None]
    zs = jnp.arange(NZ, dtype=jnp.int32)[None, None, :, None, None]
    glob_x = (xs - xs % CX + along_x - 1) % NX
    glob_y = (ys - ys % CY + along_y - 1) % NY
    glob_z = (zs - zs % CZ + along_z - 1) % NZ
    glob = (((glob_x * NY + glob_y) * NZ + glob_z) * SLOTS + slot).astype(jnp.int32).reshape(cells, SLOTS, NEIGH)
    lengths = jnp.array([NX * TICKS, NY * TICKS, NZ * TICKS], dtype=jnp.int32)
    own_pos = flat_pos.reshape(cells, SLOTS, 3)
    own_feats = flat_feats.reshape(cells, SLOTS, width)
    gains = species_gain[flat_spec]
    cells_dim = jnp.array([NX, NY, NZ], dtype=jnp.float32)
    norm = (WAVES * NX * NY * NZ * SLOTS) ** (-0.5)
    kvec, green = wave_terms(waves, cells_dim, norm)

    def tile_data(index):
        idx = glob[index]
        delta = wrap_delta(flat_pos[idx] - own_pos[index][:, None, :], lengths)
        disp = delta.astype(jnp.float32) * (1.0 / TICKS)
        return (idx, disp, flat_feats[idx], gains[idx])

    def forward(index):
        idx, disp, near, gain = tile_data(index)
        return pair_terms(disp, near, own_feats[index], gain, radial_in, radial_out, mix_weight, readout, charge_weight)
    energies, charges = lax.map(forward, jnp.arange(cells))
    live_q = charges * live[..., None]

    def add_factor(carry, index):
        theta = phase_angle(own_pos[index], waves, lengths)
        part_re = carry[0] + jnp.dot(live_q[index].T, jnp.cos(theta), precision=lax.Precision.HIGHEST)
        part_im = carry[1] + jnp.dot(live_q[index].T, jnp.sin(theta), precision=lax.Precision.HIGHEST)
        return ((part_re, part_im), None)
    empty = jnp.zeros((CHARGES, WAVES), jnp.float32)
    (sum_re, sum_im), _ = lax.scan(add_factor, (empty, empty), jnp.arange(cells))
    pot_re = 2.0 * green * sum_re
    pot_im = 2.0 * green * sum_im

    def backward(grad, index):
        idx, disp, near, gain = tile_data(index)
        theta = phase_angle(own_pos[index], waves, lengths)
        cosv = jnp.cos(theta)
        sinv = jnp.sin(theta)
        potential = jnp.dot(cosv, pot_re.T, precision=lax.Precision.HIGHEST) + jnp.dot(sinv, pot_im.T, precision=lax.Precision.HIGHEST)
        lq = live_q[index]
        weights = -sinv * jnp.dot(lq, pot_re, precision=lax.Precision.HIGHEST) + cosv * jnp.dot(lq, pot_im, precision=lax.Precision.HIGHEST)
        wave_grad = jnp.dot(weights, kvec.T, precision=lax.Precision.HIGHEST)

        def local(values):
            return pair_terms(values, near, own_feats[index], gain, radial_in, radial_out, mix_weight, readout, charge_weight)
        outs, pull = jax.vjp(local, disp)
        pair_grad, = pull((live[index], potential * live[index][:, None]))
        own_idx = (index * SLOTS + jnp.arange(SLOTS, dtype=jnp.int32)).astype(jnp.int32)
        grad = grad.at[idx.reshape(-1)].add(pair_grad.reshape(-1, 3))
        grad = grad.at[own_idx].add(wave_grad - lax.optimization_barrier(jnp.sum(pair_grad, axis=1)))
        site = live[index] * (outs[0] + 0.5 * lax.optimization_barrier(jnp.sum(lq * potential, axis=1)))
        return (grad, site)
    grad, sites = lax.scan(backward, jnp.zeros((total, 3), jnp.float32), jnp.arange(cells))
    site_energy = sites.reshape(total) + live.reshape(total) * ref_energy[flat_spec]
    forces = -grad * live.reshape(total)[:, None]
    forces = jnp.transpose(forces.reshape(NX, NY, NZ, SLOTS, 3), (0, 1, 2, 4, 3))
    return (site_energy.reshape(NX, NY, NZ, SLOTS), forces)
```

```python
import functools
import math

import jax
import jax.numpy as jnp
from jax import lax
from jax.experimental import pallas as pl
from jax.experimental.pallas import tpu as pltpu
from jax.sharding import PartitionSpec as P

TICKS = 1024
AXES = ("gx", "gy", "gz")
MESH = pl.DeviceIdType.MESH
HIGH = lax.Precision.HIGHEST
OFFS = [(a - 1, b - 1, c - 1) for a in range(3) for b in range(3) for c in range(3)]
F32 = jnp.float32
BF16 = jnp.bfloat16
SLOT = 128
GROUP = 9
FAR = -1.0e6


def iota(shape, dim):
    return lax.broadcasted_iota(jnp.int32, shape, dim)


def dot(a, b, contract=((1,), (0,)), precision=None):
    return lax.dot_general(a, b, (contract, ((), ())), precision=precision, preferred_element_type=F32)


NT = ((1,), (1,))
TN = ((0,), (0,))


def split(x):
    hi = x.astype(BF16)
    return hi, (x - hi.astype(F32)).astype(BF16)


def at_offset(sizes, d):
    return tuple(lax.rem(lax.axis_index(n) + (s + o), s) if o else lax.axis_index(n) for n, s, o in zip(AXES, sizes, d))


def greet(sizes, offsets):
    barrier = pltpu.get_barrier_semaphore()
    for d in offsets:
        pl.semaphore_signal(barrier, inc=1, device_id=at_offset(sizes, d), device_id_type=MESH)
    return lambda: pl.semaphore_wait(barrier, len(offsets))


def send(src, dst, ssem, rsem, sizes, d):
    c = pltpu.make_async_remote_copy(
        src_ref=src, dst_ref=dst, send_sem=ssem, recv_sem=rsem, device_id=at_offset(sizes, d), device_id_type=MESH
    )
    c.start()
    return c


NEAR = [(i, d) for i, d in enumerate(OFFS) if d != (0, 0, 0)]


def spread_kernel(
    sizes, pack, feats, species, rin, rout, gain, mix, readout, cw, ref_energy,
    lists, gtab, mst, wz, wr, base9, refrow, ssem, rsem, csem,
):
    wait = greet(sizes, [d for _, d in NEAR])
    wait()
    copies = [send(pack, lists.at[26 - i], ssem.at[i], rsem.at[i], sizes, d) for i, d in NEAR]
    own = pltpu.make_async_copy(pack, lists.at[13], csem)
    own.start()
    neigh = 12
    lane = iota((8, SLOT), 1)
    sel8 = jnp.where(lax.rem(lane, 16) == iota((8, SLOT), 0), 1.0, 0.0)
    sel1 = jnp.where(lax.rem(iota((1, SLOT), 1), 16) == 8, 1.0, 0.0)
    rc = dot(cw[...], sel8, precision=HIGH) + dot(readout[...], sel1, TN, HIGH)
    m = dot(mix[...].astype(F32), rc, precision=HIGH) * (neigh ** -0.5)
    mhi, mlo = split(m)
    mst[0:128, :] = mhi
    mst[128:256, :] = mlo
    base9[...] = dot(rc, feats[...].astype(F32), ((0,), (1,)), HIGH)[0:16]
    kinds = gain.shape[0]
    onehot = jnp.where(iota((kinds, SLOT), 0) == species[...], 1.0, 0.0)
    ghi, glo = split(dot(onehot, gain[...], TN, HIGH))
    gtab[:, 0:128] = ghi
    gtab[:, 128:256] = glo
    refrow[...] = jnp.broadcast_to(dot(ref_energy[...], onehot, precision=HIGH), refrow.shape)
    r = rin[...]
    h = rin.shape[1]
    dup = jnp.where(lax.rem(iota((h, 128), 1), h) == iota((h, 128), 0), 1.0, 0.0).astype(BF16)
    upper = jnp.where(iota((h, 128), 1) - h == iota((h, 128), 0), 1.0, 0.0).astype(BF16)
    rows_a = jnp.where(iota((128, 8), 0) == iota((128, 8), 1), 1.0, 0.0).astype(BF16)
    rows_b = jnp.where(iota((128, 8), 0) - 8 == iota((128, 8), 1), 1.0, 0.0).astype(BF16)
    wz[:, 0:128] = dot(dot(rows_a, r).astype(BF16), dup).astype(BF16)
    wz[:, 128:256] = dot(dot(rows_b, r).astype(BF16), upper).astype(BF16)
    ro = rout[...]
    none = jnp.zeros_like(ro)
    wr[0:64, 0:128] = ro
    wr[64:128, 0:128] = none
    wr[0:64, 128:256] = none
    wr[64:128, 128:256] = ro
    for c in copies:
        c.wait()
    own.wait()


def rows_of(loc):
    hi = loc & ~31
    return hi.astype(F32).astype(BF16), (loc & 31).astype(F32).astype(BF16)


def edges(blk, rank, base, off, own, feats, gtab, mst, wz, wr):
    slot = iota((SLOT, 128), 0).astype(F32) + base
    code = ((blk & 127) + 1).astype(F32)
    acc = jnp.zeros((SLOT, 128), F32)
    for k in range(12):
        acc = jnp.where(rank[k : k + 1] == slot, code[k : k + 1], acc)
    accb = acc.astype(BF16)
    pick_i = jnp.where(acc > 0.0, 1.0, 0.0).astype(BF16)
    named = dot(accb, jnp.ones((128, 128), BF16))
    lane = iota((SLOT, 128), 1)
    pick_j = jnp.where(named == (lane + 1).astype(F32), 1.0, 0.0).astype(BF16)
    both = jnp.concatenate([pick_i, pick_j], axis=1)
    disp = []
    for d in range(3):
        ihi, ilo = rows_of(blk[12 + d : 13 + d] & (TICKS - 1))
        jhi, jlo = rows_of(own[d : d + 1] & (TICKS - 1))
        hi = jnp.concatenate([-ihi, jhi], axis=1)
        lo = jnp.concatenate([-ilo, jlo], axis=1)
        w = jnp.concatenate([jnp.broadcast_to(hi, (128, 256)), jnp.broadcast_to(lo, (128, 256))], axis=0)
        t = dot(both, w, NT)
        disp.append((t[:, 0:128] + t[:, 128:256]) * (1.0 / TICKS) - off[d])
    dx, dy, dz = disp
    r2 = dx * dx + dy * dy + dz * dz
    s2 = r2 + 0.25
    inv = lax.rsqrt(s2)
    rs = s2 * inv
    inv1 = 1.0 / (1.0 + r2)
    t = rs - (0.25 + 0.5 * lax.rem(lane, 8).astype(F32))
    b = jnp.exp(-2.0 * t * t) * inv1
    b = jnp.where(lane < 8, b, b * (-4.0 * t - 2.0 * rs * inv1)).astype(BF16)
    zz = dot(b, wz)
    z, zp = zz[:, 0:128], zz[:, 128:256]
    sig = 1.0 / (1.0 + jnp.exp(-z))
    silu = z * sig
    hid = jnp.where(lane < 64, silu, (sig + silu * (1.0 - sig)) * zp).astype(BF16)
    rr = dot(hid, wr)
    g = dot(pick_j, gtab)
    g = g[:, 0:128] + g[:, 128:256]
    rad = rr[:, 0:128] * g
    radp = rr[:, 128:256] * g
    h = dot(pick_j, feats)
    q, qp = [], []
    for d in range(4):
        hd = h[:, 128 * d : 128 * (d + 1)]
        x = (rad * hd).astype(BF16)
        q.append(dot(jnp.concatenate([x, x], axis=1), mst))
        x = (radp * hd).astype(BF16)
        qp.append(dot(jnp.concatenate([x, x], axis=1), mst))
    ux, uy, uz = dx * inv, dy * inv, dz * inv
    along = ux * q[1] + uy * q[2] + uz * q[3]
    w = qp[0] + ux * qp[1] + uy * qp[2] + uz * qp[3] - along * inv
    part = (lane >> 4) & 3
    ua = jnp.where(part == 0, ux, jnp.where(part == 1, uy, uz))
    qa = jnp.where(part == 0, q[1], jnp.where(part == 1, q[2], q[3]))
    out = jnp.where(part == 3, q[0] + along, ua * w + qa * inv)
    return pick_i, pick_j, out


def per_atom(pick_i, out):
    lane = iota((SLOT, 128), 1)
    hi = out.astype(BF16)
    mixed = jnp.where(lane < 64, hi.astype(F32), out - hi.astype(F32)).astype(BF16)
    s = dot(mixed, pick_i, TN)
    return s[0:64] + s[64:128]


def cell_offset(a):
    return ((a // 9 - 1).astype(F32), (lax.rem(a // 3, 3) - 1).astype(F32), (lax.rem(a, 3) - 1).astype(F32))


def edge_kernel(lists, pack, feats, gtab, mst, wz, wr, sums_t, sums_j, picks_i, picks_j, outs, ranks, most, mask):
    lane = iota((16, 128), 1)
    row = iota((16, 128), 0)
    for a in range(27):
        blk = lists[a]
        keep = ((blk >> 7) == 26 - a) & (lane < blk[15:16]) & (row < 12)
        mask[16 * a : 16 * a + 16] = jnp.where(keep, 1.0, 0.0)
    m = mask[...].astype(BF16)
    tri = jnp.where(iota((128, 128), 0) <= iota((128, 128), 1), 1.0, 0.0).astype(BF16)
    both = dot(m, jnp.concatenate([tri, jnp.ones((128, 128), BF16)], axis=1))
    lower = jnp.where(iota((16, 16), 0) > iota((16, 16), 1), 1.0, 0.0).astype(BF16)
    totals = jnp.concatenate([both[16 * a : 16 * a + 16, 128:256] for a in range(27)], axis=1).astype(BF16)
    start = dot(lower, totals)
    peak = start[12:16, 0:128]
    for a in range(27):
        s = start[:, 128 * a : 128 * a + 128]
        peak = jnp.maximum(peak, s[12:16])
        r = both[16 * a : 16 * a + 16, 0:128] + s - 1.0
        ranks[a] = jnp.where(mask[16 * a : 16 * a + 16] > 0.0, r, FAR)
    most[0:4] = peak
    most[4:8] = peak
    own = pack[12:15]

    def group(gi, carry):
        done = []
        for u in range(GROUP):
            a = gi * GROUP + u
            done.append((a, edges(lists[a], ranks[a], 0.0, cell_offset(a), own, feats[...], gtab[...], mst[...], wz[...], wr[...])))
        for a, (pick_i, pick_j, out) in done:
            picks_i[a] = pick_i
            picks_j[a] = pick_j
            outs[a] = out
            s = per_atom(pick_i, out)
            sums_j[a] = s[0:48]
            sums_t[a] = s[48:64]
        return carry

    lax.fori_loop(0, 27 // GROUP, group, 0)

    @pl.when(jnp.max(peak) > SLOT)
    def _():
        def cell(a, carry):
            rank = ranks[a]
            pieces = (jnp.max(rank).astype(jnp.int32) + SLOT) // SLOT

            def piece(c, carry):
                base = (c * SLOT).astype(F32)
                pick_i, _, out = edges(lists[a], ranks[a], base, cell_offset(a), own, feats[...], gtab[...], mst[...], wz[...], wr[...])
                s = per_atom(pick_i, out)
                sums_j[a] += s[0:48]
                sums_t[a] += s[48:64]
                return carry

            return lax.fori_loop(1, pieces, piece, carry)

        lax.fori_loop(0, 27, cell, 0)


def wave_kernel(
    sizes, norm, sums_t, sums_j, base9, pack, waves, refrow,
    pots, mine,
    got_t, got_j, cos_h, cos_l, sin_h, sin_l, wrow, part, got_rs, block, got_ar, got_ag, lhs, pot_s,
    st, rt, sj, rj, srs, rrs, sar, rar, sag, rag, sp, rp,
):
    nx, ny, nz = sizes
    plane = [(dx, 0, dz) for dx in range(nx) for dz in range(nz) if (dx, dz) != (0, 0)]
    line = [(0, dy, 0) for dy in range(1, ny)]
    near = [d for _, d in NEAR]
    whom = {tuple((o + s) % s for o, s in zip(d, sizes)) for d in near + plane + line}
    wait = greet(sizes, sorted(whom))
    waves_f = waves[...].astype(F32)
    kvec = [waves_f[d : d + 1] * (2.0 * math.pi / sizes[d]) for d in range(3)]
    ksq = kvec[0] * kvec[0] + kvec[1] * kvec[1] + kvec[2] * kvec[2]
    wrow[0:1] = 2.0 * (8.0 * jnp.exp(ksq * (-1.0 / 64.0)) / (8.0 + ksq) * norm)
    for d in range(3):
        wrow[1 + d : 2 + d] = kvec[d]
    wait()
    first = [send(sums_t.at[i], got_t.at[26 - i], st.at[i], rt.at[i], sizes, d) for i, d in NEAR]
    second = [send(sums_j.at[i], got_j.at[26 - i], sj.at[i], rj.at[i], sizes, d) for i, d in NEAR]
    pos = pack[12:15]
    fields = []
    for d in range(3):
        length = float(sizes[d] * TICKS)
        p = pos[d : d + 1]
        fields.append(((p >> 7).astype(F32), waves_f[d : d + 1] * (128.0 / length)))
        fields.append(((p & 127).astype(F32), waves_f[d : d + 1] * (1.0 / length)))
    zero_i = jnp.zeros((2, 128), F32)
    zero_k = jnp.zeros((2, waves_f.shape[1]), F32)
    pos8 = jnp.concatenate([f[0] for f in fields] + [zero_i], axis=0).astype(BF16)
    wrow[8:16] = jnp.concatenate([f[1] for f in fields] + [zero_k], axis=0)
    blocks = waves_f.shape[1] // 128

    def phase(bi, carry):
        at = pl.ds(pl.multiple_of(bi * 128, 128), 128)
        turn = dot(pos8, wrow[8:16, at].astype(BF16), TN)
        quarter = jnp.floor(turn * 4.0 + 0.5)
        x = (turn - quarter * 0.25) * (2.0 * math.pi)
        qi = quarter.astype(jnp.int32)
        xx = x * x
        s = x * (1.0 + xx * (-1.0 / 6 + xx * (1.0 / 120 + xx * (-1.0 / 5040 + xx * (1.0 / 362880)))))
        c = 1.0 + xx * (-0.5 + xx * (1.0 / 24 + xx * (-1.0 / 720 + xx * (1.0 / 40320))))
        odd = (qi & 1) == 1
        cv = jnp.where(odd, s, c)
        sv = jnp.where(odd, c, s)
        cv = jnp.where(((qi + 1) & 2) == 2, -cv, cv)
        sv = jnp.where((qi & 2) == 2, -sv, sv)
        hi, lo = split(cv)
        cos_h[:, at] = hi
        cos_l[:, at] = lo
        hi, lo = split(sv)
        sin_h[:, at] = hi
        sin_l[:, at] = lo
        return carry

    lax.fori_loop(0, blocks, phase, 0)
    live = jnp.where(iota((1, 128), 1) < pack[15:16], 1.0, 0.0)
    for c in first:
        c.wait()
    total = base9[...] + sums_t[13]
    for i, _ in NEAR:
        total = total + got_t[i]
    q = total[0:8] * live
    qhi, qlo = split(q)
    q16 = jnp.concatenate([qhi, qlo], axis=0)
    for at_row, high, low in ((0, cos_h, cos_l), (8, sin_h, sin_l)):
        s = dot(q16, high[...])
        s = s[0:8] + s[8:16] + dot(q16, low[...])[0:8]
        for bi in range(blocks):
            part[bi, at_row : at_row + 8] = s[:, 128 * bi : 128 * bi + 128]
    ix, iz = lax.axis_index("gx"), lax.axis_index("gz")
    me = ix * nz + iz
    rs = []
    for n, d in enumerate(plane):
        to = lax.rem(ix + d[0], nx) * nz + lax.rem(iz + d[2], nz)
        rs.append(send(part.at[to], got_rs.at[n], srs.at[n], rrs.at[n], sizes, d))
    acc = part[me]
    for n, c in enumerate(rs):
        c.wait()
        acc = acc + got_rs[n]
    block[0] = acc
    ar = [send(block.at[0], got_ar.at[n], sar.at[n], rar.at[n], sizes, d) for n, d in enumerate(line)]
    for n, c in enumerate(ar):
        c.wait()
        acc = acc + got_ar[n]
    got_ag[me] = acc
    ag = [send(got_ag.at[me], got_ag.at[me], sag.at[n], rag.at[n], sizes, d) for n, d in enumerate(plane)]
    for c in ag:
        c.wait()
    width = blocks * 128
    for bi in range(blocks):
        at = slice(128 * bi, 128 * bi + 128)
        weight = wrow[0:1, at]
        pre = got_ag[bi, 0:8] * weight
        pim = got_ag[bi, 8:16] * weight
        kx, ky, kz = wrow[1:2, at], wrow[2:3, at], wrow[3:4, at]
        lc = jnp.concatenate([pre, kx * pim, ky * pim, kz * pim], axis=0)
        ls = jnp.concatenate([pim, -kx * pre, -ky * pre, -kz * pre], axis=0)
        hi, lo = split(lc)
        lhs[0:32, at] = hi
        lhs[32:64, at] = lo
        hi, lo = split(ls)
        lhs[64:96, at] = hi
        lhs[96:128, at] = lo
    w = dot(lhs[0:64], cos_h[...], NT)
    v = dot(lhs[64:128], sin_h[...], NT)
    w = w[0:32] + w[32:64] + dot(lhs[0:32], cos_l[...], NT)
    w = w + v[0:32] + v[32:64] + dot(lhs[64:96], sin_l[...], NT)
    pot = w[0:8]
    flag = jnp.where(iota((8, 128), 0) == 0, live, 0.0)
    pot16 = jnp.concatenate([pot * live, flag], axis=0)
    pot_s[0] = pot16
    third = [send(pot_s.at[0], pots.at[26 - i], sp.at[i], rp.at[i], sizes, d) for i, d in NEAR]
    pots[13] = pot16
    for c in second:
        c.wait()
    js = sums_j[13]
    for i, _ in NEAR:
        js = js + got_j[i]
    rows = []
    for d in range(3):
        wave = jnp.sum(q * w[8 * d + 8 : 8 * d + 16], axis=0, keepdims=True)
        rows.append(wave - jnp.sum(pot16 * js[16 * d : 16 * d + 16], axis=0, keepdims=True))
    site = live * (total[8:9] + refrow[0:1] + 0.5 * jnp.sum(q * pot, axis=0, keepdims=True))
    mine[...] = jnp.concatenate(rows + [site, live, live, live, live], axis=0)
    for c in third:
        c.wait()


def pull_back(pick_i, pick_j, out, pot16):
    hi, lo = split(pot16)
    none = jnp.zeros((16, 128), BF16)
    rep = jnp.concatenate([hi, hi, hi, none, lo, lo, lo, none], axis=0)
    prod = out * dot(pick_i, rep, NT)
    hi, lo = split(prod)
    return dot(hi, pick_j, TN) + dot(lo, pick_j, TN)


def force_kernel(picks_i, picks_j, outs, pots, mine, most, lists, ranks, pack, feats, gtab, mst, wz, wr, site, forces, total):
    def group(gi, acc):
        for u in range(GROUP):
            a = gi * GROUP + u
            acc = acc + pull_back(picks_i[a], picks_j[a], outs[a], pots[a])
        return acc

    total[...] = lax.fori_loop(0, 27 // GROUP, group, jnp.zeros((128, 128), F32))

    @pl.when(jnp.max(most[...]) > SLOT)
    def _():
        own = pack[12:15]

        def cell(a, carry):
            pieces = (jnp.max(ranks[a]).astype(jnp.int32) + SLOT) // SLOT

            def piece(c, carry):
                base = (c * SLOT).astype(F32)
                pick_i, pick_j, out = edges(lists[a], ranks[a], base, cell_offset(a), own, feats[...], gtab[...], mst[...], wz[...], wr[...])
                total[...] += pull_back(pick_i, pick_j, out, pots[a])
                return carry

            return lax.fori_loop(1, pieces, piece, carry)

        lax.fori_loop(0, 27, cell, 0)

    t = total[0:64] + total[64:128]
    live = mine[4:5]
    for d in range(3):
        g = mine[d : d + 1] + jnp.sum(t[16 * d : 16 * d + 16], axis=0, keepdims=True)
        forces[d : d + 1] = -g * live
    site[...] = mine[3:4]


def vmem(n):
    return [pl.BlockSpec(memory_space=pltpu.VMEM)] * n


def shape(dims, kind):
    return jax.ShapeDtypeStruct(dims, kind)


def per_device(
    sizes, features, positions, species, counts, neighbors, waves, radial_in, radial_out,
    species_gain, mix_weight, readout, charge_weight, ref_energy,
):
    nx, ny, nz = sizes
    slots = positions.shape[-1]
    wave_count = waves.shape[1]
    norm = (wave_count * nx * ny * nz * slots) ** -0.5
    feats = features.reshape(slots, -1)
    count_row = jnp.broadcast_to(counts.reshape(1, 1), (1, slots))
    pack = jnp.concatenate([neighbors.reshape(12, slots), positions.reshape(3, slots), count_row], axis=0)
    dma = pltpu.SemaphoreType.DMA
    lists, gtab, mst, wz, wr, base9, refrow = pl.pallas_call(
        functools.partial(spread_kernel, sizes),
        out_shape=[
            shape((27, 16, 128), jnp.int32), shape((128, 256), BF16), shape((256, 128), BF16),
            shape((128, 256), BF16), shape((128, 256), BF16), shape((16, 128), F32), shape((8, 128), F32),
        ],
        in_specs=vmem(10),
        out_specs=vmem(7),
        scratch_shapes=[dma((27,)), dma((27,)), dma],
        compiler_params=pltpu.CompilerParams(collective_id=0, has_side_effects=True),
        name="spread",
    )(
        pack, feats[:, :128], species.reshape(1, slots), radial_in, radial_out, species_gain, mix_weight,
        readout.reshape(1, -1), charge_weight, ref_energy.reshape(1, -1),
    )
    sums_t, sums_j, picks_i, picks_j, outs, ranks, most = pl.pallas_call(
        edge_kernel,
        out_shape=[
            shape((27, 16, 128), F32), shape((27, 48, 128), F32), shape((27, SLOT, 128), BF16),
            shape((27, SLOT, 128), BF16), shape((27, SLOT, 128), F32), shape((27, 16, 128), F32), shape((8, 128), F32),
        ],
        in_specs=vmem(7),
        out_specs=vmem(7),
        scratch_shapes=[pltpu.VMEM((27 * 16, 128), F32)],
        name="edges",
    )(lists, pack, feats, gtab, mst, wz, wr)
    planes, lines = nx * nz, ny
    blocks = wave_count // 128
    buf = pltpu.VMEM
    pots, mine = pl.pallas_call(
        functools.partial(wave_kernel, sizes, norm),
        out_shape=[shape((27, 16, 128), F32), shape((8, 128), F32)],
        in_specs=vmem(6),
        out_specs=vmem(2),
        scratch_shapes=[
            buf((27, 16, 128), F32), buf((27, 48, 128), F32),
            buf((128, wave_count), BF16), buf((128, wave_count), BF16), buf((128, wave_count), BF16), buf((128, wave_count), BF16),
            buf((16, wave_count), F32), buf((blocks, 16, 128), F32), buf((planes - 1, 16, 128), F32), buf((1, 16, 128), F32),
            buf((lines - 1, 16, 128), F32), buf((planes, 16, 128), F32), buf((128, wave_count), BF16), buf((1, 16, 128), F32),
            dma((27,)), dma((27,)), dma((27,)), dma((27,)),
            dma((planes - 1,)), dma((planes - 1,)), dma((lines - 1,)), dma((lines - 1,)),
            dma((planes - 1,)), dma((planes - 1,)), dma((27,)), dma((27,)),
        ],
        compiler_params=pltpu.CompilerParams(collective_id=1, has_side_effects=True),
        name="waves",
    )(sums_t, sums_j, base9, pack, waves, refrow)
    site, forces = pl.pallas_call(
        force_kernel,
        out_shape=[shape((1, 128), F32), shape((3, 128), F32)],
        in_specs=vmem(14),
        out_specs=vmem(2),
        scratch_shapes=[pltpu.VMEM((128, 128), F32)],
        name="forces",
    )(picks_i, picks_j, outs, pots, mine, most, lists, ranks, pack, feats, gtab, mst, wz, wr)
    return site.reshape(1, 1, 1, slots), forces.reshape(1, 1, 1, 3, slots)


def solution(mesh):
    sizes = tuple(mesh.shape[n] for n in AXES)
    cell = P("gx", "gy", "gz")
    placed = (cell,) * 5 + (P(),) * 8
    return jax.shard_map(
        functools.partial(per_device, sizes),
        mesh=mesh,
        in_specs=placed,
        out_specs=(cell, cell),
        check_vma=False,
    )
```

```python
import functools
import math

import jax
import jax.numpy as jnp
from jax import lax
from jax.experimental import pallas as pl
from jax.experimental.pallas import tpu as pltpu
from jax.sharding import PartitionSpec as P

TICKS = 1024
AXES = ("gx", "gy", "gz")
MESH = pl.DeviceIdType.MESH
HIGH = lax.Precision.HIGHEST
OFFS = [(a - 1, b - 1, c - 1) for a in range(3) for b in range(3) for c in range(3)]
F32 = jnp.float32
BF16 = jnp.bfloat16
SLOT = 96
GROUP = 9
LOG2E = math.log2(math.e)
FAR = -1.0e6


def iota(shape, dim):
    return lax.broadcasted_iota(jnp.int32, shape, dim)


def dot(a, b, contract=((1,), (0,)), precision=None):
    return lax.dot_general(a, b, (contract, ((), ())), precision=precision, preferred_element_type=F32)


NT = ((1,), (1,))
TN = ((0,), (0,))


def split(x):
    hi = x.astype(BF16)
    return hi, (x - hi.astype(F32)).astype(BF16)


def at_offset(sizes, d):
    return tuple(lax.rem(lax.axis_index(n) + (s + o), s) if o else lax.axis_index(n) for n, s, o in zip(AXES, sizes, d))


def greet(sizes, offsets):
    barrier = pltpu.get_barrier_semaphore()
    for d in offsets:
        pl.semaphore_signal(barrier, inc=1, device_id=at_offset(sizes, d), device_id_type=MESH)
    return lambda: pl.semaphore_wait(barrier, len(offsets))


def send(src, dst, ssem, rsem, sizes, d):
    c = pltpu.make_async_remote_copy(
        src_ref=src, dst_ref=dst, send_sem=ssem, recv_sem=rsem, device_id=at_offset(sizes, d), device_id_type=MESH
    )
    c.start()
    return c


NEAR = [(i, d) for i, d in enumerate(OFFS) if d != (0, 0, 0)]


SIDE = 128


def rows_of(pos):
    loc = pos & (TICKS - 1)
    scale = 1.0 / TICKS
    return (loc & ~31).astype(F32) * scale, (loc & 31).astype(F32) * scale


def stack(parts):
    return parts[0] if len(parts) == 1 else jnp.concatenate(parts, axis=0)


def edges(blks, ranks, base, offs, own, feats, gtab, mst, wz, wr):
    slot = iota((SLOT, 128), 0).astype(F32) + base
    accs = []
    for blk, rank in zip(blks, ranks):
        code = ((blk & 127) + 1).astype(F32)
        acc = jnp.zeros((SLOT, 128), F32)
        for k in range(12):
            acc = jnp.where(rank[k : k + 1] == slot, code[k : k + 1], acc)
        accs.append(acc)
    picks_i = [jnp.where(acc > 0.0, 1.0, 0.0).astype(BF16) for acc in accs]
    named = dot(stack(accs).astype(BF16), jnp.ones((128, 128), BF16))
    lane = iota(named.shape, 1)
    pick_j = jnp.where(named == (lane + 1).astype(F32), 1.0, 0.0).astype(BF16)
    jhi, jlo = rows_of(own)
    pieces = []
    for n, (blk, off, pick_i) in enumerate(zip(blks, offs, picks_i)):
        ihi, ilo = rows_of(blk[12:15])
        shift = jnp.concatenate([jnp.full((1, 128), o, F32) for o in off], axis=0)
        fill = jnp.zeros((2, 128), F32)
        left = jnp.concatenate([-ihi - shift, -ilo, fill], axis=0)
        right = jnp.concatenate([jhi, jlo, fill], axis=0)
        w = jnp.concatenate([left, right], axis=1).astype(BF16)
        both = jnp.concatenate([pick_i, pick_j[SLOT * n : SLOT * (n + 1)]], axis=1)
        pieces.append(dot(both, w, NT).astype(BF16))
    to_lanes = iota((8, 384), 1) >> 7
    spread = jnp.where((to_lanes == iota((8, 384), 0)) | (to_lanes + 3 == iota((8, 384), 0)), 1.0, 0.0).astype(BF16)
    disp = dot(stack(pieces), spread)
    dx, dy, dz = disp[:, 0:128], disp[:, 128:256], disp[:, 256:384]
    r2 = dx * dx + dy * dy + dz * dz
    s2 = r2 + 0.25
    inv = lax.rsqrt(s2)
    rs = s2 * inv
    inv1 = 1.0 / (1.0 + r2)
    t = rs - (0.25 + 0.5 * lax.rem(iota((1, 128), 1), 8).astype(F32))
    b = jnp.exp2((t * (-2.0 * LOG2E)) * t) * inv1
    b = jnp.where(lane < 8, b, b * (-4.0 * t - 2.0 * rs * inv1)).astype(BF16)
    zz = dot(b, wz)
    z, zp = zz[:, 0:128], zz[:, 128:256]
    sig = 0.5 * jnp.tanh(0.5 * z) + 0.5
    silu = z * sig
    hid = jnp.where(lane < 64, silu, (sig + silu * (1.0 - sig)) * zp).astype(BF16)
    rr = dot(hid, wr)
    g = dot(pick_j, gtab)
    g = g[:, 0:128] + g[:, 128:256]
    rad = rr[:, 0:128] * g
    radp = rr[:, 128:256] * g
    h = dot(pick_j, feats)
    q = []
    for r in (rad, radp):
        for d in range(2):
            x = [(r * h[:, 128 * e : 128 * (e + 1)]).astype(BF16) for e in (2 * d, 2 * d + 1)]
            t = dot(jnp.concatenate(x, axis=1), mst)
            q += [t[:, 0:128], t[:, 128:256]]
    ux, uy, uz = dx * inv, dy * inv, dz * inv
    along = ux * q[1] + uy * q[2] + uz * q[3]
    w = q[4] + ux * q[5] + uy * q[6] + uz * q[7] - along * inv
    part = (lane >> 4) & 3
    ua = jnp.where(part == 0, ux, jnp.where(part == 1, uy, uz))
    qa = jnp.where(part == 0, q[1], jnp.where(part == 1, q[2], q[3]))
    out = jnp.where(part == 3, q[0] + along, ua * w + qa * inv)
    rows = [slice(SLOT * n, SLOT * (n + 1)) for n in range(len(blks))]
    return [(pick_i, pick_j[r], out[r]) for pick_i, r in zip(picks_i, rows)]


def per_atom(pick_i, out):
    lane = iota((SLOT, 128), 1)
    hi = out.astype(BF16)
    mixed = jnp.where(lane < 64, hi.astype(F32), out - hi.astype(F32)).astype(BF16)
    s = dot(mixed, pick_i, TN)
    return s[0:64] + s[64:128]


def cell_offset(a):
    if isinstance(a, int):
        return tuple(float(o) for o in OFFS[a])
    return ((a // 9 - 1).astype(F32), (lax.rem(a // 3, 3) - 1).astype(F32), (lax.rem(a, 3) - 1).astype(F32))


def tables(feats, species, rin, rout, gain, mix, readout, cw, ref_energy, gtab, mst, wz, wr, base9, refrow):
    neigh = 12
    lane = iota((8, SIDE), 1)
    sel8 = jnp.where(lax.rem(lane, 16) == iota((8, SIDE), 0), 1.0, 0.0)
    sel1 = jnp.where(lax.rem(iota((1, SIDE), 1), 16) == 8, 1.0, 0.0)
    rc = dot(cw[...], sel8, TN, HIGH) + dot(readout[...], sel1, TN, HIGH)
    mb = (dot(mix[...].astype(F32), rc, precision=HIGH) * (neigh ** -0.5)).astype(BF16)
    mst[0:128, 0:128] = mb
    mst[0:128, 128:256] = jnp.zeros_like(mb)
    mst[128:256, 0:128] = jnp.zeros_like(mb)
    mst[128:256, 128:256] = mb
    base9[...] = dot(rc, feats[:, 0:128].astype(F32), ((0,), (1,)), HIGH)[0:16]
    kinds = gain.shape[0]
    onehot = jnp.where(iota((kinds, SIDE), 0) == species[...], 1.0, 0.0)
    ghi, glo = split(dot(onehot, gain[...], TN, HIGH))
    gtab[:, 0:128] = ghi
    gtab[:, 128:256] = glo
    refrow[...] = jnp.broadcast_to(dot(ref_energy[...], onehot, precision=HIGH), refrow.shape)
    r = rin[...]
    h = rin.shape[1]
    dup = jnp.where(lax.rem(iota((h, 128), 1), h) == iota((h, 128), 0), 1.0, 0.0).astype(BF16)
    upper = jnp.where(iota((h, 128), 1) - h == iota((h, 128), 0), 1.0, 0.0).astype(BF16)
    rows_a = jnp.where(iota((128, 8), 0) == iota((128, 8), 1), 1.0, 0.0).astype(BF16)
    rows_b = jnp.where(iota((128, 8), 0) - 8 == iota((128, 8), 1), 1.0, 0.0).astype(BF16)
    wz[:, 0:128] = dot(dot(rows_a, r).astype(BF16), dup).astype(BF16)
    wz[:, 128:256] = dot(dot(rows_b, r).astype(BF16), upper).astype(BF16)
    ro = rout[...]
    none = jnp.zeros_like(ro)
    wr[0:64, 0:128] = ro
    wr[64:128, 0:128] = none
    wr[0:64, 128:256] = none
    wr[64:128, 128:256] = ro


def rank_edges(lists, ranks, mask):
    lane = iota((16, 128), 1)
    row = iota((16, 128), 0)
    for a in range(27):
        blk = lists[a]
        keep = ((blk >> 7) == 26 - a) & (lane < blk[15:16]) & (row < 12)
        mask[16 * a : 16 * a + 16] = jnp.where(keep, 1.0, 0.0)
    m = mask[...].astype(BF16)
    tri = jnp.where(iota((128, 128), 0) <= iota((128, 128), 1), 1.0, 0.0).astype(BF16)
    both = dot(m, jnp.concatenate([tri, jnp.ones((128, 128), BF16)], axis=1))
    lower = jnp.where(iota((16, 16), 0) > iota((16, 16), 1), 1.0, 0.0).astype(BF16)
    totals = jnp.concatenate([both[16 * a : 16 * a + 16, 128:256] for a in range(27)], axis=1).astype(BF16)
    start = dot(lower, totals)
    peak = start[12:13, 0:128]
    for a in range(27):
        s = start[:, 128 * a : 128 * a + 128]
        peak = jnp.maximum(peak, s[12:13])
        r = both[16 * a : 16 * a + 16, 0:128] + s - 1.0
        ranks[a] = jnp.where(mask[16 * a : 16 * a + 16] > 0.0, r, FAR)
    return peak


def wave_tables(sizes, norm, waves, pos, wrow):
    waves_f = waves[...].astype(F32)
    kvec = [waves_f[d : d + 1] * (2.0 * math.pi / sizes[d]) for d in range(3)]
    ksq = kvec[0] * kvec[0] + kvec[1] * kvec[1] + kvec[2] * kvec[2]
    wrow[0:1] = 2.0 * (8.0 * jnp.exp(ksq * (-1.0 / 64.0)) / (8.0 + ksq) * norm)
    fields = []
    for d in range(3):
        wrow[1 + d : 2 + d] = kvec[d]
        length = float(sizes[d] * TICKS)
        p = pos[d : d + 1]
        fields.append(((p >> 7).astype(F32), waves_f[d : d + 1] * (128.0 / length)))
        fields.append(((p & 127).astype(F32), waves_f[d : d + 1] * (1.0 / length)))
    zero_i = jnp.zeros((2, 128), F32)
    zero_k = jnp.zeros((2, waves_f.shape[1]), F32)
    wrow[8:16] = jnp.concatenate([f[1] for f in fields] + [zero_k], axis=0)
    return jnp.concatenate([f[0] for f in fields] + [zero_i], axis=0).astype(BF16)


def phases(pos8, wrow, cos_h, cos_l, sin_h, sin_l):
    def phase(bi, carry):
        at = pl.ds(pl.multiple_of(bi * 128, 128), 128)
        turn = dot(pos8, wrow[8:16, at].astype(BF16), TN)
        quarter = jnp.floor(turn * 4.0 + 0.5)
        x = (turn - quarter * 0.25) * (2.0 * math.pi)
        qi = quarter.astype(jnp.int32)
        xx = x * x
        s = x * (1.0 + xx * (-1.0 / 6 + xx * (1.0 / 120 + xx * (-1.0 / 5040 + xx * (1.0 / 362880)))))
        c = 1.0 + xx * (-0.5 + xx * (1.0 / 24 + xx * (-1.0 / 720 + xx * (1.0 / 40320))))
        odd = (qi & 1) == 1
        cv = jnp.where(odd, s, c)
        sv = jnp.where(odd, c, s)
        cv = jnp.where(((qi + 1) & 2) == 2, -cv, cv)
        sv = jnp.where((qi & 2) == 2, -sv, sv)
        hi, lo = split(cv)
        cos_h[:, at] = hi
        cos_l[:, at] = lo
        hi, lo = split(sv)
        sin_h[:, at] = hi
        sin_l[:, at] = lo
        return carry

    lax.fori_loop(0, wrow.shape[1] // 128, phase, 0)


def peers(sizes):
    nx, ny, nz = sizes
    plane = [(dx, 0, dz) for dx in range(nx) for dz in range(nz) if (dx, dz) != (0, 0)]
    line = [(0, dy, 0) for dy in range(1, ny)]
    near = [d for _, d in NEAR]
    whom = {tuple((o + s) % s for o, s in zip(d, sizes)) for d in near + plane + line}
    return plane, line, sorted(whom)


def reciprocal(sizes, poison, sums_t, sums_j, base9, pack, refrow, pots, wrow, trig, bufs, sems):
    nx, ny, nz = sizes
    plane, line, _ = peers(sizes)
    cos_h, cos_l, sin_h, sin_l = trig
    got_t, got_j, part, got_rs, block, got_ar, got_ag, lhs, pot_s = bufs
    st, rt, sj, rj, srs, rrs, sar, rar, sag, rag, sp, rp = sems
    blocks = wrow.shape[1] // 128
    first = [send(sums_t.at[i], got_t.at[26 - i], st.at[i], rt.at[i], sizes, d) for i, d in NEAR]
    live = jnp.where(iota((1, 128), 1) < pack[15:16], 1.0, 0.0)
    total = base9[...] + sums_t[13].astype(F32)
    for c in first:
        c.wait()
    for i, _ in NEAR:
        total = total + got_t[i].astype(F32)
    q = total[0:8] * live
    qhi, qlo = split(q)
    q16 = jnp.concatenate([qhi, qlo], axis=0)
    for at_row, high, low in ((0, cos_h, cos_l), (8, sin_h, sin_l)):
        s = dot(q16, high[...])
        s = s[0:8] + s[8:16] + dot(q16, low[...])[0:8]
        for bi in range(blocks):
            part[bi, at_row : at_row + 8] = s[:, 128 * bi : 128 * bi + 128] + poison
    ix, iz = lax.axis_index("gx"), lax.axis_index("gz")
    me = ix * nz + iz
    rs = []
    for n, d in enumerate(plane):
        to = lax.rem(ix + d[0], nx) * nz + lax.rem(iz + d[2], nz)
        rs.append(send(part.at[to], got_rs.at[n], srs.at[n], rrs.at[n], sizes, d))
    second = [send(sums_j.at[i], got_j.at[26 - i], sj.at[i], rj.at[i], sizes, d) for i, d in NEAR]
    acc = part[me]
    for n, c in enumerate(rs):
        c.wait()
        acc = acc + got_rs[n]
    block[0] = acc
    ar = [send(block.at[0], got_ar.at[n], sar.at[n], rar.at[n], sizes, d) for n, d in enumerate(line)]
    for n, c in enumerate(ar):
        c.wait()
        acc = acc + got_ar[n]
    got_ag[me] = acc
    ag = [send(got_ag.at[me], got_ag.at[me], sag.at[n], rag.at[n], sizes, d) for n, d in enumerate(plane)]
    js = sums_j[13].astype(F32)
    for c in second:
        c.wait()
    for i, _ in NEAR:
        js = js + got_j[i].astype(F32)
    for c in ag:
        c.wait()
    for bi in range(blocks):
        at = slice(128 * bi, 128 * bi + 128)
        weight = wrow[0:1, at]
        pre = got_ag[bi, 0:8] * weight
        pim = got_ag[bi, 8:16] * weight
        kx, ky, kz = wrow[1:2, at], wrow[2:3, at], wrow[3:4, at]
        lc = jnp.concatenate([pre, kx * pim, ky * pim, kz * pim], axis=0)
        ls = jnp.concatenate([pim, -kx * pre, -ky * pre, -kz * pre], axis=0)
        hi, lo = split(lc)
        lhs[0:32, at] = hi
        lhs[32:64, at] = lo
        hi, lo = split(ls)
        lhs[64:96, at] = hi
        lhs[96:128, at] = lo
    w = dot(lhs[0:64], cos_h[...], NT)
    v = dot(lhs[64:128], sin_h[...], NT)
    w = w[0:32] + w[32:64] + dot(lhs[0:32], cos_l[...], NT)
    w = w + v[0:32] + v[32:64] + dot(lhs[64:96], sin_l[...], NT)
    pot = w[0:8]
    flag = jnp.where(iota((8, 128), 0) == 0, live, 0.0)
    pot16 = jnp.concatenate([pot * live, flag], axis=0)
    pot_s[0] = pot16.astype(BF16)
    third = [send(pot_s.at[0], pots.at[26 - i], sp.at[i], rp.at[i], sizes, d) for i, d in NEAR]
    pots[13] = pot16.astype(BF16)
    rows = []
    for d in range(3):
        wave = jnp.sum(q * w[8 * d + 8 : 8 * d + 16], axis=0, keepdims=True)
        rows.append(wave - jnp.sum(pot16 * js[16 * d : 16 * d + 16], axis=0, keepdims=True))
    site = live * (total[8:9] + refrow[0:1] + 0.5 * jnp.sum(q * pot, axis=0, keepdims=True))
    mine = jnp.concatenate(rows + [site, live, live, live, live], axis=0)
    for c in third:
        c.wait()
    return mine


def pull_back(work, pots):
    prods = []
    for (pick_i, _, out), p in zip(work, pots):
        none = jnp.zeros((16, 128), BF16)
        prods.append(out * dot(pick_i, jnp.concatenate([p, p, p, none, p, p, p, none], axis=0), NT))
    prod = stack(prods)
    hi = prod.astype(BF16)
    mixed = jnp.where(iota(prod.shape, 1) < 64, hi.astype(F32), prod - hi.astype(F32)).astype(BF16)
    return dot(mixed, stack([pick_j for _, pick_j, _ in work]), TN)


def give(mine, t, site, forces):
    t = t[0:64] + t[64:128]
    for d in range(3):
        g = mine[d : d + 1] + jnp.sum(t[16 * d : 16 * d + 16], axis=0, keepdims=True)
        forces[d] = -g * mine[4:5]
    site[...] = mine[3:4]


def gather_pack(neighbors, positions, counts, pack, sem):
    copies = [pltpu.make_async_copy(neighbors.at[k], pack.at[pl.ds(k, 1)], sem.at[k]) for k in range(12)]
    copies += [pltpu.make_async_copy(positions.at[d], pack.at[pl.ds(12 + d, 1)], sem.at[12 + d]) for d in range(3)]
    for c in copies:
        c.start()
    pack[15:16] = jnp.full((1, 128), counts[0, 0], jnp.int32)
    return copies


def hand_out(sizes, pack, lists, ssem, rsem):
    copies = [send(pack, lists.at[26 - i], ssem.at[i], rsem.at[i], sizes, d) for i, d in NEAR]
    lists[13] = pack[...]
    return copies


def whole_kernel(
    sizes, norm, neighbors, positions, counts, feats, species, waves, rin, rout, gain, mix, readout, cw, ref_energy,
    site, forces,
    pack, lists, gtab, mst, wz, wr, base9, refrow, ranks, mask, picks_i, picks_j, outs, sums_t, sums_j, pots, wrow,
    cos_h, cos_l, sin_h, sin_l, got_t, got_j, part, got_rs, block, got_ar, got_ag, lhs, pot_s,
    psem, ls, lr, *sems,
):
    wait = greet(sizes, peers(sizes)[2])
    packed = gather_pack(neighbors, positions, counts, pack, psem)
    tables(feats, species, rin, rout, gain, mix, readout, cw, ref_energy, gtab, mst, wz, wr, base9, refrow)
    for c in packed:
        c.wait()
    wait()
    out = hand_out(sizes, pack, lists, ls, lr)
    own = pack[12:15]
    trig = (cos_h, cos_l, sin_h, sin_l)
    phases(wave_tables(sizes, norm, waves, own, wrow), wrow, *trig)
    for c in out:
        c.wait()
    peak = rank_edges(lists, ranks, mask)

    def group(gi, carry):
        cells = [gi * GROUP + u for u in range(GROUP)]
        done = edges(
            [lists[a] for a in cells], [ranks[a] for a in cells], 0.0, [cell_offset(a) for a in cells],
            own, feats[...], gtab[...], mst[...], wz[...], wr[...],
        )
        for a, (pick_i, pick_j, e) in zip(cells, done):
            picks_i[a] = pick_i
            picks_j[a] = pick_j
            outs[a] = e
            s = per_atom(pick_i, e).astype(BF16)
            sums_j[a] = s[0:48]
            sums_t[a] = s[48:64]
        return carry

    lax.fori_loop(0, 27 // GROUP, group, 0)
    poison = jnp.where(peak > float(SLOT), jnp.nan, 0.0)
    bufs = (got_t, got_j, part, got_rs, block, got_ar, got_ag, lhs, pot_s)
    mine = reciprocal(sizes, poison, sums_t, sums_j, base9, pack, refrow, pots, wrow, trig, bufs, sems)

    def back(gi, acc):
        cells = [gi * GROUP + u for u in range(GROUP)]
        return acc + pull_back([(picks_i[a], picks_j[a], outs[a]) for a in cells], [pots[a] for a in cells])

    give(mine, lax.fori_loop(0, 27 // GROUP, back, jnp.zeros((128, 128), F32)), site, forces)


def spread_kernel(
    sizes, neighbors, positions, counts, feats, species, rin, rout, gain, mix, readout, cw, ref_energy,
    lists, pack_out, gtab, mst, wz, wr, base9, refrow, pack, psem, ssem, rsem,
):
    wait = greet(sizes, [d for _, d in NEAR])
    packed = gather_pack(neighbors, positions, counts, pack, psem)
    tables(feats, species, rin, rout, gain, mix, readout, cw, ref_energy, gtab, mst, wz, wr, base9, refrow)
    for c in packed:
        c.wait()
    wait()
    out = hand_out(sizes, pack, lists, ssem, rsem)
    pack_out[...] = pack[...]
    for c in out:
        c.wait()


def each_piece(ranks, run):
    def cell(a, carry):
        pieces = (jnp.max(ranks[a]).astype(jnp.int32) + SLOT) // SLOT
        return lax.fori_loop(0, pieces, lambda c, carry: run(a, (c * SLOT).astype(F32), carry), carry)

    lax.fori_loop(0, 27, cell, 0)


def edge_kernel(lists, pack, feats, gtab, mst, wz, wr, sums_t, sums_j, mask, ranks, total_t, total_j):
    rank_edges(lists, ranks, mask)
    own = pack[12:15]
    total_t[...] = jnp.zeros_like(total_t)
    total_j[...] = jnp.zeros_like(total_j)

    def piece(a, base, carry):
        pick_i, _, out = edges([lists[a]], [ranks[a]], base, [cell_offset(a)], own, feats[...], gtab[...], mst[...], wz[...], wr[...])[0]
        s = per_atom(pick_i, out)
        total_j[a] += s[0:48]
        total_t[a] += s[48:64]
        return carry

    each_piece(ranks, piece)
    sums_t[...] = total_t[...].astype(BF16)
    sums_j[...] = total_j[...].astype(BF16)


def wave_kernel(
    sizes, norm, sums_t, sums_j, base9, pack, waves, refrow, pots, mine,
    wrow, cos_h, cos_l, sin_h, sin_l, got_t, got_j, part, got_rs, block, got_ar, got_ag, lhs, pot_s, *sems,
):
    wait = greet(sizes, peers(sizes)[2])
    trig = (cos_h, cos_l, sin_h, sin_l)
    phases(wave_tables(sizes, norm, waves, pack[12:15], wrow), wrow, *trig)
    wait()
    bufs = (got_t, got_j, part, got_rs, block, got_ar, got_ag, lhs, pot_s)
    mine[...] = reciprocal(sizes, 0.0, sums_t, sums_j, base9, pack, refrow, pots, wrow, trig, bufs, sems)


def force_kernel(pots, mine, lists, pack, feats, gtab, mst, wz, wr, site, forces, mask, ranks, total):
    rank_edges(lists, ranks, mask)
    own = pack[12:15]
    total[...] = jnp.zeros_like(total)

    def piece(a, base, carry):
        work = edges([lists[a]], [ranks[a]], base, [cell_offset(a)], own, feats[...], gtab[...], mst[...], wz[...], wr[...])
        total[...] += pull_back(work, [pots[a]])
        return carry

    each_piece(ranks, piece)
    give(mine[...], total[...], site, forces)


VMEM = pl.BlockSpec(memory_space=pltpu.VMEM)
SMEM = pl.BlockSpec(memory_space=pltpu.SMEM)
HBM = pl.BlockSpec(memory_space=pl.ANY)


def shape(dims, kind):
    return jax.ShapeDtypeStruct(dims, kind)


def wave_buffers(sizes, waves):
    nx, ny, nz = sizes
    planes, blocks = nx * nz, waves // 128
    buf = pltpu.VMEM
    dma = pltpu.SemaphoreType.DMA
    trig = [buf((128, waves), BF16)] * 4
    rest = [
        buf((27, 16, 128), BF16), buf((27, 48, 128), BF16), buf((blocks, 16, 128), F32), buf((planes - 1, 16, 128), F32),
        buf((1, 16, 128), F32), buf((ny - 1, 16, 128), F32), buf((planes, 16, 128), F32), buf((128, waves), BF16),
        buf((1, 16, 128), BF16),
    ]
    counts = (27, 27, 27, 27, planes - 1, planes - 1, ny - 1, ny - 1, planes - 1, planes - 1, 27, 27)
    return [buf((16, waves), F32)] + trig + rest, [dma((n,)) for n in counts]


TABLES = [
    ((128, 256), BF16), ((256, 256), BF16), ((128, 256), BF16), ((128, 256), BF16), ((16, 128), F32), ((8, 128), F32),
]
RANKS = [((27, 16, 128), F32), ((27 * 16, 128), F32)]
RESULT = [((1, 128), F32), ((3, 1, 128), F32)]


def general(sizes, norm, neighbors, positions, counts, feats, species, waves, *params):
    dma = pltpu.SemaphoreType.DMA
    lists, pack, gtab, mst, wz, wr, base9, refrow = pl.pallas_call(
        functools.partial(spread_kernel, sizes),
        out_shape=[shape((27, 16, 128), jnp.int32), shape((16, 128), jnp.int32)] + [shape(*t) for t in TABLES],
        in_specs=[HBM, HBM, SMEM] + [VMEM] * 9,
        out_specs=[VMEM] * 8,
        scratch_shapes=[pltpu.VMEM((16, 128), jnp.int32), dma((15,)), dma((27,)), dma((27,))],
        compiler_params=pltpu.CompilerParams(collective_id=1, has_side_effects=True),
        name="spread",
    )(neighbors, positions, counts, feats, species, *params)
    ranking = [pltpu.VMEM(*RANKS[1]), pltpu.VMEM(*RANKS[0])]
    sums_t, sums_j = pl.pallas_call(
        edge_kernel,
        out_shape=[shape((27, 16, 128), BF16), shape((27, 48, 128), BF16)],
        in_specs=[VMEM] * 7,
        out_specs=[VMEM] * 2,
        scratch_shapes=ranking + [pltpu.VMEM((27, 16, 128), F32), pltpu.VMEM((27, 48, 128), F32)],
        name="edges",
    )(lists, pack, feats, gtab, mst, wz, wr)
    bufs, sems = wave_buffers(sizes, waves.shape[1])
    pots, mine = pl.pallas_call(
        functools.partial(wave_kernel, sizes, norm),
        out_shape=[shape((27, 16, 128), BF16), shape((8, 128), F32)],
        in_specs=[VMEM] * 6,
        out_specs=[VMEM] * 2,
        scratch_shapes=bufs + sems,
        compiler_params=pltpu.CompilerParams(collective_id=2, has_side_effects=True),
        name="waves",
    )(sums_t, sums_j, base9, pack, waves, refrow)
    return pl.pallas_call(
        force_kernel,
        out_shape=[shape(*r) for r in RESULT],
        in_specs=[VMEM] * 9,
        out_specs=[VMEM] * 2,
        scratch_shapes=ranking + [pltpu.VMEM((128, 128), F32)],
        name="forces",
    )(pots, mine, lists, pack, feats, gtab, mst, wz, wr)


def direct(sizes, norm, neighbors, positions, counts, feats, species, waves, *params):
    dma = pltpu.SemaphoreType.DMA
    buf = pltpu.VMEM
    bufs, sems = wave_buffers(sizes, waves.shape[1])
    scratch = [buf((16, 128), jnp.int32), buf((27, 16, 128), jnp.int32)] + [buf(*t) for t in TABLES + RANKS]
    scratch += [buf((27, SLOT, 128), BF16), buf((27, SLOT, 128), BF16), buf((27, SLOT, 128), F32)]
    scratch += [buf((27, 16, 128), BF16), buf((27, 48, 128), BF16), buf((27, 16, 128), BF16)]
    return pl.pallas_call(
        functools.partial(whole_kernel, sizes, norm),
        out_shape=[shape(*r) for r in RESULT],
        in_specs=[HBM, HBM, SMEM] + [VMEM] * 10,
        out_specs=[VMEM] * 2,
        scratch_shapes=scratch + bufs + [dma((15,)), dma((27,)), dma((27,))] + sems,
        compiler_params=pltpu.CompilerParams(collective_id=0, has_side_effects=True),
        name="whole",
    )(neighbors, positions, counts, feats, species, waves, *params)


def per_device(
    sizes, features, positions, species, counts, neighbors, waves, radial_in, radial_out,
    species_gain, mix_weight, readout, charge_weight, ref_energy,
):
    nx, ny, nz = sizes
    slots = positions.shape[-1]
    norm = (waves.shape[1] * nx * ny * nz * slots) ** -0.5
    args = (
        neighbors.reshape(12, 1, slots), positions.reshape(3, 1, slots), counts.reshape(1, 1),
        features.reshape(slots, -1), species.reshape(1, slots), waves, radial_in, radial_out, species_gain,
        mix_weight, readout.reshape(1, -1), charge_weight.T, ref_energy.reshape(1, -1),
    )
    site, forces = direct(sizes, norm, *args)
    crowded = jnp.isnan(site[0, 0])
    site, forces = lax.cond(
        crowded, lambda s, f, *a: tuple(general(sizes, norm, *a)), lambda s, f, *a: (s, f), site, forces, *args
    )
    return site.reshape(1, 1, 1, slots), forces.reshape(1, 1, 1, 3, slots)


def solution(mesh):
    sizes = tuple(mesh.shape[n] for n in AXES)
    cell = P("gx", "gy", "gz")
    placed = (cell,) * 5 + (P(),) * 8
    return jax.shard_map(
        functools.partial(per_device, sizes),
        mesh=mesh,
        in_specs=placed,
        out_specs=(cell, cell),
        check_vma=False,
    )
```

```python
import functools
import math

import jax
import jax.numpy as jnp
from jax import lax
from jax.experimental import pallas as pl
from jax.experimental.pallas import tpu as pltpu
from jax.sharding import PartitionSpec as P

TICKS = 1024
AXES = ("gx", "gy", "gz")
MESH = pl.DeviceIdType.MESH
HIGH = lax.Precision.HIGHEST
OFFS = [(a - 1, b - 1, c - 1) for a in range(3) for b in range(3) for c in range(3)]
F32 = jnp.float32
BF16 = jnp.bfloat16
SLOT = 96
GROUP = 9
LOG2E = math.log2(math.e)
FAR = -1.0e6


def iota(shape, dim):
    return lax.broadcasted_iota(jnp.int32, shape, dim)


def dot(a, b, contract=((1,), (0,)), precision=None):
    return lax.dot_general(a, b, (contract, ((), ())), precision=precision, preferred_element_type=F32)


NT = ((1,), (1,))
TN = ((0,), (0,))


def split(x):
    hi = x.astype(BF16)
    return hi, (x - hi.astype(F32)).astype(BF16)


def at_offset(sizes, d):
    return tuple(lax.rem(lax.axis_index(n) + (s + o), s) if o else lax.axis_index(n) for n, s, o in zip(AXES, sizes, d))


def in_plane(sizes, d):
    dx, flip, dz = d
    x, y, z = at_offset(sizes, (dx, 0, dz))
    return x, y + 1 - 2 * lax.rem(y, 2) if flip else y, z


def greet(devices):
    barrier = pltpu.get_barrier_semaphore()
    for device in devices:
        pl.semaphore_signal(barrier, inc=1, device_id=device, device_id_type=MESH)
    return lambda: pl.semaphore_wait(barrier, len(devices))


def send(src, dst, ssem, rsem, device):
    c = pltpu.make_async_remote_copy(
        src_ref=src, dst_ref=dst, send_sem=ssem, recv_sem=rsem, device_id=device, device_id_type=MESH
    )
    c.start()
    return c


NEAR = [(i, d) for i, d in enumerate(OFFS) if d != (0, 0, 0)]


SIDE = 128


def rows_of(pos):
    loc = pos & (TICKS - 1)
    scale = 1.0 / TICKS
    return (loc & ~31).astype(F32) * scale, (loc & 31).astype(F32) * scale


def stack(parts):
    return parts[0] if len(parts) == 1 else jnp.concatenate(parts, axis=0)


def edges(blks, ranks, base, offs, own, feats, gtab, mst, wz, wr):
    slot = iota((SLOT, 128), 0).astype(F32) + base
    accs = []
    for blk, rank in zip(blks, ranks):
        code = ((blk & 127) + 1).astype(F32)
        acc = jnp.zeros((SLOT, 128), F32)
        for k in range(12):
            acc = jnp.where(rank[k : k + 1] == slot, code[k : k + 1], acc)
        accs.append(acc)
    picks_i = [jnp.where(acc > 0.0, 1.0, 0.0).astype(BF16) for acc in accs]
    named = dot(stack(accs).astype(BF16), jnp.ones((128, 128), BF16))
    lane = iota(named.shape, 1)
    pick_j = jnp.where(named == (lane + 1).astype(F32), 1.0, 0.0).astype(BF16)
    jhi, jlo = rows_of(own)
    pieces = []
    for n, (blk, off, pick_i) in enumerate(zip(blks, offs, picks_i)):
        ihi, ilo = rows_of(blk[12:15])
        shift = jnp.concatenate([jnp.full((1, 128), o, F32) for o in off], axis=0)
        fill = jnp.zeros((2, 128), F32)
        left = jnp.concatenate([-ihi - shift, -ilo, fill], axis=0)
        right = jnp.concatenate([jhi, jlo, fill], axis=0)
        w = jnp.concatenate([left, right], axis=1).astype(BF16)
        both = jnp.concatenate([pick_i, pick_j[SLOT * n : SLOT * (n + 1)]], axis=1)
        pieces.append(dot(both, w, NT).astype(BF16))
    to_lanes = iota((8, 384), 1) >> 7
    spread = jnp.where((to_lanes == iota((8, 384), 0)) | (to_lanes + 3 == iota((8, 384), 0)), 1.0, 0.0).astype(BF16)
    disp = dot(stack(pieces), spread)
    dx, dy, dz = disp[:, 0:128], disp[:, 128:256], disp[:, 256:384]
    r2 = dx * dx + dy * dy + dz * dz
    s2 = r2 + 0.25
    inv = lax.rsqrt(s2)
    rs = s2 * inv
    inv1 = 1.0 / (1.0 + r2)
    t = rs - (0.25 + 0.5 * lax.rem(iota((1, 128), 1), 8).astype(F32))
    b = jnp.exp2((t * (-2.0 * LOG2E)) * t) * inv1
    b = jnp.where(lane < 8, b, b * (-4.0 * t - 2.0 * rs * inv1)).astype(BF16)
    zz = dot(b, wz)
    z, zp = zz[:, 0:128], zz[:, 128:256]
    sig = 0.5 * jnp.tanh(0.5 * z) + 0.5
    silu = z * sig
    hid = jnp.where(lane < 64, silu, (sig + silu * (1.0 - sig)) * zp).astype(BF16)
    rr = dot(hid, wr)
    g = dot(pick_j, gtab)
    g = g[:, 0:128] + g[:, 128:256]
    rad = rr[:, 0:128] * g
    radp = rr[:, 128:256] * g
    h = dot(pick_j, feats)
    q = []
    for r in (rad, radp):
        for d in range(2):
            x = [(r * h[:, 128 * e : 128 * (e + 1)]).astype(BF16) for e in (2 * d, 2 * d + 1)]
            t = dot(jnp.concatenate(x, axis=1), mst)
            q += [t[:, 0:128], t[:, 128:256]]
    ux, uy, uz = dx * inv, dy * inv, dz * inv
    along = ux * q[1] + uy * q[2] + uz * q[3]
    w = q[4] + ux * q[5] + uy * q[6] + uz * q[7] - along * inv
    part = (lane >> 4) & 3
    ua = jnp.where(part == 0, ux, jnp.where(part == 1, uy, uz))
    qa = jnp.where(part == 0, q[1], jnp.where(part == 1, q[2], q[3]))
    out = jnp.where(part == 3, q[0] + along, ua * w + qa * inv)
    rows = [slice(SLOT * n, SLOT * (n + 1)) for n in range(len(blks))]
    return [(pick_i, pick_j[r], out[r]) for pick_i, r in zip(picks_i, rows)]


def per_atom(pick_i, out):
    lane = iota((SLOT, 128), 1)
    hi = out.astype(BF16)
    mixed = jnp.where(lane < 64, hi.astype(F32), out - hi.astype(F32)).astype(BF16)
    s = dot(mixed, pick_i, TN)
    return s[0:64] + s[64:128]


def cell_offset(a):
    if isinstance(a, int):
        return tuple(float(o) for o in OFFS[a])
    return ((a // 9 - 1).astype(F32), (lax.rem(a // 3, 3) - 1).astype(F32), (lax.rem(a, 3) - 1).astype(F32))


def tables(feats, species, rin, rout, gain, mix, readout, cw, ref_energy, gtab, mst, wz, wr, base9, refrow):
    neigh = 12
    lane = iota((8, SIDE), 1)
    sel8 = jnp.where(lax.rem(lane, 16) == iota((8, SIDE), 0), 1.0, 0.0)
    sel1 = jnp.where(lax.rem(iota((1, SIDE), 1), 16) == 8, 1.0, 0.0)
    rc = dot(cw[...], sel8, TN, HIGH) + dot(readout[...], sel1, TN, HIGH)
    mb = (dot(mix[...].astype(F32), rc, precision=HIGH) * (neigh ** -0.5)).astype(BF16)
    mst[0:128, 0:128] = mb
    mst[0:128, 128:256] = jnp.zeros_like(mb)
    mst[128:256, 0:128] = jnp.zeros_like(mb)
    mst[128:256, 128:256] = mb
    base9[...] = dot(rc, feats[:, 0:128].astype(F32), ((0,), (1,)), HIGH)[0:16]
    kinds = gain.shape[0]
    onehot = jnp.where(iota((kinds, SIDE), 0) == species[...], 1.0, 0.0)
    ghi, glo = split(dot(onehot, gain[...], TN, HIGH))
    gtab[:, 0:128] = ghi
    gtab[:, 128:256] = glo
    refrow[...] = jnp.broadcast_to(dot(ref_energy[...], onehot, precision=HIGH), refrow.shape)
    r = rin[...]
    h = rin.shape[1]
    dup = jnp.where(lax.rem(iota((h, 128), 1), h) == iota((h, 128), 0), 1.0, 0.0).astype(BF16)
    upper = jnp.where(iota((h, 128), 1) - h == iota((h, 128), 0), 1.0, 0.0).astype(BF16)
    rows_a = jnp.where(iota((128, 8), 0) == iota((128, 8), 1), 1.0, 0.0).astype(BF16)
    rows_b = jnp.where(iota((128, 8), 0) - 8 == iota((128, 8), 1), 1.0, 0.0).astype(BF16)
    wz[:, 0:128] = dot(dot(rows_a, r).astype(BF16), dup).astype(BF16)
    wz[:, 128:256] = dot(dot(rows_b, r).astype(BF16), upper).astype(BF16)
    ro = rout[...]
    none = jnp.zeros_like(ro)
    wr[0:64, 0:128] = ro
    wr[64:128, 0:128] = none
    wr[0:64, 128:256] = none
    wr[64:128, 128:256] = ro


def rank_edges(lists, ranks, mask):
    lane = iota((16, 128), 1)
    row = iota((16, 128), 0)
    for a in range(27):
        blk = lists[a]
        keep = ((blk >> 7) == 26 - a) & (lane < blk[15:16]) & (row < 12)
        mask[16 * a : 16 * a + 16] = jnp.where(keep, 1.0, 0.0)
    m = mask[...].astype(BF16)
    tri = jnp.where(iota((128, 128), 0) <= iota((128, 128), 1), 1.0, 0.0).astype(BF16)
    both = dot(m, jnp.concatenate([tri, jnp.ones((128, 128), BF16)], axis=1))
    lower = jnp.where(iota((16, 16), 0) > iota((16, 16), 1), 1.0, 0.0).astype(BF16)
    totals = jnp.concatenate([both[16 * a : 16 * a + 16, 128:256] for a in range(27)], axis=1).astype(BF16)
    start = dot(lower, totals)
    peak = start[12:13, 0:128]
    for a in range(27):
        s = start[:, 128 * a : 128 * a + 128]
        peak = jnp.maximum(peak, s[12:13])
        r = both[16 * a : 16 * a + 16, 0:128] + s - 1.0
        ranks[a] = jnp.where(mask[16 * a : 16 * a + 16] > 0.0, r, FAR)
    return peak


def wave_tables(sizes, norm, waves, pos, wrow):
    waves_f = waves[...].astype(F32)
    kvec = [waves_f[d : d + 1] * (2.0 * math.pi / sizes[d]) for d in range(3)]
    ksq = kvec[0] * kvec[0] + kvec[1] * kvec[1] + kvec[2] * kvec[2]
    wrow[0:1] = 2.0 * (8.0 * jnp.exp(ksq * (-1.0 / 64.0)) / (8.0 + ksq) * norm)
    fields = []
    for d in range(3):
        wrow[1 + d : 2 + d] = kvec[d]
        length = float(sizes[d] * TICKS)
        p = pos[d : d + 1]
        fields.append(((p >> 7).astype(F32), waves_f[d : d + 1] * (128.0 / length)))
        fields.append(((p & 127).astype(F32), waves_f[d : d + 1] * (1.0 / length)))
    zero_i = jnp.zeros((2, 128), F32)
    zero_k = jnp.zeros((2, waves_f.shape[1]), F32)
    wrow[8:16] = jnp.concatenate([f[1] for f in fields] + [zero_k], axis=0)
    return jnp.concatenate([f[0] for f in fields] + [zero_i], axis=0).astype(BF16)


def phases(pos8, wrow, cos_h, cos_l, sin_h, sin_l):
    def phase(bi, carry):
        at = pl.ds(pl.multiple_of(bi * 128, 128), 128)
        turn = dot(pos8, wrow[8:16, at].astype(BF16), TN)
        quarter = jnp.floor(turn * 4.0 + 0.5)
        x = (turn - quarter * 0.25) * (2.0 * math.pi)
        qi = quarter.astype(jnp.int32)
        xx = x * x
        s = x * (1.0 + xx * (-1.0 / 6 + xx * (1.0 / 120 + xx * (-1.0 / 5040 + xx * (1.0 / 362880)))))
        c = 1.0 + xx * (-0.5 + xx * (1.0 / 24 + xx * (-1.0 / 720 + xx * (1.0 / 40320))))
        odd = (qi & 1) == 1
        cv = jnp.where(odd, s, c)
        sv = jnp.where(odd, c, s)
        cv = jnp.where(((qi + 1) & 2) == 2, -cv, cv)
        sv = jnp.where((qi & 2) == 2, -sv, sv)
        hi, lo = split(cv)
        cos_h[:, at] = hi
        cos_l[:, at] = lo
        hi, lo = split(sv)
        sin_h[:, at] = hi
        sin_l[:, at] = lo
        return carry

    lax.fori_loop(0, wrow.shape[1] // 128, phase, 0)


def peers(sizes):
    nx, ny, nz = sizes
    plane = [(dx, flip, dz) for dx in range(nx) for flip in range(2) for dz in range(nz)][1:]
    line = [(0, dy, 0) for dy in range(2, ny, 2)]
    near = [d for _, d in NEAR]
    known = [((d[0] + nx) % nx, abs(d[1]), (d[2] + nz) % nz) for d in near]
    whom = [at_offset(sizes, d) for d in near + line] + [in_plane(sizes, d) for d in plane if d not in known]
    return plane, line, whom


def reciprocal(sizes, poison, sums_t, sums_j, base9, pack, refrow, pots, wrow, trig, bufs, sems):
    nx, ny, nz = sizes
    plane, line, _ = peers(sizes)
    cos_h, cos_l, sin_h, sin_l = trig
    got_t, got_j, part, got_rs, block, got_ar, got_ag, lhs, pot_s = bufs
    st, rt, sj, rj, srs, rrs, sar, rar, sag, rag, sp, rp = sems
    blocks = wrow.shape[1] // 128
    first = [send(sums_t.at[i], got_t.at[26 - i], st.at[i], rt.at[i], at_offset(sizes, d)) for i, d in NEAR]
    live = jnp.where(iota((1, 128), 1) < pack[15:16], 1.0, 0.0)
    total = base9[...] + sums_t[13].astype(F32)
    for c in first:
        c.wait()
    for i, _ in NEAR:
        total = total + got_t[i].astype(F32)
    q = total[0:8] * live
    qhi, qlo = split(q)
    q16 = jnp.concatenate([qhi, qlo], axis=0)
    for half, high, low in ((0, cos_h, cos_l), (1, sin_h, sin_l)):
        s = dot(q16, high[...])
        s = s[0:8] + s[8:16] + dot(q16, low[...])[0:8]
        for bi in range(blocks):
            part[2 * bi + half] = s[:, 128 * bi : 128 * bi + 128] + poison
    ix, iy, iz = [lax.axis_index(n) for n in AXES]
    low_x = lax.rem(iy, 2)
    me = (ix * 2 + low_x) * nz + iz
    rs = []
    for n, d in enumerate(plane):
        to = (lax.rem(ix + d[0], nx) * 2 + (1 - low_x if d[1] else low_x)) * nz + lax.rem(iz + d[2], nz)
        rs.append(send(part.at[to], got_rs.at[n], srs.at[n], rrs.at[n], in_plane(sizes, d)))
    second = [send(sums_j.at[i], got_j.at[26 - i], sj.at[i], rj.at[i], at_offset(sizes, d)) for i, d in NEAR]
    acc = part[me]
    for n, c in enumerate(rs):
        c.wait()
        acc = acc + got_rs[n]
    block[0] = acc
    ar = [send(block.at[0], got_ar.at[n], sar.at[n], rar.at[n], at_offset(sizes, d)) for n, d in enumerate(line)]
    for n, c in enumerate(ar):
        c.wait()
        acc = acc + got_ar[n]
    got_ag[me] = acc
    ag = [send(got_ag.at[me], got_ag.at[me], sag.at[n], rag.at[n], in_plane(sizes, d)) for n, d in enumerate(plane)]
    js = sums_j[13].astype(F32)
    for c in second:
        c.wait()
    for i, _ in NEAR:
        js = js + got_j[i].astype(F32)
    for c in ag:
        c.wait()
    for bi in range(blocks):
        at = slice(128 * bi, 128 * bi + 128)
        weight = wrow[0:1, at]
        pre = got_ag[2 * bi] * weight
        pim = got_ag[2 * bi + 1] * weight
        kx, ky, kz = wrow[1:2, at], wrow[2:3, at], wrow[3:4, at]
        lc = jnp.concatenate([pre, kx * pim, ky * pim, kz * pim], axis=0)
        ls = jnp.concatenate([pim, -kx * pre, -ky * pre, -kz * pre], axis=0)
        hi, lo = split(lc)
        lhs[0:32, at] = hi
        lhs[32:64, at] = lo
        hi, lo = split(ls)
        lhs[64:96, at] = hi
        lhs[96:128, at] = lo
    w = dot(lhs[0:64], cos_h[...], NT)
    v = dot(lhs[64:128], sin_h[...], NT)
    w = w[0:32] + w[32:64] + dot(lhs[0:32], cos_l[...], NT)
    w = w + v[0:32] + v[32:64] + dot(lhs[64:96], sin_l[...], NT)
    pot = w[0:8]
    flag = jnp.where(iota((8, 128), 0) == 0, live, 0.0)
    pot16 = jnp.concatenate([pot * live, flag], axis=0)
    pot_s[0] = pot16.astype(BF16)
    third = [send(pot_s.at[0], pots.at[26 - i], sp.at[i], rp.at[i], at_offset(sizes, d)) for i, d in NEAR]
    pots[13] = pot16.astype(BF16)
    rows = []
    for d in range(3):
        wave = jnp.sum(q * w[8 * d + 8 : 8 * d + 16], axis=0, keepdims=True)
        rows.append(wave - jnp.sum(pot16 * js[16 * d : 16 * d + 16], axis=0, keepdims=True))
    site = live * (total[8:9] + refrow[0:1] + 0.5 * jnp.sum(q * pot, axis=0, keepdims=True))
    mine = jnp.concatenate(rows + [site, live, live, live, live], axis=0)
    for c in third:
        c.wait()
    return mine


def pull_back(work, pots):
    prods = []
    for (pick_i, _, out), p in zip(work, pots):
        none = jnp.zeros((16, 128), BF16)
        prods.append(out * dot(pick_i, jnp.concatenate([p, p, p, none, p, p, p, none], axis=0), NT))
    prod = stack(prods)
    hi = prod.astype(BF16)
    mixed = jnp.where(iota(prod.shape, 1) < 64, hi.astype(F32), prod - hi.astype(F32)).astype(BF16)
    return dot(mixed, stack([pick_j for _, pick_j, _ in work]), TN)


def give(mine, t, site, forces):
    t = t[0:64] + t[64:128]
    for d in range(3):
        g = mine[d : d + 1] + jnp.sum(t[16 * d : 16 * d + 16], axis=0, keepdims=True)
        forces[d] = -g * mine[4:5]
    site[...] = mine[3:4]


def gather_pack(neighbors, positions, counts, pack, sem):
    copies = [pltpu.make_async_copy(neighbors.at[k], pack.at[pl.ds(k, 1)], sem.at[k]) for k in range(12)]
    copies += [pltpu.make_async_copy(positions.at[d], pack.at[pl.ds(12 + d, 1)], sem.at[12 + d]) for d in range(3)]
    for c in copies:
        c.start()
    pack[15:16] = jnp.full((1, 128), counts[0, 0], jnp.int32)
    return copies


def hand_out(sizes, pack, lists, ssem, rsem):
    copies = [send(pack, lists.at[26 - i], ssem.at[i], rsem.at[i], at_offset(sizes, d)) for i, d in NEAR]
    lists[13] = pack[...]
    return copies


def whole_kernel(
    sizes, norm, neighbors, positions, counts, *rest,
):
    far, (site, forces), near = rest[:10], rest[10:12], rest[12:22]
    whole_steps(sizes, norm, neighbors, positions, counts, far, near, site, forces, *rest[22:])


def whole_steps(
    sizes, norm, neighbors, positions, counts, far, near, site, forces,
    osem, pack, lists, gtab, mst, wz, wr, base9, refrow, ranks, mask, picks_i, picks_j, outs, sums_t, sums_j, pots, wrow,
    cos_h, cos_l, sin_h, sin_l, got_t, got_j, part, got_rs, block, got_ar, got_ag, lhs, pot_s,
    psem, ls, lr, *sems,
):
    wait = greet(peers(sizes)[2])
    packed = gather_pack(neighbors, positions, counts, pack, psem)
    brought = [pltpu.make_async_copy(f, n, osem.at[i]) for i, (f, n) in enumerate(zip(far, near))]
    for c in brought:
        c.start()
    for c in brought:
        c.wait()
    feats, species, waves, rin, rout, gain, mix, readout, cw, ref_energy = near
    tables(feats, species, rin, rout, gain, mix, readout, cw, ref_energy, gtab, mst, wz, wr, base9, refrow)
    for c in packed:
        c.wait()
    wait()
    out = hand_out(sizes, pack, lists, ls, lr)
    own = pack[12:15]
    trig = (cos_h, cos_l, sin_h, sin_l)
    phases(wave_tables(sizes, norm, waves, own, wrow), wrow, *trig)
    for c in out:
        c.wait()
    peak = rank_edges(lists, ranks, mask)

    def group(gi, carry):
        cells = [gi * GROUP + u for u in range(GROUP)]
        done = edges(
            [lists[a] for a in cells], [ranks[a] for a in cells], 0.0, [cell_offset(a) for a in cells],
            own, feats[...], gtab[...], mst[...], wz[...], wr[...],
        )
        for a, (pick_i, pick_j, e) in zip(cells, done):
            picks_i[a] = pick_i
            picks_j[a] = pick_j
            outs[a] = e
            s = per_atom(pick_i, e).astype(BF16)
            sums_j[a] = s[0:48]
            sums_t[a] = s[48:64]
        return carry

    lax.fori_loop(0, 27 // GROUP, group, 0)
    poison = jnp.where(peak > float(SLOT), jnp.nan, 0.0)
    bufs = (got_t, got_j, part, got_rs, block, got_ar, got_ag, lhs, pot_s)
    mine = reciprocal(sizes, poison, sums_t, sums_j, base9, pack, refrow, pots, wrow, trig, bufs, sems)

    def back(gi, acc):
        cells = [gi * GROUP + u for u in range(GROUP)]
        return acc + pull_back([(picks_i[a], picks_j[a], outs[a]) for a in cells], [pots[a] for a in cells])

    give(mine, lax.fori_loop(0, 27 // GROUP, back, jnp.zeros((128, 128), F32)), site, forces)


def spread_kernel(
    sizes, neighbors, positions, counts, feats, species, rin, rout, gain, mix, readout, cw, ref_energy,
    lists, pack_out, gtab, mst, wz, wr, base9, refrow, pack, psem, ssem, rsem,
):
    wait = greet([at_offset(sizes, d) for _, d in NEAR])
    packed = gather_pack(neighbors, positions, counts, pack, psem)
    tables(feats, species, rin, rout, gain, mix, readout, cw, ref_energy, gtab, mst, wz, wr, base9, refrow)
    for c in packed:
        c.wait()
    wait()
    out = hand_out(sizes, pack, lists, ssem, rsem)
    pack_out[...] = pack[...]
    for c in out:
        c.wait()


def each_piece(ranks, run):
    def cell(a, carry):
        pieces = (jnp.max(ranks[a]).astype(jnp.int32) + SLOT) // SLOT
        return lax.fori_loop(0, pieces, lambda c, carry: run(a, (c * SLOT).astype(F32), carry), carry)

    lax.fori_loop(0, 27, cell, 0)


def edge_kernel(lists, pack, feats, gtab, mst, wz, wr, sums_t, sums_j, mask, ranks, total_t, total_j):
    rank_edges(lists, ranks, mask)
    own = pack[12:15]
    total_t[...] = jnp.zeros_like(total_t)
    total_j[...] = jnp.zeros_like(total_j)

    def piece(a, base, carry):
        pick_i, _, out = edges([lists[a]], [ranks[a]], base, [cell_offset(a)], own, feats[...], gtab[...], mst[...], wz[...], wr[...])[0]
        s = per_atom(pick_i, out)
        total_j[a] += s[0:48]
        total_t[a] += s[48:64]
        return carry

    each_piece(ranks, piece)
    sums_t[...] = total_t[...].astype(BF16)
    sums_j[...] = total_j[...].astype(BF16)


def wave_kernel(
    sizes, norm, sums_t, sums_j, base9, pack, waves, refrow, pots, mine,
    wrow, cos_h, cos_l, sin_h, sin_l, got_t, got_j, part, got_rs, block, got_ar, got_ag, lhs, pot_s, *sems,
):
    wait = greet(peers(sizes)[2])
    trig = (cos_h, cos_l, sin_h, sin_l)
    phases(wave_tables(sizes, norm, waves, pack[12:15], wrow), wrow, *trig)
    wait()
    bufs = (got_t, got_j, part, got_rs, block, got_ar, got_ag, lhs, pot_s)
    mine[...] = reciprocal(sizes, 0.0, sums_t, sums_j, base9, pack, refrow, pots, wrow, trig, bufs, sems)


def force_kernel(pots, mine, lists, pack, feats, gtab, mst, wz, wr, site, forces, mask, ranks, total):
    rank_edges(lists, ranks, mask)
    own = pack[12:15]
    total[...] = jnp.zeros_like(total)

    def piece(a, base, carry):
        work = edges([lists[a]], [ranks[a]], base, [cell_offset(a)], own, feats[...], gtab[...], mst[...], wz[...], wr[...])
        total[...] += pull_back(work, [pots[a]])
        return carry

    each_piece(ranks, piece)
    give(mine[...], total[...], site, forces)


VMEM = pl.BlockSpec(memory_space=pltpu.VMEM)
SMEM = pl.BlockSpec(memory_space=pltpu.SMEM)
HBM = pl.BlockSpec(memory_space=pltpu.HBM)


def shape(dims, kind):
    return jax.ShapeDtypeStruct(dims, kind)


def wave_buffers(sizes, waves):
    nx, ny, nz = sizes
    planes, lines = 2 * nx * nz, ny // 2
    assert planes == 2 * waves // 128
    buf = pltpu.VMEM
    dma = pltpu.SemaphoreType.DMA
    trig = [buf((128, waves), BF16)] * 4
    rest = [
        buf((27, 16, 128), BF16), buf((27, 48, 128), BF16), buf((planes, 8, 128), F32), buf((planes - 1, 8, 128), F32),
        buf((1, 8, 128), F32), buf((lines - 1, 8, 128), F32), buf((planes, 8, 128), F32), buf((128, waves), BF16),
        buf((1, 16, 128), BF16),
    ]
    counts = (27, 27, 27, 27, planes - 1, planes - 1, lines - 1, lines - 1, planes - 1, planes - 1, 27, 27)
    return [buf((16, waves), F32)] + trig + rest, [dma((n,)) for n in counts]


TABLES = [
    ((128, 256), BF16), ((256, 256), BF16), ((128, 256), BF16), ((128, 256), BF16), ((16, 128), F32), ((8, 128), F32),
]
RANKS = [((27, 16, 128), F32), ((27 * 16, 128), F32)]
RESULT = [((1, 128), F32), ((3, 1, 128), F32)]


def general(sizes, norm, neighbors, positions, counts, feats, species, waves, *params):
    dma = pltpu.SemaphoreType.DMA
    lists, pack, gtab, mst, wz, wr, base9, refrow = pl.pallas_call(
        functools.partial(spread_kernel, sizes),
        out_shape=[shape((27, 16, 128), jnp.int32), shape((16, 128), jnp.int32)] + [shape(*t) for t in TABLES],
        in_specs=[HBM, HBM, SMEM] + [VMEM] * 9,
        out_specs=[VMEM] * 8,
        scratch_shapes=[pltpu.VMEM((16, 128), jnp.int32), dma((15,)), dma((27,)), dma((27,))],
        compiler_params=pltpu.CompilerParams(collective_id=1, has_side_effects=True),
        name="spread",
    )(neighbors, positions, counts, feats, species, *params)
    ranking = [pltpu.VMEM(*RANKS[1]), pltpu.VMEM(*RANKS[0])]
    sums_t, sums_j = pl.pallas_call(
        edge_kernel,
        out_shape=[shape((27, 16, 128), BF16), shape((27, 48, 128), BF16)],
        in_specs=[VMEM] * 7,
        out_specs=[VMEM] * 2,
        scratch_shapes=ranking + [pltpu.VMEM((27, 16, 128), F32), pltpu.VMEM((27, 48, 128), F32)],
        name="edges",
    )(lists, pack, feats, gtab, mst, wz, wr)
    bufs, sems = wave_buffers(sizes, waves.shape[1])
    pots, mine = pl.pallas_call(
        functools.partial(wave_kernel, sizes, norm),
        out_shape=[shape((27, 16, 128), BF16), shape((8, 128), F32)],
        in_specs=[VMEM] * 6,
        out_specs=[VMEM] * 2,
        scratch_shapes=bufs + sems,
        compiler_params=pltpu.CompilerParams(collective_id=2, has_side_effects=True),
        name="waves",
    )(sums_t, sums_j, base9, pack, waves, refrow)
    return pl.pallas_call(
        force_kernel,
        out_shape=[shape(*r) for r in RESULT],
        in_specs=[VMEM] * 9,
        out_specs=[VMEM] * 2,
        scratch_shapes=ranking + [pltpu.VMEM((128, 128), F32)],
        name="forces",
    )(pots, mine, lists, pack, feats, gtab, mst, wz, wr)


def direct(sizes, norm, neighbors, positions, counts, feats, species, waves, *params):
    dma = pltpu.SemaphoreType.DMA
    buf = pltpu.VMEM
    bufs, sems = wave_buffers(sizes, waves.shape[1])
    brought = (feats, species, waves) + params
    scratch = [buf(b.shape, b.dtype) for b in brought] + [dma((len(brought),))]
    scratch += [buf((16, 128), jnp.int32), buf((27, 16, 128), jnp.int32)] + [buf(*t) for t in TABLES + RANKS]
    scratch += [buf((27, SLOT, 128), BF16), buf((27, SLOT, 128), BF16), buf((27, SLOT, 128), F32)]
    scratch += [buf((27, 16, 128), BF16), buf((27, 48, 128), BF16), buf((27, 16, 128), BF16)]
    return pl.pallas_call(
        functools.partial(whole_kernel, sizes, norm),
        out_shape=[shape(*r) for r in RESULT],
        in_specs=[HBM, HBM, SMEM] + [HBM] * 10,
        out_specs=[VMEM] * 2,
        scratch_shapes=scratch + bufs + [dma((15,)), dma((27,)), dma((27,))] + sems,
        compiler_params=pltpu.CompilerParams(collective_id=0, has_side_effects=True),
        name="whole",
    )(neighbors, positions, counts, feats, species, waves, *params)


def per_device(
    sizes, features, positions, species, counts, neighbors, waves, radial_in, radial_out,
    species_gain, mix_weight, readout, charge_weight, ref_energy,
):
    nx, ny, nz = sizes
    slots = positions.shape[-1]
    norm = (waves.shape[1] * nx * ny * nz * slots) ** -0.5
    args = (
        neighbors.reshape(12, 1, slots), positions.reshape(3, 1, slots), counts.reshape(1, 1),
        features.reshape(slots, -1), species.reshape(1, slots), waves, radial_in, radial_out, species_gain,
        mix_weight, readout.reshape(1, -1), charge_weight.T, ref_energy.reshape(1, -1),
    )
    site, forces = direct(sizes, norm, *args)
    crowded = jnp.isnan(site[0, 0])
    site, forces = lax.cond(
        crowded, lambda s, f, *a: tuple(general(sizes, norm, *a)), lambda s, f, *a: (s, f), site, forces, *args
    )
    return site.reshape(1, 1, 1, slots), forces.reshape(1, 1, 1, 3, slots)


def solution(mesh):
    sizes = tuple(mesh.shape[n] for n in AXES)
    cell = P("gx", "gy", "gz")
    placed = (cell,) * 5 + (P(),) * 8
    return jax.shard_map(
        functools.partial(per_device, sizes),
        mesh=mesh,
        in_specs=placed,
        out_specs=(cell, cell),
        check_vma=False,
    )
```

```python
import functools
import math

import jax
import jax.numpy as jnp
from jax import lax
from jax.experimental import pallas as pl
from jax.experimental.pallas import tpu as pltpu
from jax.sharding import PartitionSpec as P

TICKS = 1024
AXES = ("gx", "gy", "gz")
MESH = pl.DeviceIdType.MESH
HIGH = lax.Precision.HIGHEST
OFFS = [(a - 1, b - 1, c - 1) for a in range(3) for b in range(3) for c in range(3)]
F32 = jnp.float32
BF16 = jnp.bfloat16
SLOT = 96
GROUP = 9
LOG2E = math.log2(math.e)
FAR = -1.0e6
LIST = jnp.int16


def iota(shape, dim):
    return lax.broadcasted_iota(jnp.int32, shape, dim)


def dot(a, b, contract=((1,), (0,)), precision=None):
    return lax.dot_general(a, b, (contract, ((), ())), precision=precision, preferred_element_type=F32)


NT = ((1,), (1,))
TN = ((0,), (0,))


def split(x):
    hi = x.astype(BF16)
    return hi, (x - hi.astype(F32)).astype(BF16)


def at_offset(sizes, d):
    return tuple(lax.rem(lax.axis_index(n) + (s + o), s) if o else lax.axis_index(n) for n, s, o in zip(AXES, sizes, d))


def in_plane(sizes, d):
    dx, flip, dz = d
    x, y, z = at_offset(sizes, (dx, 0, dz))
    return x, y + 1 - 2 * lax.rem(y, 2) if flip else y, z


def greet(devices):
    barrier = pltpu.get_barrier_semaphore()
    for device in devices:
        pl.semaphore_signal(barrier, inc=1, device_id=device, device_id_type=MESH)
    return lambda: pl.semaphore_wait(barrier, len(devices))


def send(src, dst, ssem, rsem, device):
    c = pltpu.make_async_remote_copy(
        src_ref=src, dst_ref=dst, send_sem=ssem, recv_sem=rsem, device_id=device, device_id_type=MESH
    )
    c.start()
    return c


NEAR = [(i, d) for i, d in enumerate(OFFS) if d != (0, 0, 0)]


SIDE = 128


def rows_of(pos):
    loc = pos & (TICKS - 1)
    scale = 1.0 / TICKS
    return (loc & ~31).astype(F32) * scale, (loc & 31).astype(F32) * scale


def wide(x):
    return x.astype(jnp.int32)


def stack(parts):
    return parts[0] if len(parts) == 1 else jnp.concatenate(parts, axis=0)


def find(blks, ranks, base):
    slot = iota((SLOT, 128), 0).astype(F32) + base
    accs = []
    for blk, rank in zip(blks, ranks):
        code = ((blk & 127) + 1).astype(F32)
        acc = jnp.zeros((SLOT, 128), F32)
        for k in range(12):
            acc = jnp.where(rank[k : k + 1] == slot, code[k : k + 1], acc)
        accs.append(acc)
    picks_i = [jnp.where(acc > 0.0, 1.0, 0.0).astype(BF16) for acc in accs]
    named = dot(stack(accs).astype(BF16), jnp.ones((128, 128), BF16))
    lane = iota(named.shape, 1)
    return picks_i, jnp.where(named == (lane + 1).astype(F32), 1.0, 0.0).astype(BF16)


def distance(blks, offs, own, picks_i, pick_j):
    jhi, jlo = rows_of(own)
    pieces = []
    for n, (blk, off, pick_i) in enumerate(zip(blks, offs, picks_i)):
        ihi, ilo = rows_of(blk[12:15])
        shift = jnp.concatenate([jnp.full((1, 128), o, F32) for o in off], axis=0)
        fill = jnp.zeros((2, 128), F32)
        left = jnp.concatenate([-ihi - shift, -ilo, fill], axis=0)
        right = jnp.concatenate([jhi, jlo, fill], axis=0)
        w = jnp.concatenate([left, right], axis=1).astype(BF16)
        both = jnp.concatenate([pick_i, pick_j[SLOT * n : SLOT * (n + 1)]], axis=1)
        pieces.append(dot(both, w, NT).astype(BF16))
    to_lanes = iota((8, 384), 1) >> 7
    spread = jnp.where((to_lanes == iota((8, 384), 0)) | (to_lanes + 3 == iota((8, 384), 0)), 1.0, 0.0).astype(BF16)
    return dot(stack(pieces), spread)


def basis(disp):
    dx, dy, dz = disp[:, 0:128], disp[:, 128:256], disp[:, 256:384]
    r2 = dx * dx + dy * dy + dz * dz
    s2 = r2 + 0.25
    inv = lax.rsqrt(s2)
    rs = s2 * inv
    inv1 = 1.0 / (1.0 + r2)
    t = rs - (0.25 + 0.5 * lax.rem(iota((1, 128), 1), 8).astype(F32))
    b = jnp.exp2((t * (-2.0 * LOG2E)) * t) * inv1
    return (dx * inv, dy * inv, dz * inv), inv, rs, inv1, t, b


def sigmoid(z):
    return 0.5 * jnp.tanh(0.5 * z) + 0.5


def gains(pick_j, gtab):
    g = dot(pick_j, gtab)
    return g[:, 0:128] + g[:, 128:256]


def forward(disp, pick_j, feats, gtab, mst, wz, wr):
    (ux, uy, uz), _, _, _, _, b = basis(disp)
    z = dot(b.astype(BF16), wz[:, 0:128])
    rad = dot((z * sigmoid(z)).astype(BF16), wr[:, 0:128]) * gains(pick_j, gtab)
    h = dot(pick_j, feats)
    x = h[:, 0:128] + ux * h[:, 128:256] + uy * h[:, 256:384] + uz * h[:, 384:512]
    return dot((rad * x).astype(BF16), mst[0:128, 0:128])


def slopes(disp, pick_j, feats, gtab, mst, wz, wr):
    lane = iota((disp.shape[0], 128), 1)
    (ux, uy, uz), inv, rs, inv1, t, b = basis(disp)
    b = jnp.where(lane < 8, b, b * (-4.0 * t - 2.0 * rs * inv1)).astype(BF16)
    zz = dot(b, wz)
    z, zp = zz[:, 0:128], zz[:, 128:256]
    sig = sigmoid(z)
    silu = z * sig
    hid = jnp.where(lane < 64, silu, (sig + silu * (1.0 - sig)) * zp).astype(BF16)
    rr = dot(hid, wr)
    g = gains(pick_j, gtab)
    rad = rr[:, 0:128] * g
    radp = rr[:, 128:256] * g
    h = dot(pick_j, feats)
    q = []
    for r in (rad, radp):
        for d in range(2):
            x = [(r * h[:, 128 * e : 128 * (e + 1)]).astype(BF16) for e in (2 * d, 2 * d + 1)]
            t = dot(jnp.concatenate(x, axis=1), mst)
            q += [t[:, 0:128], t[:, 128:256]]
    along = ux * q[1] + uy * q[2] + uz * q[3]
    w = q[4] + ux * q[5] + uy * q[6] + uz * q[7] - along * inv
    part = (lane >> 4) & 3
    ua = jnp.where(part == 0, ux, jnp.where(part == 1, uy, uz))
    qa = jnp.where(part == 0, q[1], jnp.where(part == 1, q[2], q[3]))
    return jnp.where(part == 3, q[0] + along, ua * w + qa * inv)


def edges(blk, rank, base, off, own, *tabs):
    picks_i, pick_j = find([blk], [rank], base)
    return picks_i[0], pick_j, slopes(distance([blk], [off], own, picks_i, pick_j), pick_j, *tabs)


def per_atom(pick_i, out):
    lane = iota((SLOT, 128), 1)
    hi = out.astype(BF16)
    mixed = jnp.where(lane < 64, hi.astype(F32), out - hi.astype(F32)).astype(BF16)
    s = dot(mixed, pick_i, TN)
    return s[0:64] + s[64:128]


def cell_offset(a):
    if isinstance(a, int):
        return tuple(float(o) for o in OFFS[a])
    return ((a // 9 - 1).astype(F32), (lax.rem(a // 3, 3) - 1).astype(F32), (lax.rem(a, 3) - 1).astype(F32))


def tables(feats, species, rin, rout, gain, mix, readout, cw, ref_energy, gtab, mst, wz, wr, base9, refrow):
    neigh = 12
    lane = iota((8, SIDE), 1)
    sel8 = jnp.where(lax.rem(lane, 16) == iota((8, SIDE), 0), 1.0, 0.0)
    sel1 = jnp.where(lax.rem(iota((1, SIDE), 1), 16) == 8, 1.0, 0.0)
    rc = dot(cw[...], sel8, TN, HIGH) + dot(readout[...], sel1, TN, HIGH)
    mb = (dot(mix[...].astype(F32), rc, precision=HIGH) * (neigh ** -0.5)).astype(BF16)
    mst[0:128, 0:128] = mb
    mst[0:128, 128:256] = jnp.zeros_like(mb)
    mst[128:256, 0:128] = jnp.zeros_like(mb)
    mst[128:256, 128:256] = mb
    base9[...] = dot(rc, feats[:, 0:128].astype(F32), ((0,), (1,)), HIGH)[0:16]
    kinds = gain.shape[0]
    onehot = jnp.where(iota((kinds, SIDE), 0) == species[...], 1.0, 0.0)
    ghi, glo = split(dot(onehot, gain[...], TN, HIGH))
    gtab[:, 0:128] = ghi
    gtab[:, 128:256] = glo
    refrow[...] = jnp.broadcast_to(dot(ref_energy[...], onehot, precision=HIGH), refrow.shape)
    r = rin[...]
    h = rin.shape[1]
    dup = jnp.where(lax.rem(iota((h, 128), 1), h) == iota((h, 128), 0), 1.0, 0.0).astype(BF16)
    upper = jnp.where(iota((h, 128), 1) - h == iota((h, 128), 0), 1.0, 0.0).astype(BF16)
    rows_a = jnp.where(iota((128, 8), 0) == iota((128, 8), 1), 1.0, 0.0).astype(BF16)
    rows_b = jnp.where(iota((128, 8), 0) - 8 == iota((128, 8), 1), 1.0, 0.0).astype(BF16)
    wz[:, 0:128] = dot(dot(rows_a, r).astype(BF16), dup).astype(BF16)
    wz[:, 128:256] = dot(dot(rows_b, r).astype(BF16), upper).astype(BF16)
    ro = rout[...]
    none = jnp.zeros_like(ro)
    wr[0:64, 0:128] = ro
    wr[64:128, 0:128] = none
    wr[0:64, 128:256] = none
    wr[64:128, 128:256] = ro


def rank_edges(lists, ranks, mask):
    lane = iota((16, 128), 1)
    row = iota((16, 128), 0)
    for a in range(27):
        blk = wide(lists[a])
        keep = ((blk >> 7) == 26 - a) & (lane < blk[15:16]) & (row < 12)
        mask[16 * a : 16 * a + 16] = jnp.where(keep, 1.0, 0.0)
    m = mask[...].astype(BF16)
    tri = jnp.where(iota((128, 128), 0) <= iota((128, 128), 1), 1.0, 0.0).astype(BF16)
    both = dot(m, jnp.concatenate([tri, jnp.ones((128, 128), BF16)], axis=1))
    lower = jnp.where(iota((16, 16), 0) > iota((16, 16), 1), 1.0, 0.0).astype(BF16)
    totals = jnp.concatenate([both[16 * a : 16 * a + 16, 128:256] for a in range(27)], axis=1).astype(BF16)
    start = dot(lower, totals)
    peak = start[12:13, 0:128]
    for a in range(27):
        s = start[:, 128 * a : 128 * a + 128]
        peak = jnp.maximum(peak, s[12:13])
        r = both[16 * a : 16 * a + 16, 0:128] + s - 1.0
        ranks[a] = jnp.where(mask[16 * a : 16 * a + 16] > 0.0, r, FAR)
    return peak


def wave_tables(sizes, norm, waves, pos, wrow):
    waves_f = waves[...].astype(F32)
    kvec = [waves_f[d : d + 1] * (2.0 * math.pi / sizes[d]) for d in range(3)]
    ksq = kvec[0] * kvec[0] + kvec[1] * kvec[1] + kvec[2] * kvec[2]
    wrow[0:1] = 2.0 * (8.0 * jnp.exp(ksq * (-1.0 / 64.0)) / (8.0 + ksq) * norm)
    fields = []
    for d in range(3):
        wrow[1 + d : 2 + d] = kvec[d]
        length = float(sizes[d] * TICKS)
        p = pos[d : d + 1]
        fields.append(((p >> 7).astype(F32), waves_f[d : d + 1] * (128.0 / length)))
        fields.append(((p & 127).astype(F32), waves_f[d : d + 1] * (1.0 / length)))
    zero_i = jnp.zeros((2, 128), F32)
    zero_k = jnp.zeros((2, waves_f.shape[1]), F32)
    wrow[8:16] = jnp.concatenate([f[1] for f in fields] + [zero_k], axis=0)
    return jnp.concatenate([f[0] for f in fields] + [zero_i], axis=0).astype(BF16)


def phases(pos8, wrow, cos_h, cos_l, sin_h, sin_l):
    def phase(bi, carry):
        at = pl.ds(pl.multiple_of(bi * 128, 128), 128)
        turn = dot(pos8, wrow[8:16, at].astype(BF16), TN)
        quarter = jnp.floor(turn * 4.0 + 0.5)
        x = (turn - quarter * 0.25) * (2.0 * math.pi)
        qi = quarter.astype(jnp.int32)
        xx = x * x
        s = x * (1.0 + xx * (-1.0 / 6 + xx * (1.0 / 120 + xx * (-1.0 / 5040 + xx * (1.0 / 362880)))))
        c = 1.0 + xx * (-0.5 + xx * (1.0 / 24 + xx * (-1.0 / 720 + xx * (1.0 / 40320))))
        odd = (qi & 1) == 1
        cv = jnp.where(odd, s, c)
        sv = jnp.where(odd, c, s)
        cv = jnp.where(((qi + 1) & 2) == 2, -cv, cv)
        sv = jnp.where((qi & 2) == 2, -sv, sv)
        hi, lo = split(cv)
        cos_h[:, at] = hi
        cos_l[:, at] = lo
        hi, lo = split(sv)
        sin_h[:, at] = hi
        sin_l[:, at] = lo
        return carry

    lax.fori_loop(0, wrow.shape[1] // 128, phase, 0)


def peers(sizes):
    nx, ny, nz = sizes
    plane = [(dx, flip, dz) for dx in range(nx) for flip in range(2) for dz in range(nz)][1:]
    line = [(0, dy, 0) for dy in range(2, ny, 2)]
    near = [d for _, d in NEAR]
    known = [((d[0] + nx) % nx, abs(d[1]), (d[2] + nz) % nz) for d in near]
    whom = [at_offset(sizes, d) for d in near + line] + [in_plane(sizes, d) for d in plane if d not in known]
    return plane, line, whom


def reciprocal(sizes, poison, sums_t, sums_j, base9, pack, refrow, pots, wrow, trig, bufs, sems, meanwhile=lambda n: None):
    nx, ny, nz = sizes
    plane, line, _ = peers(sizes)
    cos_h, cos_l, sin_h, sin_l = trig
    got_t, got_j, part, got_rs, block, got_ar, got_ag, lhs, pot_s = bufs
    st, rt, sj, rj, srs, rrs, sar, rar, sag, rag, sp, rp = sems
    blocks = wrow.shape[1] // 128
    first = [send(sums_t.at[i], got_t.at[26 - i], st.at[i], rt.at[i], at_offset(sizes, d)) for i, d in NEAR]
    live = jnp.where(iota((1, 128), 1) < pack[15:16], 1.0, 0.0)
    total = base9[...] + sums_t[13].astype(F32)
    meanwhile(0)
    for c in first:
        c.wait()
    for i, _ in NEAR:
        total = total + got_t[i].astype(F32)
    q = total[0:8] * live
    qhi, qlo = split(q)
    q16 = jnp.concatenate([qhi, qlo], axis=0)
    for half, high, low in ((0, cos_h, cos_l), (1, sin_h, sin_l)):
        s = dot(q16, high[...])
        s = s[0:8] + s[8:16] + dot(q16, low[...])[0:8]
        for bi in range(blocks):
            part[2 * bi + half] = s[:, 128 * bi : 128 * bi + 128] + poison
    ix, iy, iz = [lax.axis_index(n) for n in AXES]
    low_x = lax.rem(iy, 2)
    me = (ix * 2 + low_x) * nz + iz
    rs = []
    for n, d in enumerate(plane):
        to = (lax.rem(ix + d[0], nx) * 2 + (1 - low_x if d[1] else low_x)) * nz + lax.rem(iz + d[2], nz)
        rs.append(send(part.at[to], got_rs.at[n], srs.at[n], rrs.at[n], in_plane(sizes, d)))
    meanwhile(1)
    acc = part[me]
    for n, c in enumerate(rs):
        c.wait()
        acc = acc + got_rs[n]
    block[0] = acc
    ar = [send(block.at[0], got_ar.at[n], sar.at[n], rar.at[n], at_offset(sizes, d)) for n, d in enumerate(line)]
    meanwhile(2)
    for n, c in enumerate(ar):
        c.wait()
        acc = acc + got_ar[n]
    got_ag[me] = acc
    ag = [send(got_ag.at[me], got_ag.at[me], sag.at[n], rag.at[n], in_plane(sizes, d)) for n, d in enumerate(plane)]
    second = [send(sums_j.at[i], got_j.at[26 - i], sj.at[i], rj.at[i], at_offset(sizes, d)) for i, d in NEAR]
    for c in ag:
        c.wait()
    for bi in range(blocks):
        at = slice(128 * bi, 128 * bi + 128)
        weight = wrow[0:1, at]
        pre = got_ag[2 * bi] * weight
        pim = got_ag[2 * bi + 1] * weight
        kx, ky, kz = wrow[1:2, at], wrow[2:3, at], wrow[3:4, at]
        lc = jnp.concatenate([pre, kx * pim, ky * pim, kz * pim], axis=0)
        ls = jnp.concatenate([pim, -kx * pre, -ky * pre, -kz * pre], axis=0)
        hi, lo = split(lc)
        lhs[0:32, at] = hi
        lhs[32:64, at] = lo
        hi, lo = split(ls)
        lhs[64:96, at] = hi
        lhs[96:128, at] = lo
    w = dot(lhs[0:64], cos_h[...], NT)
    v = dot(lhs[64:128], sin_h[...], NT)
    w = w[0:32] + w[32:64] + dot(lhs[0:32], cos_l[...], NT)
    w = w + v[0:32] + v[32:64] + dot(lhs[64:96], sin_l[...], NT)
    pot = w[0:8]
    flag = jnp.where(iota((8, 128), 0) == 0, live, 0.0)
    pot16 = jnp.concatenate([pot * live, flag], axis=0)
    pot_s[0] = pot16.astype(BF16)
    third = [send(pot_s.at[0], pots.at[26 - i], sp.at[i], rp.at[i], at_offset(sizes, d)) for i, d in NEAR]
    pots[13] = pot16.astype(BF16)
    js = sums_j[13].astype(F32)
    for c in second:
        c.wait()
    for i, _ in NEAR:
        js = js + got_j[i].astype(F32)
    rows = []
    for d in range(3):
        wave = jnp.sum(q * w[8 * d + 8 : 8 * d + 16], axis=0, keepdims=True)
        rows.append(wave - jnp.sum(pot16 * js[16 * d : 16 * d + 16], axis=0, keepdims=True))
    site = live * (total[8:9] + refrow[0:1] + 0.5 * jnp.sum(q * pot, axis=0, keepdims=True))
    mine = jnp.concatenate(rows + [site, live, live, live, live], axis=0)
    for c in third:
        c.wait()
    return mine


def pull_back(work, pots):
    prods = []
    for (pick_i, _, out), p in zip(work, pots):
        none = jnp.zeros((16, 128), BF16)
        prods.append(out * dot(pick_i, jnp.concatenate([p, p, p, none, p, p, p, none], axis=0), NT))
    prod = stack(prods)
    hi = prod.astype(BF16)
    mixed = jnp.where(iota(prod.shape, 1) < 64, hi.astype(F32), prod - hi.astype(F32)).astype(BF16)
    return dot(mixed, stack([pick_j for _, pick_j, _ in work]), TN)


def give(mine, t, site, forces):
    t = t[0:64] + t[64:128]
    for d in range(3):
        g = mine[d : d + 1] + jnp.sum(t[16 * d : 16 * d + 16], axis=0, keepdims=True)
        forces[d] = -g * mine[4:5]
    site[...] = mine[3:4]


def gather_pack(neighbors, positions, counts, pack, sem):
    copies = [pltpu.make_async_copy(neighbors.at[k], pack.at[pl.ds(k, 1)], sem.at[k]) for k in range(12)]
    copies += [pltpu.make_async_copy(positions.at[d], pack.at[pl.ds(12 + d, 1)], sem.at[12 + d]) for d in range(3)]
    for c in copies:
        c.start()
    pack[15:16] = jnp.full((1, 128), counts[0, 0], jnp.int32)
    return copies


def hand_out(sizes, pack, lists, ssem, rsem):
    copies = [send(pack, lists.at[26 - i], ssem.at[i], rsem.at[i], at_offset(sizes, d)) for i, d in NEAR]
    lists[13] = pack[...]
    return copies


def shorten(pack, short):
    row = iota((16, 128), 0)
    local = (row >= 12) & (row < 15)
    short[...] = jnp.where(local, pack[...] & (TICKS - 1), pack[...]).astype(LIST)


def whole_kernel(
    sizes, norm, neighbors, positions, counts, *rest,
):
    far, (site, forces), near = rest[:10], rest[10:12], rest[12:22]
    whole_steps(sizes, norm, neighbors, positions, counts, far, near, site, forces, *rest[22:])


def whole_steps(
    sizes, norm, neighbors, positions, counts, far, near, site, forces,
    osem, pack, short, lists, gtab, mst, wz, wr, base9, refrow, ranks, mask, picks_i, picks_j, outs, sums_t, sums_j, pots, wrow,
    cos_h, cos_l, sin_h, sin_l, got_t, got_j, part, got_rs, block, got_ar, got_ag, lhs, pot_s,
    psem, ls, lr, *sems,
):
    wait = greet(peers(sizes)[2])
    packed = gather_pack(neighbors, positions, counts, pack, psem)
    brought = [pltpu.make_async_copy(f, n, osem.at[i]) for i, (f, n) in enumerate(zip(far, near))]
    for c in brought:
        c.start()
    for c in brought:
        c.wait()
    feats, species, waves, rin, rout, gain, mix, readout, cw, ref_energy = near
    tables(feats, species, rin, rout, gain, mix, readout, cw, ref_energy, gtab, mst, wz, wr, base9, refrow)
    for c in packed:
        c.wait()
    shorten(pack, short)
    wait()
    out = hand_out(sizes, short, lists, ls, lr)
    own = pack[12:15]
    trig = (cos_h, cos_l, sin_h, sin_l)
    phases(wave_tables(sizes, norm, waves, own, wrow), wrow, *trig)
    for c in out:
        c.wait()
    peak = rank_edges(lists, ranks, mask)

    tabs = (feats, gtab, mst, wz, wr)

    def first(gi, carry):
        cells = [gi * GROUP + u for u in range(GROUP)]
        blks = [wide(lists[a]) for a in cells]
        found, pick_j = find(blks, [ranks[a] for a in cells], 0.0)
        disp = distance(blks, [cell_offset(a) for a in cells], own, found, pick_j)
        out = forward(disp, pick_j, *[t[...] for t in tabs])
        for n, a in enumerate(cells):
            rows = slice(SLOT * n, SLOT * n + SLOT)
            picks_i[a] = found[n]
            picks_j[a] = pick_j[rows]
            sums_t[a] = per_atom(found[n], out[rows])[0:16].astype(BF16)
        return carry

    def later(gi):
        cells = [gi * GROUP + u for u in range(GROUP)]
        found = [picks_i[a] for a in cells]
        pick_j = stack([picks_j[a] for a in cells])
        disp = distance([wide(lists[a]) for a in cells], [cell_offset(a) for a in cells], own, found, pick_j)
        out = slopes(disp, pick_j, *[t[...] for t in tabs])
        for n, a in enumerate(cells):
            rows = slice(SLOT * n, SLOT * n + SLOT)
            outs[a] = out[rows]
            sums_j[a] = per_atom(found[n], out[rows])[0:48].astype(BF16)

    lax.fori_loop(0, 27 // GROUP, first, 0)
    poison = jnp.where(peak > float(SLOT), jnp.nan, 0.0)
    bufs = (got_t, got_j, part, got_rs, block, got_ar, got_ag, lhs, pot_s)
    mine = reciprocal(sizes, poison, sums_t, sums_j, base9, pack, refrow, pots, wrow, trig, bufs, sems, later)

    def back(gi, acc):
        cells = [gi * GROUP + u for u in range(GROUP)]
        return acc + pull_back([(picks_i[a], picks_j[a], outs[a]) for a in cells], [pots[a] for a in cells])

    give(mine, lax.fori_loop(0, 27 // GROUP, back, jnp.zeros((128, 128), F32)), site, forces)


def spread_kernel(
    sizes, neighbors, positions, counts, feats, species, rin, rout, gain, mix, readout, cw, ref_energy,
    lists, pack_out, gtab, mst, wz, wr, base9, refrow, pack, short, psem, ssem, rsem,
):
    wait = greet([at_offset(sizes, d) for _, d in NEAR])
    packed = gather_pack(neighbors, positions, counts, pack, psem)
    tables(feats, species, rin, rout, gain, mix, readout, cw, ref_energy, gtab, mst, wz, wr, base9, refrow)
    for c in packed:
        c.wait()
    shorten(pack, short)
    wait()
    out = hand_out(sizes, short, lists, ssem, rsem)
    pack_out[...] = pack[...]
    for c in out:
        c.wait()


def each_piece(ranks, run):
    def cell(a, carry):
        pieces = (jnp.max(ranks[a]).astype(jnp.int32) + SLOT) // SLOT
        return lax.fori_loop(0, pieces, lambda c, carry: run(a, (c * SLOT).astype(F32), carry), carry)

    lax.fori_loop(0, 27, cell, 0)


def edge_kernel(lists, pack, feats, gtab, mst, wz, wr, sums_t, sums_j, mask, ranks, total_t, total_j):
    rank_edges(lists, ranks, mask)
    own = pack[12:15]
    total_t[...] = jnp.zeros_like(total_t)
    total_j[...] = jnp.zeros_like(total_j)

    def piece(a, base, carry):
        pick_i, _, out = edges(wide(lists[a]), ranks[a], base, cell_offset(a), own, feats[...], gtab[...], mst[...], wz[...], wr[...])
        s = per_atom(pick_i, out)
        total_j[a] += s[0:48]
        total_t[a] += s[48:64]
        return carry

    each_piece(ranks, piece)
    sums_t[...] = total_t[...].astype(BF16)
    sums_j[...] = total_j[...].astype(BF16)


def wave_kernel(
    sizes, norm, sums_t, sums_j, base9, pack, waves, refrow, pots, mine,
    wrow, cos_h, cos_l, sin_h, sin_l, got_t, got_j, part, got_rs, block, got_ar, got_ag, lhs, pot_s, *sems,
):
    wait = greet(peers(sizes)[2])
    trig = (cos_h, cos_l, sin_h, sin_l)
    phases(wave_tables(sizes, norm, waves, pack[12:15], wrow), wrow, *trig)
    wait()
    bufs = (got_t, got_j, part, got_rs, block, got_ar, got_ag, lhs, pot_s)
    mine[...] = reciprocal(sizes, 0.0, sums_t, sums_j, base9, pack, refrow, pots, wrow, trig, bufs, sems)


def force_kernel(pots, mine, lists, pack, feats, gtab, mst, wz, wr, site, forces, mask, ranks, total):
    rank_edges(lists, ranks, mask)
    own = pack[12:15]
    total[...] = jnp.zeros_like(total)

    def piece(a, base, carry):
        work = edges(wide(lists[a]), ranks[a], base, cell_offset(a), own, feats[...], gtab[...], mst[...], wz[...], wr[...])
        total[...] += pull_back([work], [pots[a]])
        return carry

    each_piece(ranks, piece)
    give(mine[...], total[...], site, forces)


VMEM = pl.BlockSpec(memory_space=pltpu.VMEM)
SMEM = pl.BlockSpec(memory_space=pltpu.SMEM)
HBM = pl.BlockSpec(memory_space=pltpu.HBM)


def shape(dims, kind):
    return jax.ShapeDtypeStruct(dims, kind)


def wave_buffers(sizes, waves):
    nx, ny, nz = sizes
    planes, lines = 2 * nx * nz, ny // 2
    assert planes == 2 * waves // 128
    buf = pltpu.VMEM
    dma = pltpu.SemaphoreType.DMA
    trig = [buf((128, waves), BF16)] * 4
    rest = [
        buf((27, 16, 128), BF16), buf((27, 48, 128), BF16), buf((planes, 8, 128), F32), buf((planes - 1, 8, 128), F32),
        buf((1, 8, 128), F32), buf((lines - 1, 8, 128), F32), buf((planes, 8, 128), F32), buf((128, waves), BF16),
        buf((1, 16, 128), BF16),
    ]
    counts = (27, 27, 27, 27, planes - 1, planes - 1, lines - 1, lines - 1, planes - 1, planes - 1, 27, 27)
    return [buf((16, waves), F32)] + trig + rest, [dma((n,)) for n in counts]


TABLES = [
    ((128, 256), BF16), ((256, 256), BF16), ((128, 256), BF16), ((128, 256), BF16), ((16, 128), F32), ((8, 128), F32),
]
RANKS = [((27, 16, 128), F32), ((27 * 16, 128), F32)]
RESULT = [((1, 128), F32), ((3, 1, 128), F32)]


def general(sizes, norm, neighbors, positions, counts, feats, species, waves, *params):
    dma = pltpu.SemaphoreType.DMA
    lists, pack, gtab, mst, wz, wr, base9, refrow = pl.pallas_call(
        functools.partial(spread_kernel, sizes),
        out_shape=[shape((27, 16, 128), LIST), shape((16, 128), jnp.int32)] + [shape(*t) for t in TABLES],
        in_specs=[HBM, HBM, SMEM] + [VMEM] * 9,
        out_specs=[VMEM] * 8,
        scratch_shapes=[pltpu.VMEM((16, 128), jnp.int32), pltpu.VMEM((16, 128), LIST), dma((15,)), dma((27,)), dma((27,))],
        compiler_params=pltpu.CompilerParams(collective_id=1, has_side_effects=True),
        name="spread",
    )(neighbors, positions, counts, feats, species, *params)
    ranking = [pltpu.VMEM(*RANKS[1]), pltpu.VMEM(*RANKS[0])]
    sums_t, sums_j = pl.pallas_call(
        edge_kernel,
        out_shape=[shape((27, 16, 128), BF16), shape((27, 48, 128), BF16)],
        in_specs=[VMEM] * 7,
        out_specs=[VMEM] * 2,
        scratch_shapes=ranking + [pltpu.VMEM((27, 16, 128), F32), pltpu.VMEM((27, 48, 128), F32)],
        name="edges",
    )(lists, pack, feats, gtab, mst, wz, wr)
    bufs, sems = wave_buffers(sizes, waves.shape[1])
    pots, mine = pl.pallas_call(
        functools.partial(wave_kernel, sizes, norm),
        out_shape=[shape((27, 16, 128), BF16), shape((8, 128), F32)],
        in_specs=[VMEM] * 6,
        out_specs=[VMEM] * 2,
        scratch_shapes=bufs + sems,
        compiler_params=pltpu.CompilerParams(collective_id=2, has_side_effects=True),
        name="waves",
    )(sums_t, sums_j, base9, pack, waves, refrow)
    return pl.pallas_call(
        force_kernel,
        out_shape=[shape(*r) for r in RESULT],
        in_specs=[VMEM] * 9,
        out_specs=[VMEM] * 2,
        scratch_shapes=ranking + [pltpu.VMEM((128, 128), F32)],
        name="forces",
    )(pots, mine, lists, pack, feats, gtab, mst, wz, wr)


def direct(sizes, norm, neighbors, positions, counts, feats, species, waves, *params):
    dma = pltpu.SemaphoreType.DMA
    buf = pltpu.VMEM
    bufs, sems = wave_buffers(sizes, waves.shape[1])
    brought = (feats, species, waves) + params
    scratch = [buf(b.shape, b.dtype) for b in brought] + [dma((len(brought),))]
    scratch += [buf((16, 128), jnp.int32), buf((16, 128), LIST), buf((27, 16, 128), LIST)] + [buf(*t) for t in TABLES + RANKS]
    scratch += [buf((27, SLOT, 128), BF16), buf((27, SLOT, 128), BF16), buf((27, SLOT, 128), F32)]
    scratch += [buf((27, 16, 128), BF16), buf((27, 48, 128), BF16), buf((27, 16, 128), BF16)]
    return pl.pallas_call(
        functools.partial(whole_kernel, sizes, norm),
        out_shape=[shape(*r) for r in RESULT],
        in_specs=[HBM, HBM, SMEM] + [HBM] * 10,
        out_specs=[VMEM] * 2,
        scratch_shapes=scratch + bufs + [dma((15,)), dma((27,)), dma((27,))] + sems,
        compiler_params=pltpu.CompilerParams(collective_id=0, has_side_effects=True),
        name="whole",
    )(neighbors, positions, counts, feats, species, waves, *params)


def per_device(
    sizes, features, positions, species, counts, neighbors, waves, radial_in, radial_out,
    species_gain, mix_weight, readout, charge_weight, ref_energy,
):
    nx, ny, nz = sizes
    slots = positions.shape[-1]
    norm = (waves.shape[1] * nx * ny * nz * slots) ** -0.5
    args = (
        neighbors.reshape(12, 1, slots), positions.reshape(3, 1, slots), counts.reshape(1, 1),
        features.reshape(slots, -1), species.reshape(1, slots), waves, radial_in, radial_out, species_gain,
        mix_weight, readout.reshape(1, -1), charge_weight.T, ref_energy.reshape(1, -1),
    )
    site, forces = direct(sizes, norm, *args)
    crowded = jnp.isnan(site[0, 0])
    site, forces = lax.cond(
        crowded, lambda s, f, *a: tuple(general(sizes, norm, *a)), lambda s, f, *a: (s, f), site, forces, *args
    )
    return site.reshape(1, 1, 1, slots), forces.reshape(1, 1, 1, 3, slots)


def solution(mesh):
    sizes = tuple(mesh.shape[n] for n in AXES)
    cell = P("gx", "gy", "gz")
    placed = (cell,) * 5 + (P(),) * 8
    return jax.shard_map(
        functools.partial(per_device, sizes),
        mesh=mesh,
        in_specs=placed,
        out_specs=(cell, cell),
        check_vma=False,
    )
```

```python
import functools
import math

import jax
import jax.numpy as jnp
from jax import lax
from jax.experimental import pallas as pl
from jax.experimental.pallas import tpu as pltpu
from jax.sharding import PartitionSpec as P

TICKS = 1024
AXES = ("gx", "gy", "gz")
MESH = pl.DeviceIdType.MESH
HIGH = lax.Precision.HIGHEST
OFFS = [(a - 1, b - 1, c - 1) for a in range(3) for b in range(3) for c in range(3)]
F32 = jnp.float32
BF16 = jnp.bfloat16
SLOT = 96
GROUP = 9
LOG2E = math.log2(math.e)
FAR = -1.0e6
LIST = jnp.int16


def iota(shape, dim):
    return lax.broadcasted_iota(jnp.int32, shape, dim)


def dot(a, b, contract=((1,), (0,)), precision=None):
    return lax.dot_general(a, b, (contract, ((), ())), precision=precision, preferred_element_type=F32)


NT = ((1,), (1,))
TN = ((0,), (0,))


def split(x):
    hi = x.astype(BF16)
    return hi, (x - hi.astype(F32)).astype(BF16)


def at_offset(sizes, d):
    return tuple(lax.rem(lax.axis_index(n) + (s + o), s) if o else lax.axis_index(n) for n, s, o in zip(AXES, sizes, d))


def in_plane(sizes, d):
    dx, flip, dz = d
    x, y, z = at_offset(sizes, (dx, 0, dz))
    return x, y + 1 - 2 * lax.rem(y, 2) if flip else y, z


def greet(devices):
    barrier = pltpu.get_barrier_semaphore()
    for device in devices:
        pl.semaphore_signal(barrier, inc=1, device_id=device, device_id_type=MESH)
    return lambda: pl.semaphore_wait(barrier, len(devices))


def send(src, dst, ssem, rsem, device):
    c = pltpu.make_async_remote_copy(
        src_ref=src, dst_ref=dst, send_sem=ssem, recv_sem=rsem, device_id=device, device_id_type=MESH
    )
    c.start()
    return c


LEVEL = [i for i, d in enumerate(OFFS) if d[0] == 0]
APART = [i for i, d in enumerate(OFFS) if d[0] != 0]
NEAR = [(i, OFFS[i]) for i in LEVEL + APART if i != 13]


SIDE = 128


def rows_of(pos):
    loc = pos & (TICKS - 1)
    scale = 1.0 / TICKS
    return (loc & ~31).astype(F32) * scale, (loc & 31).astype(F32) * scale


def wide(x):
    return x.astype(jnp.int32)


def stack(parts):
    return parts[0] if len(parts) == 1 else jnp.concatenate(parts, axis=0)


def find(blks, ranks, base):
    slot = iota((SLOT, 128), 0).astype(F32) + base
    accs = []
    for blk, rank in zip(blks, ranks):
        code = ((blk & 127) + 1).astype(F32)
        acc = jnp.zeros((SLOT, 128), F32)
        for k in range(12):
            acc = jnp.where(rank[k : k + 1] == slot, code[k : k + 1], acc)
        accs.append(acc)
    picks_i = [jnp.where(acc > 0.0, 1.0, 0.0).astype(BF16) for acc in accs]
    named = dot(stack(accs).astype(BF16), jnp.ones((128, 128), BF16))
    lane = iota(named.shape, 1)
    return picks_i, jnp.where(named == (lane + 1).astype(F32), 1.0, 0.0).astype(BF16)


def distance(blks, offs, own, picks_i, pick_j):
    jhi, jlo = rows_of(own)
    pieces = []
    for n, (blk, off, pick_i) in enumerate(zip(blks, offs, picks_i)):
        ihi, ilo = rows_of(blk[12:15])
        shift = jnp.concatenate([jnp.full((1, 128), o, F32) for o in off], axis=0)
        fill = jnp.zeros((2, 128), F32)
        left = jnp.concatenate([-ihi - shift, -ilo, fill], axis=0)
        right = jnp.concatenate([jhi, jlo, fill], axis=0)
        w = jnp.concatenate([left, right], axis=1).astype(BF16)
        both = jnp.concatenate([pick_i, pick_j[SLOT * n : SLOT * (n + 1)]], axis=1)
        pieces.append(dot(both, w, NT).astype(BF16))
    to_lanes = iota((8, 384), 1) >> 7
    spread = jnp.where((to_lanes == iota((8, 384), 0)) | (to_lanes + 3 == iota((8, 384), 0)), 1.0, 0.0).astype(BF16)
    return dot(stack(pieces), spread)


def basis(disp):
    dx, dy, dz = disp[:, 0:128], disp[:, 128:256], disp[:, 256:384]
    r2 = dx * dx + dy * dy + dz * dz
    s2 = r2 + 0.25
    inv = lax.rsqrt(s2)
    rs = s2 * inv
    inv1 = 1.0 / (1.0 + r2)
    t = rs - (0.25 + 0.5 * lax.rem(iota((1, 128), 1), 8).astype(F32))
    b = jnp.exp2((t * (-2.0 * LOG2E)) * t) * inv1
    return (dx * inv, dy * inv, dz * inv), inv, rs, inv1, t, b


def sigmoid(z):
    return 0.5 * jnp.tanh(0.5 * z) + 0.5


def gains(pick_j, gtab):
    g = dot(pick_j, gtab)
    return g[:, 0:128] + g[:, 128:256]


def forward(disp, pick_j, feats, gtab, mst, wz, wr):
    (ux, uy, uz), _, _, _, _, b = basis(disp)
    z = dot(b.astype(BF16), wz[:, 0:128])
    rad = dot((z * sigmoid(z)).astype(BF16), wr[:, 0:128]) * gains(pick_j, gtab)
    h = dot(pick_j, feats)
    x = h[:, 0:128] + ux * h[:, 128:256] + uy * h[:, 256:384] + uz * h[:, 384:512]
    return dot((rad * x).astype(BF16), mst[0:128, 0:128])


def slopes(disp, pick_j, feats, gtab, mst, wz, wr):
    lane = iota((disp.shape[0], 128), 1)
    (ux, uy, uz), inv, rs, inv1, t, b = basis(disp)
    b = jnp.where(lane < 8, b, b * (-4.0 * t - 2.0 * rs * inv1)).astype(BF16)
    zz = dot(b, wz)
    z, zp = zz[:, 0:128], zz[:, 128:256]
    sig = sigmoid(z)
    silu = z * sig
    hid = jnp.where(lane < 64, silu, (sig + silu * (1.0 - sig)) * zp).astype(BF16)
    rr = dot(hid, wr)
    g = gains(pick_j, gtab)
    rad = rr[:, 0:128] * g
    radp = rr[:, 128:256] * g
    h = dot(pick_j, feats)
    q = []
    for r in (rad, radp):
        for d in range(2):
            x = [(r * h[:, 128 * e : 128 * (e + 1)]).astype(BF16) for e in (2 * d, 2 * d + 1)]
            t = dot(jnp.concatenate(x, axis=1), mst)
            q += [t[:, 0:128], t[:, 128:256]]
    along = ux * q[1] + uy * q[2] + uz * q[3]
    w = q[4] + ux * q[5] + uy * q[6] + uz * q[7] - along * inv
    part = (lane >> 4) & 3
    ua = jnp.where(part == 0, ux, jnp.where(part == 1, uy, uz))
    qa = jnp.where(part == 0, q[1], jnp.where(part == 1, q[2], q[3]))
    return jnp.where(part == 3, q[0] + along, ua * w + qa * inv)


def edges(blk, rank, base, off, own, *tabs):
    picks_i, pick_j = find([blk], [rank], base)
    return picks_i[0], pick_j, slopes(distance([blk], [off], own, picks_i, pick_j), pick_j, *tabs)


def per_atom(pick_i, out):
    lane = iota((SLOT, 128), 1)
    hi = out.astype(BF16)
    mixed = jnp.where(lane < 64, hi.astype(F32), out - hi.astype(F32)).astype(BF16)
    s = dot(mixed, pick_i, TN)
    return s[0:64] + s[64:128]


def cell_offset(a):
    if isinstance(a, int):
        return tuple(float(o) for o in OFFS[a])
    return ((a // 9 - 1).astype(F32), (lax.rem(a // 3, 3) - 1).astype(F32), (lax.rem(a, 3) - 1).astype(F32))


def tables(feats, species, rin, rout, gain, mix, readout, cw, ref_energy, gtab, mst, wz, wr, base9, refrow):
    neigh = 12
    lane = iota((8, SIDE), 1)
    sel8 = jnp.where(lax.rem(lane, 16) == iota((8, SIDE), 0), 1.0, 0.0)
    sel1 = jnp.where(lax.rem(iota((1, SIDE), 1), 16) == 8, 1.0, 0.0)
    rc = dot(cw[...], sel8, TN, HIGH) + dot(readout[...], sel1, TN, HIGH)
    mb = (dot(mix[...].astype(F32), rc, precision=HIGH) * (neigh ** -0.5)).astype(BF16)
    mst[0:128, 0:128] = mb
    mst[0:128, 128:256] = jnp.zeros_like(mb)
    mst[128:256, 0:128] = jnp.zeros_like(mb)
    mst[128:256, 128:256] = mb
    base9[...] = dot(rc, feats[:, 0:128].astype(F32), ((0,), (1,)), HIGH)[0:16]
    kinds = gain.shape[0]
    onehot = jnp.where(iota((kinds, SIDE), 0) == species[...], 1.0, 0.0)
    ghi, glo = split(dot(onehot, gain[...], TN, HIGH))
    gtab[:, 0:128] = ghi
    gtab[:, 128:256] = glo
    refrow[...] = jnp.broadcast_to(dot(ref_energy[...], onehot, precision=HIGH), refrow.shape)
    r = rin[...]
    h = rin.shape[1]
    dup = jnp.where(lax.rem(iota((h, 128), 1), h) == iota((h, 128), 0), 1.0, 0.0).astype(BF16)
    upper = jnp.where(iota((h, 128), 1) - h == iota((h, 128), 0), 1.0, 0.0).astype(BF16)
    rows_a = jnp.where(iota((128, 8), 0) == iota((128, 8), 1), 1.0, 0.0).astype(BF16)
    rows_b = jnp.where(iota((128, 8), 0) - 8 == iota((128, 8), 1), 1.0, 0.0).astype(BF16)
    wz[:, 0:128] = dot(dot(rows_a, r).astype(BF16), dup).astype(BF16)
    wz[:, 128:256] = dot(dot(rows_b, r).astype(BF16), upper).astype(BF16)
    ro = rout[...]
    none = jnp.zeros_like(ro)
    wr[0:64, 0:128] = ro
    wr[64:128, 0:128] = none
    wr[0:64, 128:256] = none
    wr[64:128, 128:256] = ro


def rank_edges(lists, ranks, mask, cells):
    lane = iota((16, 128), 1)
    row = iota((16, 128), 0)
    many = len(cells)
    for n, a in enumerate(cells):
        blk = wide(lists[a])
        keep = ((blk >> 7) == 26 - a) & (lane < blk[15:16]) & (row < 12)
        mask[16 * n : 16 * n + 16] = jnp.where(keep, 1.0, 0.0)
    m = mask[0 : 16 * many].astype(BF16)
    tri = jnp.where(iota((128, 128), 0) <= iota((128, 128), 1), 1.0, 0.0).astype(BF16)
    both = dot(m, jnp.concatenate([tri, jnp.ones((128, 128), BF16)], axis=1))
    lower = jnp.where(iota((16, 16), 0) > iota((16, 16), 1), 1.0, 0.0).astype(BF16)
    totals = jnp.concatenate([both[16 * n : 16 * n + 16, 128:256] for n in range(many)], axis=1).astype(BF16)
    start = dot(lower, totals)
    peak = start[12:13, 0:128]
    for n, a in enumerate(cells):
        s = start[:, 128 * n : 128 * n + 128]
        peak = jnp.maximum(peak, s[12:13])
        r = both[16 * n : 16 * n + 16, 0:128] + s - 1.0
        ranks[a] = jnp.where(mask[16 * n : 16 * n + 16] > 0.0, r, FAR)
    return peak


def wave_tables(sizes, norm, waves, pos, wrow):
    waves_f = waves[...].astype(F32)
    kvec = [waves_f[d : d + 1] * (2.0 * math.pi / sizes[d]) for d in range(3)]
    ksq = kvec[0] * kvec[0] + kvec[1] * kvec[1] + kvec[2] * kvec[2]
    wrow[0:1] = 2.0 * (8.0 * jnp.exp(ksq * (-1.0 / 64.0)) / (8.0 + ksq) * norm)
    fields = []
    for d in range(3):
        wrow[1 + d : 2 + d] = kvec[d]
        length = float(sizes[d] * TICKS)
        p = pos[d : d + 1]
        fields.append(((p >> 7).astype(F32), waves_f[d : d + 1] * (128.0 / length)))
        fields.append(((p & 127).astype(F32), waves_f[d : d + 1] * (1.0 / length)))
    zero_i = jnp.zeros((2, 128), F32)
    zero_k = jnp.zeros((2, waves_f.shape[1]), F32)
    wrow[8:16] = jnp.concatenate([f[1] for f in fields] + [zero_k], axis=0)
    return jnp.concatenate([f[0] for f in fields] + [zero_i], axis=0).astype(BF16)


def phases(pos8, wrow, cos_h, cos_l, sin_h, sin_l):
    def phase(bi, carry):
        at = pl.ds(pl.multiple_of(bi * 128, 128), 128)
        turn = dot(pos8, wrow[8:16, at].astype(BF16), TN)
        quarter = jnp.floor(turn * 4.0 + 0.5)
        x = (turn - quarter * 0.25) * (2.0 * math.pi)
        qi = quarter.astype(jnp.int32)
        xx = x * x
        s = x * (1.0 + xx * (-1.0 / 6 + xx * (1.0 / 120 + xx * (-1.0 / 5040 + xx * (1.0 / 362880)))))
        c = 1.0 + xx * (-0.5 + xx * (1.0 / 24 + xx * (-1.0 / 720 + xx * (1.0 / 40320))))
        odd = (qi & 1) == 1
        cv = jnp.where(odd, s, c)
        sv = jnp.where(odd, c, s)
        cv = jnp.where(((qi + 1) & 2) == 2, -cv, cv)
        sv = jnp.where((qi & 2) == 2, -sv, sv)
        hi, lo = split(cv)
        cos_h[:, at] = hi
        cos_l[:, at] = lo
        hi, lo = split(sv)
        sin_h[:, at] = hi
        sin_l[:, at] = lo
        return carry

    lax.fori_loop(0, wrow.shape[1] // 128, phase, 0)


def peers(sizes):
    nx, ny, nz = sizes
    plane = [(dx, flip, dz) for dx in range(nx) for flip in range(2) for dz in range(nz)][1:]
    line = [(0, dy, 0) for dy in range(2, ny, 2)]
    near = [d for _, d in NEAR]
    known = [((d[0] + nx) % nx, abs(d[1]), (d[2] + nz) % nz) for d in near]
    whom = [at_offset(sizes, d) for d in near + line] + [in_plane(sizes, d) for d in plane if d not in known]
    return plane, line, whom


def reciprocal(sizes, poison, first, sums_t, sums_j, base9, pack, refrow, pots, wrow, trig, bufs, sems, meanwhile=lambda n: None):
    nx, ny, nz = sizes
    plane, line, _ = peers(sizes)
    cos_h, cos_l, sin_h, sin_l = trig
    got_t, got_j, part, got_rs, block, got_ar, got_ag, lhs, pot_s = bufs
    _, _, sj, rj, srs, rrs, sar, rar, sag, rag, sp, rp = sems
    blocks = wrow.shape[1] // 128
    live = jnp.where(iota((1, 128), 1) < pack[15:16], 1.0, 0.0)
    total = base9[...] + sums_t[13].astype(F32)
    meanwhile(0)
    for c in first:
        c.wait()
    for i, _ in NEAR:
        total = total + got_t[i].astype(F32)
    q = total[0:8] * live
    qhi, qlo = split(q)
    q16 = jnp.concatenate([qhi, qlo], axis=0)
    for half, high, low in ((0, cos_h, cos_l), (1, sin_h, sin_l)):
        s = dot(q16, high[...])
        s = s[0:8] + s[8:16] + dot(q16, low[...])[0:8]
        for bi in range(blocks):
            part[2 * bi + half] = s[:, 128 * bi : 128 * bi + 128] + poison
    ix, iy, iz = [lax.axis_index(n) for n in AXES]
    low_x = lax.rem(iy, 2)
    me = (ix * 2 + low_x) * nz + iz
    rs = []
    for n, d in enumerate(plane):
        to = (lax.rem(ix + d[0], nx) * 2 + (1 - low_x if d[1] else low_x)) * nz + lax.rem(iz + d[2], nz)
        rs.append(send(part.at[to], got_rs.at[n], srs.at[n], rrs.at[n], in_plane(sizes, d)))
    meanwhile(1)
    acc = part[me]
    for n, c in enumerate(rs):
        c.wait()
        acc = acc + got_rs[n]
    block[0] = acc
    ar = [send(block.at[0], got_ar.at[n], sar.at[n], rar.at[n], at_offset(sizes, d)) for n, d in enumerate(line)]
    meanwhile(2)
    for n, c in enumerate(ar):
        c.wait()
        acc = acc + got_ar[n]
    got_ag[me] = acc
    ag = [send(got_ag.at[me], got_ag.at[me], sag.at[n], rag.at[n], in_plane(sizes, d)) for n, d in enumerate(plane)]
    second = [send(sums_j.at[i], got_j.at[26 - i], sj.at[i], rj.at[i], at_offset(sizes, d)) for i, d in NEAR]
    for c in ag:
        c.wait()
    for bi in range(blocks):
        at = slice(128 * bi, 128 * bi + 128)
        weight = wrow[0:1, at]
        pre = got_ag[2 * bi] * weight
        pim = got_ag[2 * bi + 1] * weight
        kx, ky, kz = wrow[1:2, at], wrow[2:3, at], wrow[3:4, at]
        lc = jnp.concatenate([pre, kx * pim, ky * pim, kz * pim], axis=0)
        ls = jnp.concatenate([pim, -kx * pre, -ky * pre, -kz * pre], axis=0)
        hi, lo = split(lc)
        lhs[0:32, at] = hi
        lhs[32:64, at] = lo
        hi, lo = split(ls)
        lhs[64:96, at] = hi
        lhs[96:128, at] = lo
    w = dot(lhs[0:64], cos_h[...], NT)
    v = dot(lhs[64:128], sin_h[...], NT)
    w = w[0:32] + w[32:64] + dot(lhs[0:32], cos_l[...], NT)
    w = w + v[0:32] + v[32:64] + dot(lhs[64:96], sin_l[...], NT)
    pot = w[0:8]
    flag = jnp.where(iota((8, 128), 0) == 0, live, 0.0)
    pot16 = jnp.concatenate([pot * live, flag], axis=0)
    pot_s[0] = pot16.astype(BF16)
    third = [send(pot_s.at[0], pots.at[26 - i], sp.at[i], rp.at[i], at_offset(sizes, d)) for i, d in NEAR]
    pots[13] = pot16.astype(BF16)
    js = sums_j[13].astype(F32)
    for c in second:
        c.wait()
    for i, _ in NEAR:
        js = js + got_j[i].astype(F32)
    rows = []
    for d in range(3):
        wave = jnp.sum(q * w[8 * d + 8 : 8 * d + 16], axis=0, keepdims=True)
        rows.append(wave - jnp.sum(pot16 * js[16 * d : 16 * d + 16], axis=0, keepdims=True))
    site = live * (total[8:9] + refrow[0:1] + 0.5 * jnp.sum(q * pot, axis=0, keepdims=True))
    mine = jnp.concatenate(rows + [site, live, live, live, live], axis=0)
    return mine, third


def hand_sums(sizes, sums_t, got_t, ssem, rsem, cells):
    return [
        send(sums_t.at[i], got_t.at[26 - i], ssem.at[i], rsem.at[i], at_offset(sizes, d)) for i, d in NEAR if i in cells
    ]


def pull_back(work, pots):
    prods = []
    for (pick_i, _, out), p in zip(work, pots):
        none = jnp.zeros((16, 128), BF16)
        prods.append(out * dot(pick_i, jnp.concatenate([p, p, p, none, p, p, p, none], axis=0), NT))
    prod = stack(prods)
    hi = prod.astype(BF16)
    mixed = jnp.where(iota(prod.shape, 1) < 64, hi.astype(F32), prod - hi.astype(F32)).astype(BF16)
    return dot(mixed, stack([pick_j for _, pick_j, _ in work]), TN)


def give(mine, t, site, forces):
    t = t[0:64] + t[64:128]
    for d in range(3):
        g = mine[d : d + 1] + jnp.sum(t[16 * d : 16 * d + 16], axis=0, keepdims=True)
        forces[d] = -g * mine[4:5]
    site[...] = mine[3:4]


def gather_pack(neighbors, positions, counts, pack, sem):
    copies = [pltpu.make_async_copy(neighbors.at[k], pack.at[pl.ds(k, 1)], sem.at[k]) for k in range(12)]
    copies += [pltpu.make_async_copy(positions.at[d], pack.at[pl.ds(12 + d, 1)], sem.at[12 + d]) for d in range(3)]
    for c in copies:
        c.start()
    pack[15:16] = jnp.full((1, 128), counts[0, 0], jnp.int32)
    return copies


def hand_out(sizes, pack, lists, ssem, rsem):
    copies = [send(pack, lists.at[26 - i], ssem.at[i], rsem.at[i], at_offset(sizes, d)) for i, d in NEAR]
    lists[13] = pack[...]
    return copies


def shorten(pack, short):
    row = iota((16, 128), 0)
    local = (row >= 12) & (row < 15)
    short[...] = jnp.where(local, pack[...] & (TICKS - 1), pack[...]).astype(LIST)


def whole_kernel(
    sizes, norm, neighbors, positions, counts, *rest,
):
    far, (site, forces), near = rest[:10], rest[10:12], rest[12:22]
    whole_steps(sizes, norm, neighbors, positions, counts, far, near, site, forces, *rest[22:])


def whole_steps(
    sizes, norm, neighbors, positions, counts, far, near, site, forces,
    osem, pack, short, lists, gtab, mst, wz, wr, base9, refrow, ranks, mask, picks_i, picks_j, outs, sums_t, sums_j, pots, wrow,
    cos_h, cos_l, sin_h, sin_l, got_t, got_j, part, got_rs, block, got_ar, got_ag, lhs, pot_s,
    psem, ls, lr, *sems,
):
    wait = greet(peers(sizes)[2])
    packed = gather_pack(neighbors, positions, counts, pack, psem)
    brought = [pltpu.make_async_copy(f, n, osem.at[i]) for i, (f, n) in enumerate(zip(far, near))]
    for c in brought:
        c.start()
    for c in brought:
        c.wait()
    feats, species, waves, rin, rout, gain, mix, readout, cw, ref_energy = near
    tables(feats, species, rin, rout, gain, mix, readout, cw, ref_energy, gtab, mst, wz, wr, base9, refrow)
    for c in packed:
        c.wait()
    shorten(pack, short)
    wait()
    out = hand_out(sizes, short, lists, ls, lr)
    own = pack[12:15]
    trig = (cos_h, cos_l, sin_h, sin_l)
    phases(wave_tables(sizes, norm, waves, own, wrow), wrow, *trig)
    tabs = (feats, gtab, mst, wz, wr)

    def first(cells):
        blks = [wide(lists[a]) for a in cells]
        found, pick_j = find(blks, [ranks[a] for a in cells], 0.0)
        disp = distance(blks, [cell_offset(a) for a in cells], own, found, pick_j)
        out = forward(disp, pick_j, *[t[...] for t in tabs])
        for n, a in enumerate(cells):
            rows = slice(SLOT * n, SLOT * n + SLOT)
            picks_i[a] = found[n]
            picks_j[a] = pick_j[rows]
            sums_t[a] = per_atom(found[n], out[rows])[0:16].astype(BF16)

    def later(gi):
        cells = [gi * GROUP + u for u in range(GROUP)]
        found = [picks_i[a] for a in cells]
        pick_j = stack([picks_j[a] for a in cells])
        disp = distance([wide(lists[a]) for a in cells], [cell_offset(a) for a in cells], own, found, pick_j)
        out = slopes(disp, pick_j, *[t[...] for t in tabs])
        for n, a in enumerate(cells):
            rows = slice(SLOT * n, SLOT * n + SLOT)
            outs[a] = out[rows]
            sums_j[a] = per_atom(found[n], out[rows])[0:48].astype(BF16)

    peak = jnp.zeros((1, 128), F32)
    sums = []
    for cells in (LEVEL, APART):
        here = [n for n, (i, _) in enumerate(NEAR) if i in cells]
        for n in here:
            out[n].wait()
        peak = jnp.maximum(peak, rank_edges(lists, ranks, mask, cells))
        first(cells)
        sums += hand_sums(sizes, sums_t, got_t, sems[0], sems[1], cells)
    poison = jnp.where(peak > float(SLOT), jnp.nan, 0.0)
    bufs = (got_t, got_j, part, got_rs, block, got_ar, got_ag, lhs, pot_s)
    mine, third = reciprocal(sizes, poison, sums, sums_t, sums_j, base9, pack, refrow, pots, wrow, trig, bufs, sems, later)
    total = jnp.zeros((128, 128), F32)
    for cells in (LEVEL, APART):
        for n, (i, _) in enumerate(NEAR):
            if i in cells:
                third[n].wait()
        total = total + pull_back([(picks_i[a], picks_j[a], outs[a]) for a in cells], [pots[a] for a in cells])
    give(mine, total, site, forces)


def spread_kernel(
    sizes, neighbors, positions, counts, feats, species, rin, rout, gain, mix, readout, cw, ref_energy,
    lists, pack_out, gtab, mst, wz, wr, base9, refrow, pack, short, psem, ssem, rsem,
):
    wait = greet([at_offset(sizes, d) for _, d in NEAR])
    packed = gather_pack(neighbors, positions, counts, pack, psem)
    tables(feats, species, rin, rout, gain, mix, readout, cw, ref_energy, gtab, mst, wz, wr, base9, refrow)
    for c in packed:
        c.wait()
    shorten(pack, short)
    wait()
    out = hand_out(sizes, short, lists, ssem, rsem)
    pack_out[...] = pack[...]
    for c in out:
        c.wait()


def each_piece(ranks, run):
    def cell(a, carry):
        pieces = (jnp.max(ranks[a]).astype(jnp.int32) + SLOT) // SLOT
        return lax.fori_loop(0, pieces, lambda c, carry: run(a, (c * SLOT).astype(F32), carry), carry)

    lax.fori_loop(0, 27, cell, 0)


def edge_kernel(lists, pack, feats, gtab, mst, wz, wr, sums_t, sums_j, mask, ranks, total_t, total_j):
    rank_edges(lists, ranks, mask, range(27))
    own = pack[12:15]
    total_t[...] = jnp.zeros_like(total_t)
    total_j[...] = jnp.zeros_like(total_j)

    def piece(a, base, carry):
        pick_i, _, out = edges(wide(lists[a]), ranks[a], base, cell_offset(a), own, feats[...], gtab[...], mst[...], wz[...], wr[...])
        s = per_atom(pick_i, out)
        total_j[a] += s[0:48]
        total_t[a] += s[48:64]
        return carry

    each_piece(ranks, piece)
    sums_t[...] = total_t[...].astype(BF16)
    sums_j[...] = total_j[...].astype(BF16)


def wave_kernel(
    sizes, norm, sums_t, sums_j, base9, pack, waves, refrow, pots, mine,
    wrow, cos_h, cos_l, sin_h, sin_l, got_t, got_j, part, got_rs, block, got_ar, got_ag, lhs, pot_s, *sems,
):
    wait = greet(peers(sizes)[2])
    trig = (cos_h, cos_l, sin_h, sin_l)
    phases(wave_tables(sizes, norm, waves, pack[12:15], wrow), wrow, *trig)
    wait()
    bufs = (got_t, got_j, part, got_rs, block, got_ar, got_ag, lhs, pot_s)
    sums = hand_sums(sizes, sums_t, got_t, sems[0], sems[1], LEVEL + APART)
    mine[...], third = reciprocal(sizes, 0.0, sums, sums_t, sums_j, base9, pack, refrow, pots, wrow, trig, bufs, sems)
    for c in third:
        c.wait()


def force_kernel(pots, mine, lists, pack, feats, gtab, mst, wz, wr, site, forces, mask, ranks, total):
    rank_edges(lists, ranks, mask, range(27))
    own = pack[12:15]
    total[...] = jnp.zeros_like(total)

    def piece(a, base, carry):
        work = edges(wide(lists[a]), ranks[a], base, cell_offset(a), own, feats[...], gtab[...], mst[...], wz[...], wr[...])
        total[...] += pull_back([work], [pots[a]])
        return carry

    each_piece(ranks, piece)
    give(mine[...], total[...], site, forces)


VMEM = pl.BlockSpec(memory_space=pltpu.VMEM)
SMEM = pl.BlockSpec(memory_space=pltpu.SMEM)
HBM = pl.BlockSpec(memory_space=pltpu.HBM)


def shape(dims, kind):
    return jax.ShapeDtypeStruct(dims, kind)


def wave_buffers(sizes, waves):
    nx, ny, nz = sizes
    planes, lines = 2 * nx * nz, ny // 2
    assert planes == 2 * waves // 128
    buf = pltpu.VMEM
    dma = pltpu.SemaphoreType.DMA
    trig = [buf((128, waves), BF16)] * 4
    rest = [
        buf((27, 16, 128), BF16), buf((27, 48, 128), BF16), buf((planes, 8, 128), F32), buf((planes - 1, 8, 128), F32),
        buf((1, 8, 128), F32), buf((lines - 1, 8, 128), F32), buf((planes, 8, 128), F32), buf((128, waves), BF16),
        buf((1, 16, 128), BF16),
    ]
    counts = (27, 27, 27, 27, planes - 1, planes - 1, lines - 1, lines - 1, planes - 1, planes - 1, 27, 27)
    return [buf((16, waves), F32)] + trig + rest, [dma((n,)) for n in counts]


TABLES = [
    ((128, 256), BF16), ((256, 256), BF16), ((128, 256), BF16), ((128, 256), BF16), ((16, 128), F32), ((8, 128), F32),
]
RANKS = [((27, 16, 128), F32), ((27 * 16, 128), F32)]
RESULT = [((1, 128), F32), ((3, 1, 128), F32)]


def general(sizes, norm, neighbors, positions, counts, feats, species, waves, *params):
    dma = pltpu.SemaphoreType.DMA
    lists, pack, gtab, mst, wz, wr, base9, refrow = pl.pallas_call(
        functools.partial(spread_kernel, sizes),
        out_shape=[shape((27, 16, 128), LIST), shape((16, 128), jnp.int32)] + [shape(*t) for t in TABLES],
        in_specs=[HBM, HBM, SMEM] + [VMEM] * 9,
        out_specs=[VMEM] * 8,
        scratch_shapes=[pltpu.VMEM((16, 128), jnp.int32), pltpu.VMEM((16, 128), LIST), dma((15,)), dma((27,)), dma((27,))],
        compiler_params=pltpu.CompilerParams(collective_id=1, has_side_effects=True),
        name="spread",
    )(neighbors, positions, counts, feats, species, *params)
    ranking = [pltpu.VMEM(*RANKS[1]), pltpu.VMEM(*RANKS[0])]
    sums_t, sums_j = pl.pallas_call(
        edge_kernel,
        out_shape=[shape((27, 16, 128), BF16), shape((27, 48, 128), BF16)],
        in_specs=[VMEM] * 7,
        out_specs=[VMEM] * 2,
        scratch_shapes=ranking + [pltpu.VMEM((27, 16, 128), F32), pltpu.VMEM((27, 48, 128), F32)],
        name="edges",
    )(lists, pack, feats, gtab, mst, wz, wr)
    bufs, sems = wave_buffers(sizes, waves.shape[1])
    pots, mine = pl.pallas_call(
        functools.partial(wave_kernel, sizes, norm),
        out_shape=[shape((27, 16, 128), BF16), shape((8, 128), F32)],
        in_specs=[VMEM] * 6,
        out_specs=[VMEM] * 2,
        scratch_shapes=bufs + sems,
        compiler_params=pltpu.CompilerParams(collective_id=2, has_side_effects=True),
        name="waves",
    )(sums_t, sums_j, base9, pack, waves, refrow)
    return pl.pallas_call(
        force_kernel,
        out_shape=[shape(*r) for r in RESULT],
        in_specs=[VMEM] * 9,
        out_specs=[VMEM] * 2,
        scratch_shapes=ranking + [pltpu.VMEM((128, 128), F32)],
        name="forces",
    )(pots, mine, lists, pack, feats, gtab, mst, wz, wr)


def direct(sizes, norm, neighbors, positions, counts, feats, species, waves, *params):
    dma = pltpu.SemaphoreType.DMA
    buf = pltpu.VMEM
    bufs, sems = wave_buffers(sizes, waves.shape[1])
    brought = (feats, species, waves) + params
    scratch = [buf(b.shape, b.dtype) for b in brought] + [dma((len(brought),))]
    scratch += [buf((16, 128), jnp.int32), buf((16, 128), LIST), buf((27, 16, 128), LIST)] + [buf(*t) for t in TABLES + RANKS]
    scratch += [buf((27, SLOT, 128), BF16), buf((27, SLOT, 128), BF16), buf((27, SLOT, 128), F32)]
    scratch += [buf((27, 16, 128), BF16), buf((27, 48, 128), BF16), buf((27, 16, 128), BF16)]
    return pl.pallas_call(
        functools.partial(whole_kernel, sizes, norm),
        out_shape=[shape(*r) for r in RESULT],
        in_specs=[HBM, HBM, SMEM] + [HBM] * 10,
        out_specs=[VMEM] * 2,
        scratch_shapes=scratch + bufs + [dma((15,)), dma((27,)), dma((27,))] + sems,
        compiler_params=pltpu.CompilerParams(collective_id=0, has_side_effects=True),
        name="whole",
    )(neighbors, positions, counts, feats, species, waves, *params)


def per_device(
    sizes, features, positions, species, counts, neighbors, waves, radial_in, radial_out,
    species_gain, mix_weight, readout, charge_weight, ref_energy,
):
    nx, ny, nz = sizes
    slots = positions.shape[-1]
    norm = (waves.shape[1] * nx * ny * nz * slots) ** -0.5
    args = (
        neighbors.reshape(12, 1, slots), positions.reshape(3, 1, slots), counts.reshape(1, 1),
        features.reshape(slots, -1), species.reshape(1, slots), waves, radial_in, radial_out, species_gain,
        mix_weight, readout.reshape(1, -1), charge_weight.T, ref_energy.reshape(1, -1),
    )
    site, forces = direct(sizes, norm, *args)
    crowded = jnp.isnan(site[0, 0])
    site, forces = lax.cond(
        crowded, lambda s, f, *a: tuple(general(sizes, norm, *a)), lambda s, f, *a: (s, f), site, forces, *args
    )
    return site.reshape(1, 1, 1, slots), forces.reshape(1, 1, 1, 3, slots)


def solution(mesh):
    sizes = tuple(mesh.shape[n] for n in AXES)
    cell = P("gx", "gy", "gz")
    placed = (cell,) * 5 + (P(),) * 8
    return jax.shard_map(
        functools.partial(per_device, sizes),
        mesh=mesh,
        in_specs=placed,
        out_specs=(cell, cell),
        check_vma=False,
    )
```

```python
import functools
import math

import jax
import jax.numpy as jnp
from jax import lax
from jax.experimental import pallas as pl
from jax.experimental.pallas import tpu as pltpu
from jax.sharding import PartitionSpec as P

TICKS = 1024
AXES = ("gx", "gy", "gz")
MESH = pl.DeviceIdType.MESH
HIGH = lax.Precision.HIGHEST
OFFS = [(a - 1, b - 1, c - 1) for a in range(3) for b in range(3) for c in range(3)]
F32 = jnp.float32
BF16 = jnp.bfloat16
SLOT = 96
GROUP = 9
LOG2E = math.log2(math.e)
FAR = -1.0e6
ALL_VMEM = 67_043_328
LIST = jnp.int16


def iota(shape, dim):
    return lax.broadcasted_iota(jnp.int32, shape, dim)


def dot(a, b, contract=((1,), (0,)), precision=None):
    return lax.dot_general(a, b, (contract, ((), ())), precision=precision, preferred_element_type=F32)


NT = ((1,), (1,))
TN = ((0,), (0,))


def split(x):
    hi = x.astype(BF16)
    return hi, (x - hi.astype(F32)).astype(BF16)


def at_offset(sizes, d):
    return tuple(lax.rem(lax.axis_index(n) + (s + o), s) if o else lax.axis_index(n) for n, s, o in zip(AXES, sizes, d))


def in_plane(sizes, d):
    dx, flip, dz = d
    x, y, z = at_offset(sizes, (dx, 0, dz))
    return x, y + 1 - 2 * lax.rem(y, 2) if flip else y, z


def greet(devices):
    barrier = pltpu.get_barrier_semaphore()
    for device in devices:
        pl.semaphore_signal(barrier, inc=1, device_id=device, device_id_type=MESH)
    return lambda: pl.semaphore_wait(barrier, len(devices))


def send(src, dst, ssem, rsem, device):
    c = pltpu.make_async_remote_copy(
        src_ref=src, dst_ref=dst, send_sem=ssem, recv_sem=rsem, device_id=device, device_id_type=MESH
    )
    c.start()
    return c


LEVEL = [i for i, d in enumerate(OFFS) if d[0] == 0]
APART = [i for i, d in enumerate(OFFS) if d[0] != 0]
NEAR = [(i, OFFS[i]) for i in LEVEL + APART if i != 13]
NEAR.sort(key=lambda n: (n[0] in APART, -abs(n[1][1]) - abs(n[1][2])))


SIDE = 128


def rows_of(pos):
    loc = pos & (TICKS - 1)
    scale = 1.0 / TICKS
    return (loc & ~31).astype(F32) * scale, (loc & 31).astype(F32) * scale


def wide(x):
    return x.astype(jnp.int32)


def stack(parts):
    return parts[0] if len(parts) == 1 else jnp.concatenate(parts, axis=0)


def find(blks, ranks, base):
    slot = iota((SLOT, 128), 0).astype(F32) + base
    accs = []
    for blk, rank in zip(blks, ranks):
        code = ((blk & 127) + 1).astype(F32)
        acc = jnp.zeros((SLOT, 128), F32)
        for k in range(12):
            acc = jnp.where(rank[k : k + 1] == slot, code[k : k + 1], acc)
        accs.append(acc)
    picks_i = [jnp.where(acc > 0.0, 1.0, 0.0).astype(BF16) for acc in accs]
    named = dot(stack(accs).astype(BF16), jnp.ones((128, 128), BF16))
    lane = iota(named.shape, 1)
    return picks_i, jnp.where(named == (lane + 1).astype(F32), 1.0, 0.0).astype(BF16)


def distance(blks, offs, own, picks_i, pick_j):
    jhi, jlo = rows_of(own)
    pieces = []
    for n, (blk, off, pick_i) in enumerate(zip(blks, offs, picks_i)):
        ihi, ilo = rows_of(blk[12:15])
        shift = jnp.concatenate([jnp.full((1, 128), o, F32) for o in off], axis=0)
        fill = jnp.zeros((2, 128), F32)
        left = jnp.concatenate([-ihi - shift, -ilo, fill], axis=0)
        right = jnp.concatenate([jhi, jlo, fill], axis=0)
        w = jnp.concatenate([left, right], axis=1).astype(BF16)
        both = jnp.concatenate([pick_i, pick_j[SLOT * n : SLOT * (n + 1)]], axis=1)
        pieces.append(dot(both, w, NT).astype(BF16))
    to_lanes = iota((8, 384), 1) >> 7
    spread = jnp.where((to_lanes == iota((8, 384), 0)) | (to_lanes + 3 == iota((8, 384), 0)), 1.0, 0.0).astype(BF16)
    return dot(stack(pieces), spread)


def basis(disp):
    dx, dy, dz = disp[:, 0:128], disp[:, 128:256], disp[:, 256:384]
    r2 = dx * dx + dy * dy + dz * dz
    s2 = r2 + 0.25
    inv = lax.rsqrt(s2)
    rs = s2 * inv
    inv1 = 1.0 / (1.0 + r2)
    t = rs - (0.25 + 0.5 * lax.rem(iota((1, 128), 1), 8).astype(F32))
    b = jnp.exp2((t * (-2.0 * LOG2E)) * t) * inv1
    return (dx * inv, dy * inv, dz * inv), inv, rs, inv1, t, b


def sigmoid(z):
    return 0.5 * jnp.tanh(0.5 * z) + 0.5


def gains(pick_j, gtab):
    g = dot(pick_j, gtab)
    return g[:, 0:128] + g[:, 128:256]


def forward(disp, pick_j, feats, gtab, mst, wz, wr):
    (ux, uy, uz), _, _, _, _, b = basis(disp)
    z = dot(b.astype(BF16), wz[:, 0:128])
    rad = dot((z * sigmoid(z)).astype(BF16), wr[:, 0:128]) * gains(pick_j, gtab)
    h = dot(pick_j, feats)
    x = h[:, 0:128] + ux * h[:, 128:256] + uy * h[:, 256:384] + uz * h[:, 384:512]
    return dot((rad * x).astype(BF16), mst[0:128, 0:128])


def slopes(disp, pick_j, feats, gtab, mst, wz, wr):
    lane = iota((disp.shape[0], 128), 1)
    (ux, uy, uz), inv, rs, inv1, t, b = basis(disp)
    b = jnp.where(lane < 8, b, b * (-4.0 * t - 2.0 * rs * inv1)).astype(BF16)
    zz = dot(b, wz)
    z, zp = zz[:, 0:128], zz[:, 128:256]
    sig = sigmoid(z)
    silu = z * sig
    hid = jnp.where(lane < 64, silu, (sig + silu * (1.0 - sig)) * zp).astype(BF16)
    rr = dot(hid, wr)
    g = gains(pick_j, gtab)
    rad = rr[:, 0:128] * g
    radp = rr[:, 128:256] * g
    h = dot(pick_j, feats)
    q = []
    for r in (rad, radp):
        for d in range(2):
            x = [(r * h[:, 128 * e : 128 * (e + 1)]).astype(BF16) for e in (2 * d, 2 * d + 1)]
            t = dot(jnp.concatenate(x, axis=1), mst)
            q += [t[:, 0:128], t[:, 128:256]]
    along = ux * q[1] + uy * q[2] + uz * q[3]
    w = q[4] + ux * q[5] + uy * q[6] + uz * q[7] - along * inv
    part = (lane >> 4) & 3
    ua = jnp.where(part == 0, ux, jnp.where(part == 1, uy, uz))
    qa = jnp.where(part == 0, q[1], jnp.where(part == 1, q[2], q[3]))
    return jnp.where(part == 3, q[0] + along, ua * w + qa * inv)


def edges(blk, rank, base, off, own, *tabs):
    picks_i, pick_j = find([blk], [rank], base)
    return picks_i[0], pick_j, slopes(distance([blk], [off], own, picks_i, pick_j), pick_j, *tabs)


def per_atom(pick_i, out):
    lane = iota((SLOT, 128), 1)
    hi = out.astype(BF16)
    mixed = jnp.where(lane < 64, hi.astype(F32), out - hi.astype(F32)).astype(BF16)
    s = dot(mixed, pick_i, TN)
    return s[0:64] + s[64:128]


def cell_offset(a):
    if isinstance(a, int):
        return tuple(float(o) for o in OFFS[a])
    return ((a // 9 - 1).astype(F32), (lax.rem(a // 3, 3) - 1).astype(F32), (lax.rem(a, 3) - 1).astype(F32))


def tables(feats, species, rin, rout, gain, mix, readout, cw, ref_energy, gtab, mst, wz, wr, base9, refrow):
    neigh = 12
    lane = iota((8, SIDE), 1)
    sel8 = jnp.where(lax.rem(lane, 16) == iota((8, SIDE), 0), 1.0, 0.0)
    sel1 = jnp.where(lax.rem(iota((1, SIDE), 1), 16) == 8, 1.0, 0.0)
    rc = dot(cw[...], sel8, TN, HIGH) + dot(readout[...], sel1, TN, HIGH)
    mb = (dot(mix[...].astype(F32), rc, precision=HIGH) * (neigh ** -0.5)).astype(BF16)
    mst[0:128, 0:128] = mb
    mst[0:128, 128:256] = jnp.zeros_like(mb)
    mst[128:256, 0:128] = jnp.zeros_like(mb)
    mst[128:256, 128:256] = mb
    base9[...] = dot(rc, feats[:, 0:128].astype(F32), ((0,), (1,)), HIGH)[0:16]
    kinds = gain.shape[0]
    onehot = jnp.where(iota((kinds, SIDE), 0) == species[...], 1.0, 0.0)
    ghi, glo = split(dot(onehot, gain[...], TN, HIGH))
    gtab[:, 0:128] = ghi
    gtab[:, 128:256] = glo
    refrow[...] = jnp.broadcast_to(dot(ref_energy[...], onehot, precision=HIGH), refrow.shape)
    r = rin[...]
    h = rin.shape[1]
    dup = jnp.where(lax.rem(iota((h, 128), 1), h) == iota((h, 128), 0), 1.0, 0.0).astype(BF16)
    upper = jnp.where(iota((h, 128), 1) - h == iota((h, 128), 0), 1.0, 0.0).astype(BF16)
    rows_a = jnp.where(iota((128, 8), 0) == iota((128, 8), 1), 1.0, 0.0).astype(BF16)
    rows_b = jnp.where(iota((128, 8), 0) - 8 == iota((128, 8), 1), 1.0, 0.0).astype(BF16)
    wz[:, 0:128] = dot(dot(rows_a, r).astype(BF16), dup).astype(BF16)
    wz[:, 128:256] = dot(dot(rows_b, r).astype(BF16), upper).astype(BF16)
    ro = rout[...]
    none = jnp.zeros_like(ro)
    wr[0:64, 0:128] = ro
    wr[64:128, 0:128] = none
    wr[0:64, 128:256] = none
    wr[64:128, 128:256] = ro


def rank_edges(lists, ranks, mask, cells):
    lane = iota((16, 128), 1)
    row = iota((16, 128), 0)
    many = len(cells)
    for n, a in enumerate(cells):
        blk = wide(lists[a])
        keep = ((blk >> 7) == 26 - a) & (lane < blk[15:16]) & (row < 12)
        mask[16 * n : 16 * n + 16] = jnp.where(keep, 1.0, 0.0)
    m = mask[0 : 16 * many].astype(BF16)
    tri = jnp.where(iota((128, 128), 0) <= iota((128, 128), 1), 1.0, 0.0).astype(BF16)
    both = dot(m, jnp.concatenate([tri, jnp.ones((128, 128), BF16)], axis=1))
    lower = jnp.where(iota((16, 16), 0) > iota((16, 16), 1), 1.0, 0.0).astype(BF16)
    totals = jnp.concatenate([both[16 * n : 16 * n + 16, 128:256] for n in range(many)], axis=1).astype(BF16)
    start = dot(lower, totals)
    peak = start[12:13, 0:128]
    for n, a in enumerate(cells):
        s = start[:, 128 * n : 128 * n + 128]
        peak = jnp.maximum(peak, s[12:13])
        r = both[16 * n : 16 * n + 16, 0:128] + s - 1.0
        ranks[a] = jnp.where(mask[16 * n : 16 * n + 16] > 0.0, r, FAR)
    return peak


def wave_tables(sizes, norm, waves, pos, wrow):
    waves_f = waves[...].astype(F32)
    kvec = [waves_f[d : d + 1] * (2.0 * math.pi / sizes[d]) for d in range(3)]
    ksq = kvec[0] * kvec[0] + kvec[1] * kvec[1] + kvec[2] * kvec[2]
    wrow[0:1] = 2.0 * (8.0 * jnp.exp(ksq * (-1.0 / 64.0)) / (8.0 + ksq) * norm)
    fields = []
    for d in range(3):
        wrow[1 + d : 2 + d] = kvec[d]
        length = float(sizes[d] * TICKS)
        p = pos[d : d + 1]
        fields.append(((p >> 7).astype(F32), waves_f[d : d + 1] * (128.0 / length)))
        fields.append(((p & 127).astype(F32), waves_f[d : d + 1] * (1.0 / length)))
    zero_i = jnp.zeros((2, 128), F32)
    zero_k = jnp.zeros((2, waves_f.shape[1]), F32)
    wrow[8:16] = jnp.concatenate([f[1] for f in fields] + [zero_k], axis=0)
    return jnp.concatenate([f[0] for f in fields] + [zero_i], axis=0).astype(BF16)


def phases(pos8, wrow, cos_h, cos_l, sin_h, sin_l):
    def phase(bi, carry):
        at = pl.ds(pl.multiple_of(bi * 128, 128), 128)
        turn = dot(pos8, wrow[8:16, at].astype(BF16), TN)
        quarter = jnp.floor(turn * 4.0 + 0.5)
        x = (turn - quarter * 0.25) * (2.0 * math.pi)
        qi = quarter.astype(jnp.int32)
        xx = x * x
        s = x * (1.0 + xx * (-1.0 / 6 + xx * (1.0 / 120 + xx * (-1.0 / 5040 + xx * (1.0 / 362880)))))
        c = 1.0 + xx * (-0.5 + xx * (1.0 / 24 + xx * (-1.0 / 720 + xx * (1.0 / 40320))))
        odd = (qi & 1) == 1
        cv = jnp.where(odd, s, c)
        sv = jnp.where(odd, c, s)
        cv = jnp.where(((qi + 1) & 2) == 2, -cv, cv)
        sv = jnp.where((qi & 2) == 2, -sv, sv)
        hi, lo = split(cv)
        cos_h[:, at] = hi
        cos_l[:, at] = lo
        hi, lo = split(sv)
        sin_h[:, at] = hi
        sin_l[:, at] = lo
        return carry

    lax.fori_loop(0, wrow.shape[1] // 128, phase, 0)


def peers(sizes):
    nx, ny, nz = sizes
    plane = [(dx, flip, dz) for dx in range(nx) for flip in range(2) for dz in range(nz)][1:]
    plane.sort(key=lambda d: -min(d[0], nx - d[0]) - d[1] - min(d[2], nz - d[2]))
    line = sorted([(0, dy, 0) for dy in range(2, ny, 2)], key=lambda d: -min(d[1], ny - d[1]))
    near = [d for _, d in NEAR]
    known = [((d[0] + nx) % nx, abs(d[1]), (d[2] + nz) % nz) for d in near]
    whom = [at_offset(sizes, d) for d in line] + [in_plane(sizes, d) for d in plane if d not in known]
    whom += [at_offset(sizes, d) for d in near[::-1]]
    return plane, line, whom


def reciprocal(sizes, poison, first, sums_t, sums_j, base9, pack, refrow, pots, wrow, trig, bufs, sems, meanwhile=lambda n: None):
    nx, ny, nz = sizes
    plane, line, _ = peers(sizes)
    cos_h, cos_l, sin_h, sin_l = trig
    got_t, got_j, part, got_rs, block, got_ar, got_ag, lhs, pot_s = bufs
    _, _, sj, rj, srs, rrs, sar, rar, sag, rag, sp, rp = sems
    blocks = wrow.shape[1] // 128
    live = jnp.where(iota((1, 128), 1) < pack[15:16], 1.0, 0.0)
    total = base9[...] + sums_t[13].astype(F32)
    meanwhile(0)
    for c in first:
        c.wait()
    for i, _ in NEAR:
        total = total + got_t[i].astype(F32)
    q = total[0:8] * live
    qhi, qlo = split(q)
    q16 = jnp.concatenate([qhi, qlo], axis=0)
    for half, high, low in ((0, cos_h, cos_l), (1, sin_h, sin_l)):
        s = dot(q16, high[...])
        s = s[0:8] + s[8:16] + dot(q16, low[...])[0:8]
        for bi in range(blocks):
            part[2 * bi + half] = s[:, 128 * bi : 128 * bi + 128] + poison
    ix, iy, iz = [lax.axis_index(n) for n in AXES]
    low_x = lax.rem(iy, 2)
    me = (ix * 2 + low_x) * nz + iz
    rs = []
    for n, d in enumerate(plane):
        to = (lax.rem(ix + d[0], nx) * 2 + (1 - low_x if d[1] else low_x)) * nz + lax.rem(iz + d[2], nz)
        rs.append(send(part.at[to], got_rs.at[n], srs.at[n], rrs.at[n], in_plane(sizes, d)))
    meanwhile(1)
    acc = part[me]
    for n, c in enumerate(rs):
        c.wait()
        acc = acc + got_rs[n]
    block[0] = acc
    ar = [send(block.at[0], got_ar.at[n], sar.at[n], rar.at[n], at_offset(sizes, d)) for n, d in enumerate(line)]
    meanwhile(2)
    for n, c in enumerate(ar):
        c.wait()
        acc = acc + got_ar[n]
    got_ag[me] = acc
    ag = [send(got_ag.at[me], got_ag.at[me], sag.at[n], rag.at[n], in_plane(sizes, d)) for n, d in enumerate(plane)]
    second = [send(sums_j.at[i], got_j.at[26 - i], sj.at[i], rj.at[i], at_offset(sizes, d)) for i, d in NEAR]
    for c in ag:
        c.wait()
    for bi in range(blocks):
        at = slice(128 * bi, 128 * bi + 128)
        weight = wrow[0:1, at]
        pre = got_ag[2 * bi] * weight
        pim = got_ag[2 * bi + 1] * weight
        kx, ky, kz = wrow[1:2, at], wrow[2:3, at], wrow[3:4, at]
        lc = jnp.concatenate([pre, kx * pim, ky * pim, kz * pim], axis=0)
        ls = jnp.concatenate([pim, -kx * pre, -ky * pre, -kz * pre], axis=0)
        hi, lo = split(lc)
        lhs[0:32, at] = hi
        lhs[32:64, at] = lo
        hi, lo = split(ls)
        lhs[64:96, at] = hi
        lhs[96:128, at] = lo
    w = dot(lhs[0:64], cos_h[...], NT)
    v = dot(lhs[64:128], sin_h[...], NT)
    w = w[0:32] + w[32:64] + dot(lhs[0:32], cos_l[...], NT)
    w = w + v[0:32] + v[32:64] + dot(lhs[64:96], sin_l[...], NT)
    pot = w[0:8]
    flag = jnp.where(iota((8, 128), 0) == 0, live, 0.0)
    pot16 = jnp.concatenate([pot * live, flag], axis=0)
    pot_s[0] = pot16.astype(BF16)
    third = [send(pot_s.at[0], pots.at[26 - i], sp.at[i], rp.at[i], at_offset(sizes, d)) for i, d in NEAR]
    pots[13] = pot16.astype(BF16)
    js = sums_j[13].astype(F32)
    for c in second:
        c.wait()
    for i, _ in NEAR:
        js = js + got_j[i].astype(F32)
    rows = []
    for d in range(3):
        wave = jnp.sum(q * w[8 * d + 8 : 8 * d + 16], axis=0, keepdims=True)
        rows.append(wave - jnp.sum(pot16 * js[16 * d : 16 * d + 16], axis=0, keepdims=True))
    site = live * (total[8:9] + refrow[0:1] + 0.5 * jnp.sum(q * pot, axis=0, keepdims=True))
    mine = jnp.concatenate(rows + [site, live, live, live, live], axis=0)
    return mine, third


def hand_sums(sizes, sums_t, got_t, ssem, rsem, cells):
    return [
        send(sums_t.at[i], got_t.at[26 - i], ssem.at[i], rsem.at[i], at_offset(sizes, d)) for i, d in NEAR if i in cells
    ]


def pull_back(work, pots):
    prods = []
    for (pick_i, _, out), p in zip(work, pots):
        none = jnp.zeros((16, 128), BF16)
        prods.append(out * dot(pick_i, jnp.concatenate([p, p, p, none, p, p, p, none], axis=0), NT))
    prod = stack(prods)
    hi = prod.astype(BF16)
    mixed = jnp.where(iota(prod.shape, 1) < 64, hi.astype(F32), prod - hi.astype(F32)).astype(BF16)
    return dot(mixed, stack([pick_j for _, pick_j, _ in work]), TN)


def give(mine, t, site, forces):
    t = t[0:64] + t[64:128]
    for d in range(3):
        g = mine[d : d + 1] + jnp.sum(t[16 * d : 16 * d + 16], axis=0, keepdims=True)
        forces[d] = -g * mine[4:5]
    site[...] = mine[3:4]


def gather_pack(neighbors, positions, counts, pack, sem):
    copies = [pltpu.make_async_copy(neighbors.at[k], pack.at[pl.ds(k, 1)], sem.at[k]) for k in range(12)]
    copies += [pltpu.make_async_copy(positions.at[d], pack.at[pl.ds(12 + d, 1)], sem.at[12 + d]) for d in range(3)]
    for c in copies:
        c.start()
    pack[15:16] = jnp.full((1, 128), counts[0, 0], jnp.int32)
    return copies


def hand_out(sizes, pack, lists, ssem, rsem):
    copies = [send(pack, lists.at[26 - i], ssem.at[i], rsem.at[i], at_offset(sizes, d)) for i, d in NEAR]
    lists[13] = pack[...]
    return copies


def shorten(pack, short):
    row = iota((16, 128), 0)
    local = (row >= 12) & (row < 15)
    short[...] = jnp.where(local, pack[...] & (TICKS - 1), pack[...]).astype(LIST)


def whole_kernel(
    sizes, norm, neighbors, positions, counts, *rest,
):
    far, (site, forces), near = rest[:10], rest[10:12], rest[12:22]
    whole_steps(sizes, norm, neighbors, positions, counts, far, near, site, forces, *rest[22:])


def whole_steps(
    sizes, norm, neighbors, positions, counts, far, near, site, forces,
    osem, pack, short, lists, gtab, mst, wz, wr, base9, refrow, ranks, mask, picks_i, picks_j, outs, sums_t, sums_j, pots, wrow,
    cos_h, cos_l, sin_h, sin_l, got_t, got_j, part, got_rs, block, got_ar, got_ag, lhs, pot_s,
    psem, ls, lr, *sems,
):
    wait = greet(peers(sizes)[2])
    packed = gather_pack(neighbors, positions, counts, pack, psem)
    brought = [pltpu.make_async_copy(f, n, osem.at[i]) for i, (f, n) in enumerate(zip(far, near))]
    for c in brought:
        c.start()
    for c in brought:
        c.wait()
    feats, species, waves, rin, rout, gain, mix, readout, cw, ref_energy = near
    tables(feats, species, rin, rout, gain, mix, readout, cw, ref_energy, gtab, mst, wz, wr, base9, refrow)
    for c in packed:
        c.wait()
    shorten(pack, short)
    wait()
    out = hand_out(sizes, short, lists, ls, lr)
    own = pack[12:15]
    trig = (cos_h, cos_l, sin_h, sin_l)
    phases(wave_tables(sizes, norm, waves, own, wrow), wrow, *trig)
    tabs = (feats, gtab, mst, wz, wr)

    def first(cells):
        blks = [wide(lists[a]) for a in cells]
        found, pick_j = find(blks, [ranks[a] for a in cells], 0.0)
        disp = distance(blks, [cell_offset(a) for a in cells], own, found, pick_j)
        out = forward(disp, pick_j, *[t[...] for t in tabs])
        for n, a in enumerate(cells):
            rows = slice(SLOT * n, SLOT * n + SLOT)
            picks_i[a] = found[n]
            picks_j[a] = pick_j[rows]
            sums_t[a] = per_atom(found[n], out[rows])[0:16].astype(BF16)

    def later(gi):
        cells = [gi * GROUP + u for u in range(GROUP)]
        found = [picks_i[a] for a in cells]
        pick_j = stack([picks_j[a] for a in cells])
        disp = distance([wide(lists[a]) for a in cells], [cell_offset(a) for a in cells], own, found, pick_j)
        out = slopes(disp, pick_j, *[t[...] for t in tabs])
        for n, a in enumerate(cells):
            rows = slice(SLOT * n, SLOT * n + SLOT)
            outs[a] = out[rows]
            sums_j[a] = per_atom(found[n], out[rows])[0:48].astype(BF16)

    peak = jnp.zeros((1, 128), F32)
    sums = []
    for cells in (LEVEL, APART):
        here = [n for n, (i, _) in enumerate(NEAR) if i in cells]
        for n in here:
            out[n].wait()
        peak = jnp.maximum(peak, rank_edges(lists, ranks, mask, cells))
        first(cells)
        sums += hand_sums(sizes, sums_t, got_t, sems[0], sems[1], cells)
    poison = jnp.where(peak > float(SLOT), jnp.nan, 0.0)
    bufs = (got_t, got_j, part, got_rs, block, got_ar, got_ag, lhs, pot_s)
    mine, third = reciprocal(sizes, poison, sums, sums_t, sums_j, base9, pack, refrow, pots, wrow, trig, bufs, sems, later)
    total = jnp.zeros((128, 128), F32)
    for cells in (LEVEL, APART):
        for n, (i, _) in enumerate(NEAR):
            if i in cells:
                third[n].wait()
        total = total + pull_back([(picks_i[a], picks_j[a], outs[a]) for a in cells], [pots[a] for a in cells])
    give(mine, total, site, forces)


def spread_kernel(
    sizes, neighbors, positions, counts, feats, species, rin, rout, gain, mix, readout, cw, ref_energy,
    lists, pack_out, gtab, mst, wz, wr, base9, refrow, pack, short, psem, ssem, rsem,
):
    wait = greet([at_offset(sizes, d) for _, d in NEAR])
    packed = gather_pack(neighbors, positions, counts, pack, psem)
    tables(feats, species, rin, rout, gain, mix, readout, cw, ref_energy, gtab, mst, wz, wr, base9, refrow)
    for c in packed:
        c.wait()
    shorten(pack, short)
    wait()
    out = hand_out(sizes, short, lists, ssem, rsem)
    pack_out[...] = pack[...]
    for c in out:
        c.wait()


def each_piece(ranks, run):
    def cell(a, carry):
        pieces = (jnp.max(ranks[a]).astype(jnp.int32) + SLOT) // SLOT
        return lax.fori_loop(0, pieces, lambda c, carry: run(a, (c * SLOT).astype(F32), carry), carry)

    lax.fori_loop(0, 27, cell, 0)


def edge_kernel(lists, pack, feats, gtab, mst, wz, wr, sums_t, sums_j, mask, ranks, total_t, total_j):
    rank_edges(lists, ranks, mask, range(27))
    own = pack[12:15]
    total_t[...] = jnp.zeros_like(total_t)
    total_j[...] = jnp.zeros_like(total_j)

    def piece(a, base, carry):
        pick_i, _, out = edges(wide(lists[a]), ranks[a], base, cell_offset(a), own, feats[...], gtab[...], mst[...], wz[...], wr[...])
        s = per_atom(pick_i, out)
        total_j[a] += s[0:48]
        total_t[a] += s[48:64]
        return carry

    each_piece(ranks, piece)
    sums_t[...] = total_t[...].astype(BF16)
    sums_j[...] = total_j[...].astype(BF16)


def wave_kernel(
    sizes, norm, sums_t, sums_j, base9, pack, waves, refrow, pots, mine,
    wrow, cos_h, cos_l, sin_h, sin_l, got_t, got_j, part, got_rs, block, got_ar, got_ag, lhs, pot_s, *sems,
):
    wait = greet(peers(sizes)[2])
    trig = (cos_h, cos_l, sin_h, sin_l)
    phases(wave_tables(sizes, norm, waves, pack[12:15], wrow), wrow, *trig)
    wait()
    bufs = (got_t, got_j, part, got_rs, block, got_ar, got_ag, lhs, pot_s)
    sums = hand_sums(sizes, sums_t, got_t, sems[0], sems[1], LEVEL + APART)
    mine[...], third = reciprocal(sizes, 0.0, sums, sums_t, sums_j, base9, pack, refrow, pots, wrow, trig, bufs, sems)
    for c in third:
        c.wait()


def force_kernel(pots, mine, lists, pack, feats, gtab, mst, wz, wr, site, forces, mask, ranks, total):
    rank_edges(lists, ranks, mask, range(27))
    own = pack[12:15]
    total[...] = jnp.zeros_like(total)

    def piece(a, base, carry):
        work = edges(wide(lists[a]), ranks[a], base, cell_offset(a), own, feats[...], gtab[...], mst[...], wz[...], wr[...])
        total[...] += pull_back([work], [pots[a]])
        return carry

    each_piece(ranks, piece)
    give(mine[...], total[...], site, forces)


VMEM = pl.BlockSpec(memory_space=pltpu.VMEM)
SMEM = pl.BlockSpec(memory_space=pltpu.SMEM)
HBM = pl.BlockSpec(memory_space=pltpu.HBM)


def shape(dims, kind):
    return jax.ShapeDtypeStruct(dims, kind)


def wave_buffers(sizes, waves):
    nx, ny, nz = sizes
    planes, lines = 2 * nx * nz, ny // 2
    assert planes == 2 * waves // 128
    buf = pltpu.VMEM
    dma = pltpu.SemaphoreType.DMA
    trig = [buf((128, waves), BF16)] * 4
    rest = [
        buf((27, 16, 128), BF16), buf((27, 48, 128), BF16), buf((planes, 8, 128), F32), buf((planes - 1, 8, 128), F32),
        buf((1, 8, 128), F32), buf((lines - 1, 8, 128), F32), buf((planes, 8, 128), F32), buf((128, waves), BF16),
        buf((1, 16, 128), BF16),
    ]
    counts = (27, 27, 27, 27, planes - 1, planes - 1, lines - 1, lines - 1, planes - 1, planes - 1, 27, 27)
    return [buf((16, waves), F32)] + trig + rest, [dma((n,)) for n in counts]


TABLES = [
    ((128, 256), BF16), ((256, 256), BF16), ((128, 256), BF16), ((128, 256), BF16), ((16, 128), F32), ((8, 128), F32),
]
RANKS = [((27, 16, 128), F32), ((27 * 16, 128), F32)]
RESULT = [((1, 128), F32), ((3, 1, 128), F32)]


def general(sizes, norm, neighbors, positions, counts, feats, species, waves, *params):
    dma = pltpu.SemaphoreType.DMA
    lists, pack, gtab, mst, wz, wr, base9, refrow = pl.pallas_call(
        functools.partial(spread_kernel, sizes),
        out_shape=[shape((27, 16, 128), LIST), shape((16, 128), jnp.int32)] + [shape(*t) for t in TABLES],
        in_specs=[HBM, HBM, SMEM] + [VMEM] * 9,
        out_specs=[VMEM] * 8,
        scratch_shapes=[pltpu.VMEM((16, 128), jnp.int32), pltpu.VMEM((16, 128), LIST), dma((15,)), dma((27,)), dma((27,))],
        compiler_params=pltpu.CompilerParams(collective_id=1, has_side_effects=True, vmem_limit_bytes=ALL_VMEM),
        name="spread",
    )(neighbors, positions, counts, feats, species, *params)
    ranking = [pltpu.VMEM(*RANKS[1]), pltpu.VMEM(*RANKS[0])]
    sums_t, sums_j = pl.pallas_call(
        edge_kernel,
        out_shape=[shape((27, 16, 128), BF16), shape((27, 48, 128), BF16)],
        in_specs=[VMEM] * 7,
        out_specs=[VMEM] * 2,
        scratch_shapes=ranking + [pltpu.VMEM((27, 16, 128), F32), pltpu.VMEM((27, 48, 128), F32)],
        compiler_params=pltpu.CompilerParams(vmem_limit_bytes=ALL_VMEM),
        name="edges",
    )(lists, pack, feats, gtab, mst, wz, wr)
    bufs, sems = wave_buffers(sizes, waves.shape[1])
    pots, mine = pl.pallas_call(
        functools.partial(wave_kernel, sizes, norm),
        out_shape=[shape((27, 16, 128), BF16), shape((8, 128), F32)],
        in_specs=[VMEM] * 6,
        out_specs=[VMEM] * 2,
        scratch_shapes=bufs + sems,
        compiler_params=pltpu.CompilerParams(collective_id=2, has_side_effects=True, vmem_limit_bytes=ALL_VMEM),
        name="waves",
    )(sums_t, sums_j, base9, pack, waves, refrow)
    return pl.pallas_call(
        force_kernel,
        out_shape=[shape(*r) for r in RESULT],
        in_specs=[VMEM] * 9,
        out_specs=[VMEM] * 2,
        scratch_shapes=ranking + [pltpu.VMEM((128, 128), F32)],
        name="forces",
    )(pots, mine, lists, pack, feats, gtab, mst, wz, wr)


def direct(sizes, norm, neighbors, positions, counts, feats, species, waves, *params):
    dma = pltpu.SemaphoreType.DMA
    buf = pltpu.VMEM
    bufs, sems = wave_buffers(sizes, waves.shape[1])
    brought = (feats, species, waves) + params
    scratch = [buf(b.shape, b.dtype) for b in brought] + [dma((len(brought),))]
    scratch += [buf((16, 128), jnp.int32), buf((16, 128), LIST), buf((27, 16, 128), LIST)] + [buf(*t) for t in TABLES + RANKS]
    scratch += [buf((27, SLOT, 128), BF16), buf((27, SLOT, 128), BF16), buf((27, SLOT, 128), F32)]
    scratch += [buf((27, 16, 128), BF16), buf((27, 48, 128), BF16), buf((27, 16, 128), BF16)]
    return pl.pallas_call(
        functools.partial(whole_kernel, sizes, norm),
        out_shape=[shape(*r) for r in RESULT],
        in_specs=[HBM, HBM, SMEM] + [HBM] * 10,
        out_specs=[VMEM] * 2,
        scratch_shapes=scratch + bufs + [dma((15,)), dma((27,)), dma((27,))] + sems,
        compiler_params=pltpu.CompilerParams(collective_id=0, has_side_effects=True),
        name="whole",
    )(neighbors, positions, counts, feats, species, waves, *params)


def per_device(
    sizes, features, positions, species, counts, neighbors, waves, radial_in, radial_out,
    species_gain, mix_weight, readout, charge_weight, ref_energy,
):
    nx, ny, nz = sizes
    slots = positions.shape[-1]
    norm = (waves.shape[1] * nx * ny * nz * slots) ** -0.5
    args = (
        neighbors.reshape(12, 1, slots), positions.reshape(3, 1, slots), counts.reshape(1, 1),
        features.reshape(slots, -1), species.reshape(1, slots), waves, radial_in, radial_out, species_gain,
        mix_weight, readout.reshape(1, -1), charge_weight.T, ref_energy.reshape(1, -1),
    )
    site, forces = direct(sizes, norm, *args)
    crowded = jnp.isnan(site[0, 0])
    site, forces = lax.cond(
        crowded, lambda s, f, *a: tuple(general(sizes, norm, *a)), lambda s, f, *a: (s, f), site, forces, *args
    )
    return site.reshape(1, 1, 1, slots), forces.reshape(1, 1, 1, 3, slots)


def solution(mesh):
    sizes = tuple(mesh.shape[n] for n in AXES)
    cell = P("gx", "gy", "gz")
    placed = (cell,) * 5 + (P(),) * 8
    return jax.shard_map(
        functools.partial(per_device, sizes),
        mesh=mesh,
        in_specs=placed,
        out_specs=(cell, cell),
        check_vma=False,
    )
```

```python
import functools
import math

import jax
import jax.numpy as jnp
from jax import lax
from jax.experimental import pallas as pl
from jax.experimental.pallas import tpu as pltpu
from jax.sharding import PartitionSpec as P

TICKS = 1024
AXES = ("gx", "gy", "gz")
MESH = pl.DeviceIdType.MESH
HIGH = lax.Precision.HIGHEST
OFFS = [(a - 1, b - 1, c - 1) for a in range(3) for b in range(3) for c in range(3)]
F32 = jnp.float32
BF16 = jnp.bfloat16
SLOT = 96
GROUP = 9
LOG2E = math.log2(math.e)
FAR = -1.0e6
ALL_VMEM = 67_043_328
LIST = jnp.int16


def iota(shape, dim):
    return lax.broadcasted_iota(jnp.int32, shape, dim)


def dot(a, b, contract=((1,), (0,)), precision=None):
    return lax.dot_general(a, b, (contract, ((), ())), precision=precision, preferred_element_type=F32)


NT = ((1,), (1,))
TN = ((0,), (0,))


def split(x):
    hi = x.astype(BF16)
    return hi, (x - hi.astype(F32)).astype(BF16)


COORDS = {}


def along(axis, size, o):
    if (axis, o % size) not in COORDS:
        here = lax.axis_index(axis)
        COORDS[axis, o % size] = lax.rem(here + o % size, size) if o % size else here
    return COORDS[axis, o % size]


def at_offset(sizes, d):
    return tuple(along(n, s, o) for n, s, o in zip(AXES, sizes, d))


def in_plane(sizes, d):
    dx, flip, dz = d
    x, y, z = at_offset(sizes, (dx, 0, dz))
    if flip and "flip" not in COORDS:
        COORDS["flip"] = y + 1 - 2 * lax.rem(y, 2)
    return x, COORDS["flip"] if flip else y, z


def greet(devices):
    barrier = pltpu.get_barrier_semaphore()
    for device in devices:
        pl.semaphore_signal(barrier, inc=1, device_id=device, device_id_type=MESH)
    return lambda: pl.semaphore_wait(barrier, len(devices))


def send(src, dst, ssem, rsem, device):
    c = pltpu.make_async_remote_copy(
        src_ref=src, dst_ref=dst, send_sem=ssem, recv_sem=rsem, device_id=device, device_id_type=MESH
    )
    c.start()
    return c


LEVEL = [i for i, d in enumerate(OFFS) if d[0] == 0]
APART = [i for i, d in enumerate(OFFS) if d[0] != 0]
NEAR = [(i, OFFS[i]) for i in LEVEL + APART if i != 13]
NEAR.sort(key=lambda n: (n[0] in APART, -abs(n[1][1]) - abs(n[1][2])))


SIDE = 128


def rows_of(pos):
    loc = pos & (TICKS - 1)
    scale = 1.0 / TICKS
    return (loc & ~31).astype(F32) * scale, (loc & 31).astype(F32) * scale


def wide(x):
    return x.astype(jnp.int32)


def stack(parts):
    return parts[0] if len(parts) == 1 else jnp.concatenate(parts, axis=0)


def find(blks, ranks, base):
    slot = iota((SLOT, 128), 0).astype(F32) + base
    accs = []
    for blk, rank in zip(blks, ranks):
        code = ((blk & 127) + 1).astype(F32)
        acc = jnp.zeros((SLOT, 128), F32)
        for k in range(12):
            acc = jnp.where(rank[k : k + 1] == slot, code[k : k + 1], acc)
        accs.append(acc)
    picks_i = [jnp.where(acc > 0.0, 1.0, 0.0).astype(BF16) for acc in accs]
    named = dot(stack(accs).astype(BF16), jnp.ones((128, 128), BF16))
    lane = iota(named.shape, 1)
    return picks_i, jnp.where(named == (lane + 1).astype(F32), 1.0, 0.0).astype(BF16)


def distance(blks, offs, own, picks_i, pick_j):
    jhi, jlo = rows_of(own)
    pieces = []
    for n, (blk, off, pick_i) in enumerate(zip(blks, offs, picks_i)):
        ihi, ilo = rows_of(blk[12:15])
        shift = jnp.concatenate([jnp.full((1, 128), o, F32) for o in off], axis=0)
        fill = jnp.zeros((2, 128), F32)
        left = jnp.concatenate([-ihi - shift, -ilo, fill], axis=0)
        right = jnp.concatenate([jhi, jlo, fill], axis=0)
        w = jnp.concatenate([left, right], axis=1).astype(BF16)
        both = jnp.concatenate([pick_i, pick_j[SLOT * n : SLOT * (n + 1)]], axis=1)
        pieces.append(dot(both, w, NT).astype(BF16))
    to_lanes = iota((8, 384), 1) >> 7
    spread = jnp.where((to_lanes == iota((8, 384), 0)) | (to_lanes + 3 == iota((8, 384), 0)), 1.0, 0.0).astype(BF16)
    return dot(stack(pieces), spread)


def basis(disp):
    dx, dy, dz = disp[:, 0:128], disp[:, 128:256], disp[:, 256:384]
    r2 = dx * dx + dy * dy + dz * dz
    s2 = r2 + 0.25
    inv = lax.rsqrt(s2)
    rs = s2 * inv
    inv1 = 1.0 / (1.0 + r2)
    t = rs - (0.25 + 0.5 * lax.rem(iota((1, 128), 1), 8).astype(F32))
    b = jnp.exp2((t * (-2.0 * LOG2E)) * t) * inv1
    return (dx * inv, dy * inv, dz * inv), inv, rs, inv1, t, b


def sigmoid(z):
    return 0.5 * jnp.tanh(0.5 * z) + 0.5


def gains(pick_j, gtab):
    g = dot(pick_j, gtab)
    return g[:, 0:128] + g[:, 128:256]


def forward(disp, pick_j, feats, gtab, mst, wz, wr):
    (ux, uy, uz), _, _, _, _, b = basis(disp)
    z = dot(b.astype(BF16), wz[:, 0:128])
    rad = dot((z * sigmoid(z)).astype(BF16), wr[:, 0:128]) * gains(pick_j, gtab)
    h = dot(pick_j, feats)
    x = h[:, 0:128] + ux * h[:, 128:256] + uy * h[:, 256:384] + uz * h[:, 384:512]
    return dot((rad * x).astype(BF16), mst[0:128, 0:128])


def slopes(disp, pick_j, feats, gtab, mst, wz, wr):
    lane = iota((disp.shape[0], 128), 1)
    (ux, uy, uz), inv, rs, inv1, t, b = basis(disp)
    b = jnp.where(lane < 8, b, b * (-4.0 * t - 2.0 * rs * inv1)).astype(BF16)
    zz = dot(b, wz)
    z, zp = zz[:, 0:128], zz[:, 128:256]
    sig = sigmoid(z)
    silu = z * sig
    hid = jnp.where(lane < 64, silu, (sig + silu * (1.0 - sig)) * zp).astype(BF16)
    rr = dot(hid, wr)
    g = gains(pick_j, gtab)
    rad = rr[:, 0:128] * g
    radp = rr[:, 128:256] * g
    h = dot(pick_j, feats)
    q = []
    for r in (rad, radp):
        for d in range(2):
            x = [(r * h[:, 128 * e : 128 * (e + 1)]).astype(BF16) for e in (2 * d, 2 * d + 1)]
            t = dot(jnp.concatenate(x, axis=1), mst)
            q += [t[:, 0:128], t[:, 128:256]]
    along = ux * q[1] + uy * q[2] + uz * q[3]
    w = q[4] + ux * q[5] + uy * q[6] + uz * q[7] - along * inv
    part = (lane >> 4) & 3
    ua = jnp.where(part == 0, ux, jnp.where(part == 1, uy, uz))
    qa = jnp.where(part == 0, q[1], jnp.where(part == 1, q[2], q[3]))
    return jnp.where(part == 3, q[0] + along, ua * w + qa * inv)


def edges(blk, rank, base, off, own, *tabs):
    picks_i, pick_j = find([blk], [rank], base)
    return picks_i[0], pick_j, slopes(distance([blk], [off], own, picks_i, pick_j), pick_j, *tabs)


def per_atom(pick_i, out):
    lane = iota((SLOT, 128), 1)
    hi = out.astype(BF16)
    mixed = jnp.where(lane < 64, hi.astype(F32), out - hi.astype(F32)).astype(BF16)
    s = dot(mixed, pick_i, TN)
    return s[0:64] + s[64:128]


def cell_offset(a):
    if isinstance(a, int):
        return tuple(float(o) for o in OFFS[a])
    return ((a // 9 - 1).astype(F32), (lax.rem(a // 3, 3) - 1).astype(F32), (lax.rem(a, 3) - 1).astype(F32))


def tables(feats, species, rin, rout, gain, mix, readout, cw, ref_energy, gtab, mst, wz, wr, base9, refrow):
    neigh = 12
    lane = iota((8, SIDE), 1)
    sel8 = jnp.where(lax.rem(lane, 16) == iota((8, SIDE), 0), 1.0, 0.0)
    sel1 = jnp.where(lax.rem(iota((1, SIDE), 1), 16) == 8, 1.0, 0.0)
    rc = dot(cw[...], sel8, TN, HIGH) + dot(readout[...], sel1, TN, HIGH)
    mb = (dot(mix[...].astype(F32), rc, precision=HIGH) * (neigh ** -0.5)).astype(BF16)
    mst[0:128, 0:128] = mb
    mst[0:128, 128:256] = jnp.zeros_like(mb)
    mst[128:256, 0:128] = jnp.zeros_like(mb)
    mst[128:256, 128:256] = mb
    base9[...] = dot(rc, feats[:, 0:128].astype(F32), ((0,), (1,)), HIGH)[0:16]
    kinds = gain.shape[0]
    onehot = jnp.where(iota((kinds, SIDE), 0) == species[...], 1.0, 0.0)
    ghi, glo = split(dot(onehot, gain[...], TN, HIGH))
    gtab[:, 0:128] = ghi
    gtab[:, 128:256] = glo
    refrow[...] = jnp.broadcast_to(dot(ref_energy[...], onehot, precision=HIGH), refrow.shape)
    r = rin[...]
    h = rin.shape[1]
    dup = jnp.where(lax.rem(iota((h, 128), 1), h) == iota((h, 128), 0), 1.0, 0.0).astype(BF16)
    upper = jnp.where(iota((h, 128), 1) - h == iota((h, 128), 0), 1.0, 0.0).astype(BF16)
    rows_a = jnp.where(iota((128, 8), 0) == iota((128, 8), 1), 1.0, 0.0).astype(BF16)
    rows_b = jnp.where(iota((128, 8), 0) - 8 == iota((128, 8), 1), 1.0, 0.0).astype(BF16)
    wz[:, 0:128] = dot(dot(rows_a, r).astype(BF16), dup).astype(BF16)
    wz[:, 128:256] = dot(dot(rows_b, r).astype(BF16), upper).astype(BF16)
    ro = rout[...]
    none = jnp.zeros_like(ro)
    wr[0:64, 0:128] = ro
    wr[64:128, 0:128] = none
    wr[0:64, 128:256] = none
    wr[64:128, 128:256] = ro


def rank_edges(lists, ranks, mask, cells):
    lane = iota((16, 128), 1)
    row = iota((16, 128), 0)
    many = len(cells)
    for n, a in enumerate(cells):
        blk = wide(lists[a])
        keep = ((blk >> 7) == 26 - a) & (lane < blk[15:16]) & (row < 12)
        mask[16 * n : 16 * n + 16] = jnp.where(keep, 1.0, 0.0)
    m = mask[0 : 16 * many].astype(BF16)
    tri = jnp.where(iota((128, 128), 0) <= iota((128, 128), 1), 1.0, 0.0).astype(BF16)
    both = dot(m, jnp.concatenate([tri, jnp.ones((128, 128), BF16)], axis=1))
    lower = jnp.where(iota((16, 16), 0) > iota((16, 16), 1), 1.0, 0.0).astype(BF16)
    totals = jnp.concatenate([both[16 * n : 16 * n + 16, 128:256] for n in range(many)], axis=1).astype(BF16)
    start = dot(lower, totals)
    peak = start[12:13, 0:128]
    for n, a in enumerate(cells):
        s = start[:, 128 * n : 128 * n + 128]
        peak = jnp.maximum(peak, s[12:13])
        r = both[16 * n : 16 * n + 16, 0:128] + s - 1.0
        ranks[a] = jnp.where(mask[16 * n : 16 * n + 16] > 0.0, r, FAR)
    return peak


def wave_tables(sizes, norm, waves, pos, wrow):
    waves_f = waves[...].astype(F32)
    kvec = [waves_f[d : d + 1] * (2.0 * math.pi / sizes[d]) for d in range(3)]
    ksq = kvec[0] * kvec[0] + kvec[1] * kvec[1] + kvec[2] * kvec[2]
    wrow[0:1] = 2.0 * (8.0 * jnp.exp(ksq * (-1.0 / 64.0)) / (8.0 + ksq) * norm)
    fields = []
    for d in range(3):
        wrow[1 + d : 2 + d] = kvec[d]
        length = float(sizes[d] * TICKS)
        p = pos[d : d + 1]
        fields.append(((p >> 7).astype(F32), waves_f[d : d + 1] * (128.0 / length)))
        fields.append(((p & 127).astype(F32), waves_f[d : d + 1] * (1.0 / length)))
    zero_i = jnp.zeros((2, 128), F32)
    zero_k = jnp.zeros((2, waves_f.shape[1]), F32)
    wrow[8:16] = jnp.concatenate([f[1] for f in fields] + [zero_k], axis=0)
    return jnp.concatenate([f[0] for f in fields] + [zero_i], axis=0).astype(BF16)


def phases(pos8, wrow, cos_h, cos_l, sin_h, sin_l):
    def phase(bi, carry):
        at = pl.ds(pl.multiple_of(bi * 128, 128), 128)
        turn = dot(pos8, wrow[8:16, at].astype(BF16), TN)
        quarter = jnp.floor(turn * 4.0 + 0.5)
        x = (turn - quarter * 0.25) * (2.0 * math.pi)
        qi = quarter.astype(jnp.int32)
        xx = x * x
        s = x * (1.0 + xx * (-1.0 / 6 + xx * (1.0 / 120 + xx * (-1.0 / 5040 + xx * (1.0 / 362880)))))
        c = 1.0 + xx * (-0.5 + xx * (1.0 / 24 + xx * (-1.0 / 720 + xx * (1.0 / 40320))))
        odd = (qi & 1) == 1
        cv = jnp.where(odd, s, c)
        sv = jnp.where(odd, c, s)
        cv = jnp.where(((qi + 1) & 2) == 2, -cv, cv)
        sv = jnp.where((qi & 2) == 2, -sv, sv)
        hi, lo = split(cv)
        cos_h[:, at] = hi
        cos_l[:, at] = lo
        hi, lo = split(sv)
        sin_h[:, at] = hi
        sin_l[:, at] = lo
        return carry

    lax.fori_loop(0, wrow.shape[1] // 128, phase, 0)


def peers(sizes):
    nx, ny, nz = sizes
    plane = [(dx, flip, dz) for dx in range(nx) for flip in range(2) for dz in range(nz)][1:]
    plane.sort(key=lambda d: -min(d[0], nx - d[0]) - d[1] - min(d[2], nz - d[2]))
    line = sorted([(0, dy, 0) for dy in range(2, ny, 2)], key=lambda d: -min(d[1], ny - d[1]))
    near = [d for _, d in NEAR]
    known = [((d[0] + nx) % nx, abs(d[1]), (d[2] + nz) % nz) for d in near]
    whom = [at_offset(sizes, d) for d in line] + [in_plane(sizes, d) for d in plane if d not in known]
    whom += [at_offset(sizes, d) for d in near[::-1]]
    return plane, line, whom


def reciprocal(sizes, poison, first, sums_t, sums_j, base9, pack, refrow, pots, wrow, trig, bufs, sems, meanwhile=lambda n: None):
    nx, ny, nz = sizes
    plane, line, _ = peers(sizes)
    cos_h, cos_l, sin_h, sin_l = trig
    got_t, got_j, part, got_rs, block, got_ar, got_ag, lhs, pot_s = bufs
    _, _, sj, rj, srs, rrs, sar, rar, sag, rag, sp, rp = sems
    blocks = wrow.shape[1] // 128
    live = jnp.where(iota((1, 128), 1) < pack[15:16], 1.0, 0.0)
    total = base9[...] + sums_t[13].astype(F32)
    meanwhile(0)
    for c in first:
        c.wait()
    for i, _ in NEAR:
        total = total + got_t[i].astype(F32)
    q = total[0:8] * live
    qhi, qlo = split(q)
    q16 = jnp.concatenate([qhi, qlo], axis=0)
    for half, high, low in ((0, cos_h, cos_l), (1, sin_h, sin_l)):
        s = dot(q16, high[...])
        s = s[0:8] + s[8:16] + dot(q16, low[...])[0:8]
        for bi in range(blocks):
            part[2 * bi + half] = s[:, 128 * bi : 128 * bi + 128] + poison
    ix, iy, iz = [lax.axis_index(n) for n in AXES]
    low_x = lax.rem(iy, 2)
    me = (ix * 2 + low_x) * nz + iz
    rs = []
    for n, d in enumerate(plane):
        to = (lax.rem(ix + d[0], nx) * 2 + (1 - low_x if d[1] else low_x)) * nz + lax.rem(iz + d[2], nz)
        rs.append(send(part.at[to], got_rs.at[n], srs.at[n], rrs.at[n], in_plane(sizes, d)))
    meanwhile(1)
    acc = part[me]
    for n, c in enumerate(rs):
        c.wait()
        acc = acc + got_rs[n]
    block[0] = acc
    ar = [send(block.at[0], got_ar.at[n], sar.at[n], rar.at[n], at_offset(sizes, d)) for n, d in enumerate(line)]
    meanwhile(2)
    for n, c in enumerate(ar):
        c.wait()
        acc = acc + got_ar[n]
    got_ag[me] = acc
    ag = [send(got_ag.at[me], got_ag.at[me], sag.at[n], rag.at[n], in_plane(sizes, d)) for n, d in enumerate(plane)]
    second = [send(sums_j.at[i], got_j.at[26 - i], sj.at[i], rj.at[i], at_offset(sizes, d)) for i, d in NEAR]
    for c in ag:
        c.wait()
    for bi in range(blocks):
        at = slice(128 * bi, 128 * bi + 128)
        weight = wrow[0:1, at]
        pre = got_ag[2 * bi] * weight
        pim = got_ag[2 * bi + 1] * weight
        kx, ky, kz = wrow[1:2, at], wrow[2:3, at], wrow[3:4, at]
        lc = jnp.concatenate([pre, kx * pim, ky * pim, kz * pim], axis=0)
        ls = jnp.concatenate([pim, -kx * pre, -ky * pre, -kz * pre], axis=0)
        hi, lo = split(lc)
        lhs[0:32, at] = hi
        lhs[32:64, at] = lo
        hi, lo = split(ls)
        lhs[64:96, at] = hi
        lhs[96:128, at] = lo
    w = dot(lhs[0:64], cos_h[...], NT)
    v = dot(lhs[64:128], sin_h[...], NT)
    w = w[0:32] + w[32:64] + dot(lhs[0:32], cos_l[...], NT)
    w = w + v[0:32] + v[32:64] + dot(lhs[64:96], sin_l[...], NT)
    pot = w[0:8]
    flag = jnp.where(iota((8, 128), 0) == 0, live, 0.0)
    pot16 = jnp.concatenate([pot * live, flag], axis=0)
    pot_s[0] = pot16.astype(BF16)
    third = [send(pot_s.at[0], pots.at[26 - i], sp.at[i], rp.at[i], at_offset(sizes, d)) for i, d in NEAR]
    pots[13] = pot16.astype(BF16)
    js = sums_j[13].astype(F32)
    for c in second:
        c.wait()
    for i, _ in NEAR:
        js = js + got_j[i].astype(F32)
    rows = []
    for d in range(3):
        wave = jnp.sum(q * w[8 * d + 8 : 8 * d + 16], axis=0, keepdims=True)
        rows.append(wave - jnp.sum(pot16 * js[16 * d : 16 * d + 16], axis=0, keepdims=True))
    site = live * (total[8:9] + refrow[0:1] + 0.5 * jnp.sum(q * pot, axis=0, keepdims=True))
    mine = jnp.concatenate(rows + [site, live, live, live, live], axis=0)
    return mine, third


def hand_sums(sizes, sums_t, got_t, ssem, rsem, cells):
    return [
        send(sums_t.at[i], got_t.at[26 - i], ssem.at[i], rsem.at[i], at_offset(sizes, d)) for i, d in NEAR if i in cells
    ]


def pull_back(work, pots):
    prods = []
    for (pick_i, _, out), p in zip(work, pots):
        none = jnp.zeros((16, 128), BF16)
        prods.append(out * dot(pick_i, jnp.concatenate([p, p, p, none, p, p, p, none], axis=0), NT))
    prod = stack(prods)
    hi = prod.astype(BF16)
    mixed = jnp.where(iota(prod.shape, 1) < 64, hi.astype(F32), prod - hi.astype(F32)).astype(BF16)
    return dot(mixed, stack([pick_j for _, pick_j, _ in work]), TN)


def give(mine, t, site, forces):
    t = t[0:64] + t[64:128]
    for d in range(3):
        g = mine[d : d + 1] + jnp.sum(t[16 * d : 16 * d + 16], axis=0, keepdims=True)
        forces[d] = -g * mine[4:5]
    site[...] = mine[3:4]


def gather_pack(neighbors, positions, counts, pack, sem):
    copies = [pltpu.make_async_copy(neighbors.at[k], pack.at[pl.ds(k, 1)], sem.at[k]) for k in range(12)]
    copies += [pltpu.make_async_copy(positions.at[d], pack.at[pl.ds(12 + d, 1)], sem.at[12 + d]) for d in range(3)]
    for c in copies:
        c.start()
    pack[15:16] = jnp.full((1, 128), counts[0, 0], jnp.int32)
    return copies


def hand_out(sizes, pack, lists, ssem, rsem):
    copies = [send(pack, lists.at[26 - i], ssem.at[i], rsem.at[i], at_offset(sizes, d)) for i, d in NEAR]
    lists[13] = pack[...]
    return copies


def shorten(pack, short):
    row = iota((16, 128), 0)
    local = (row >= 12) & (row < 15)
    short[...] = jnp.where(local, pack[...] & (TICKS - 1), pack[...]).astype(LIST)


def whole_kernel(
    sizes, norm, neighbors, positions, counts, *rest,
):
    far, (site, forces), near = rest[:10], rest[10:12], rest[12:22]
    whole_steps(sizes, norm, neighbors, positions, counts, far, near, site, forces, *rest[22:])


def whole_steps(
    sizes, norm, neighbors, positions, counts, far, near, site, forces,
    osem, pack, short, lists, gtab, mst, wz, wr, base9, refrow, ranks, mask, picks_i, picks_j, outs, sums_t, sums_j, pots, wrow,
    cos_h, cos_l, sin_h, sin_l, got_t, got_j, part, got_rs, block, got_ar, got_ag, lhs, pot_s,
    psem, ls, lr, *sems,
):
    COORDS.clear()
    wait = greet(peers(sizes)[2])
    packed = gather_pack(neighbors, positions, counts, pack, psem)
    brought = [pltpu.make_async_copy(f, n, osem.at[i]) for i, (f, n) in enumerate(zip(far, near))]
    for c in brought:
        c.start()
    for c in brought:
        c.wait()
    feats, species, waves, rin, rout, gain, mix, readout, cw, ref_energy = near
    tables(feats, species, rin, rout, gain, mix, readout, cw, ref_energy, gtab, mst, wz, wr, base9, refrow)
    for c in packed:
        c.wait()
    shorten(pack, short)
    wait()
    out = hand_out(sizes, short, lists, ls, lr)
    own = pack[12:15]
    trig = (cos_h, cos_l, sin_h, sin_l)
    phases(wave_tables(sizes, norm, waves, own, wrow), wrow, *trig)
    tabs = (feats, gtab, mst, wz, wr)

    def first(cells):
        blks = [wide(lists[a]) for a in cells]
        found, pick_j = find(blks, [ranks[a] for a in cells], 0.0)
        disp = distance(blks, [cell_offset(a) for a in cells], own, found, pick_j)
        out = forward(disp, pick_j, *[t[...] for t in tabs])
        for n, a in enumerate(cells):
            rows = slice(SLOT * n, SLOT * n + SLOT)
            picks_i[a] = found[n]
            picks_j[a] = pick_j[rows]
            sums_t[a] = per_atom(found[n], out[rows])[0:16].astype(BF16)

    def later(gi):
        cells = [gi * GROUP + u for u in range(GROUP)]
        found = [picks_i[a] for a in cells]
        pick_j = stack([picks_j[a] for a in cells])
        disp = distance([wide(lists[a]) for a in cells], [cell_offset(a) for a in cells], own, found, pick_j)
        out = slopes(disp, pick_j, *[t[...] for t in tabs])
        for n, a in enumerate(cells):
            rows = slice(SLOT * n, SLOT * n + SLOT)
            outs[a] = out[rows]
            sums_j[a] = per_atom(found[n], out[rows])[0:48].astype(BF16)

    peak = jnp.zeros((1, 128), F32)
    sums = []
    for cells in (LEVEL, APART):
        here = [n for n, (i, _) in enumerate(NEAR) if i in cells]
        for n in here:
            out[n].wait()
        peak = jnp.maximum(peak, rank_edges(lists, ranks, mask, cells))
        first(cells)
        sums += hand_sums(sizes, sums_t, got_t, sems[0], sems[1], cells)
    poison = jnp.where(peak > float(SLOT), jnp.nan, 0.0)
    bufs = (got_t, got_j, part, got_rs, block, got_ar, got_ag, lhs, pot_s)
    mine, third = reciprocal(sizes, poison, sums, sums_t, sums_j, base9, pack, refrow, pots, wrow, trig, bufs, sems, later)
    total = jnp.zeros((128, 128), F32)
    for cells in (LEVEL, APART):
        for n, (i, _) in enumerate(NEAR):
            if i in cells:
                third[n].wait()
        total = total + pull_back([(picks_i[a], picks_j[a], outs[a]) for a in cells], [pots[a] for a in cells])
    give(mine, total, site, forces)


def spread_kernel(
    sizes, neighbors, positions, counts, feats, species, rin, rout, gain, mix, readout, cw, ref_energy,
    lists, pack_out, gtab, mst, wz, wr, base9, refrow, pack, short, psem, ssem, rsem,
):
    COORDS.clear()
    wait = greet([at_offset(sizes, d) for _, d in NEAR])
    packed = gather_pack(neighbors, positions, counts, pack, psem)
    tables(feats, species, rin, rout, gain, mix, readout, cw, ref_energy, gtab, mst, wz, wr, base9, refrow)
    for c in packed:
        c.wait()
    shorten(pack, short)
    wait()
    out = hand_out(sizes, short, lists, ssem, rsem)
    pack_out[...] = pack[...]
    for c in out:
        c.wait()


def each_piece(ranks, run):
    def cell(a, carry):
        pieces = (jnp.max(ranks[a]).astype(jnp.int32) + SLOT) // SLOT
        return lax.fori_loop(0, pieces, lambda c, carry: run(a, (c * SLOT).astype(F32), carry), carry)

    lax.fori_loop(0, 27, cell, 0)


def edge_kernel(lists, pack, feats, gtab, mst, wz, wr, sums_t, sums_j, mask, ranks, total_t, total_j):
    rank_edges(lists, ranks, mask, range(27))
    own = pack[12:15]
    total_t[...] = jnp.zeros_like(total_t)
    total_j[...] = jnp.zeros_like(total_j)

    def piece(a, base, carry):
        pick_i, _, out = edges(wide(lists[a]), ranks[a], base, cell_offset(a), own, feats[...], gtab[...], mst[...], wz[...], wr[...])
        s = per_atom(pick_i, out)
        total_j[a] += s[0:48]
        total_t[a] += s[48:64]
        return carry

    each_piece(ranks, piece)
    sums_t[...] = total_t[...].astype(BF16)
    sums_j[...] = total_j[...].astype(BF16)


def wave_kernel(
    sizes, norm, sums_t, sums_j, base9, pack, waves, refrow, pots, mine,
    wrow, cos_h, cos_l, sin_h, sin_l, got_t, got_j, part, got_rs, block, got_ar, got_ag, lhs, pot_s, *sems,
):
    COORDS.clear()
    wait = greet(peers(sizes)[2])
    trig = (cos_h, cos_l, sin_h, sin_l)
    phases(wave_tables(sizes, norm, waves, pack[12:15], wrow), wrow, *trig)
    wait()
    bufs = (got_t, got_j, part, got_rs, block, got_ar, got_ag, lhs, pot_s)
    sums = hand_sums(sizes, sums_t, got_t, sems[0], sems[1], LEVEL + APART)
    mine[...], third = reciprocal(sizes, 0.0, sums, sums_t, sums_j, base9, pack, refrow, pots, wrow, trig, bufs, sems)
    for c in third:
        c.wait()


def force_kernel(pots, mine, lists, pack, feats, gtab, mst, wz, wr, site, forces, mask, ranks, total):
    rank_edges(lists, ranks, mask, range(27))
    own = pack[12:15]
    total[...] = jnp.zeros_like(total)

    def piece(a, base, carry):
        work = edges(wide(lists[a]), ranks[a], base, cell_offset(a), own, feats[...], gtab[...], mst[...], wz[...], wr[...])
        total[...] += pull_back([work], [pots[a]])
        return carry

    each_piece(ranks, piece)
    give(mine[...], total[...], site, forces)


VMEM = pl.BlockSpec(memory_space=pltpu.VMEM)
SMEM = pl.BlockSpec(memory_space=pltpu.SMEM)
HBM = pl.BlockSpec(memory_space=pltpu.HBM)


def shape(dims, kind):
    return jax.ShapeDtypeStruct(dims, kind)


def wave_buffers(sizes, waves):
    nx, ny, nz = sizes
    planes, lines = 2 * nx * nz, ny // 2
    assert planes == 2 * waves // 128
    buf = pltpu.VMEM
    dma = pltpu.SemaphoreType.DMA
    trig = [buf((128, waves), BF16)] * 4
    rest = [
        buf((27, 16, 128), BF16), buf((27, 48, 128), BF16), buf((planes, 8, 128), F32), buf((planes - 1, 8, 128), F32),
        buf((1, 8, 128), F32), buf((lines - 1, 8, 128), F32), buf((planes, 8, 128), F32), buf((128, waves), BF16),
        buf((1, 16, 128), BF16),
    ]
    counts = (27, 27, 27, 27, planes - 1, planes - 1, lines - 1, lines - 1, planes - 1, planes - 1, 27, 27)
    return [buf((16, waves), F32)] + trig + rest, [dma((n,)) for n in counts]


TABLES = [
    ((128, 256), BF16), ((256, 256), BF16), ((128, 256), BF16), ((128, 256), BF16), ((16, 128), F32), ((8, 128), F32),
]
RANKS = [((27, 16, 128), F32), ((27 * 16, 128), F32)]
RESULT = [((1, 128), F32), ((3, 1, 128), F32)]


def general(sizes, norm, neighbors, positions, counts, feats, species, waves, *params):
    dma = pltpu.SemaphoreType.DMA
    lists, pack, gtab, mst, wz, wr, base9, refrow = pl.pallas_call(
        functools.partial(spread_kernel, sizes),
        out_shape=[shape((27, 16, 128), LIST), shape((16, 128), jnp.int32)] + [shape(*t) for t in TABLES],
        in_specs=[HBM, HBM, SMEM] + [VMEM] * 9,
        out_specs=[VMEM] * 8,
        scratch_shapes=[pltpu.VMEM((16, 128), jnp.int32), pltpu.VMEM((16, 128), LIST), dma((15,)), dma((27,)), dma((27,))],
        compiler_params=pltpu.CompilerParams(collective_id=1, has_side_effects=True, vmem_limit_bytes=ALL_VMEM),
        name="spread",
    )(neighbors, positions, counts, feats, species, *params)
    ranking = [pltpu.VMEM(*RANKS[1]), pltpu.VMEM(*RANKS[0])]
    sums_t, sums_j = pl.pallas_call(
        edge_kernel,
        out_shape=[shape((27, 16, 128), BF16), shape((27, 48, 128), BF16)],
        in_specs=[VMEM] * 7,
        out_specs=[VMEM] * 2,
        scratch_shapes=ranking + [pltpu.VMEM((27, 16, 128), F32), pltpu.VMEM((27, 48, 128), F32)],
        compiler_params=pltpu.CompilerParams(vmem_limit_bytes=ALL_VMEM),
        name="edges",
    )(lists, pack, feats, gtab, mst, wz, wr)
    bufs, sems = wave_buffers(sizes, waves.shape[1])
    pots, mine = pl.pallas_call(
        functools.partial(wave_kernel, sizes, norm),
        out_shape=[shape((27, 16, 128), BF16), shape((8, 128), F32)],
        in_specs=[VMEM] * 6,
        out_specs=[VMEM] * 2,
        scratch_shapes=bufs + sems,
        compiler_params=pltpu.CompilerParams(collective_id=2, has_side_effects=True, vmem_limit_bytes=ALL_VMEM),
        name="waves",
    )(sums_t, sums_j, base9, pack, waves, refrow)
    return pl.pallas_call(
        force_kernel,
        out_shape=[shape(*r) for r in RESULT],
        in_specs=[VMEM] * 9,
        out_specs=[VMEM] * 2,
        scratch_shapes=ranking + [pltpu.VMEM((128, 128), F32)],
        name="forces",
    )(pots, mine, lists, pack, feats, gtab, mst, wz, wr)


def direct(sizes, norm, neighbors, positions, counts, feats, species, waves, *params):
    dma = pltpu.SemaphoreType.DMA
    buf = pltpu.VMEM
    bufs, sems = wave_buffers(sizes, waves.shape[1])
    brought = (feats, species, waves) + params
    scratch = [buf(b.shape, b.dtype) for b in brought] + [dma((len(brought),))]
    scratch += [buf((16, 128), jnp.int32), buf((16, 128), LIST), buf((27, 16, 128), LIST)] + [buf(*t) for t in TABLES + RANKS]
    scratch += [buf((27, SLOT, 128), BF16), buf((27, SLOT, 128), BF16), buf((27, SLOT, 128), F32)]
    scratch += [buf((27, 16, 128), BF16), buf((27, 48, 128), BF16), buf((27, 16, 128), BF16)]
    return pl.pallas_call(
        functools.partial(whole_kernel, sizes, norm),
        out_shape=[shape(*r) for r in RESULT],
        in_specs=[HBM, HBM, SMEM] + [HBM] * 10,
        out_specs=[VMEM] * 2,
        scratch_shapes=scratch + bufs + [dma((15,)), dma((27,)), dma((27,))] + sems,
        compiler_params=pltpu.CompilerParams(collective_id=0, has_side_effects=True),
        name="whole",
    )(neighbors, positions, counts, feats, species, waves, *params)


def per_device(
    sizes, features, positions, species, counts, neighbors, waves, radial_in, radial_out,
    species_gain, mix_weight, readout, charge_weight, ref_energy,
):
    nx, ny, nz = sizes
    slots = positions.shape[-1]
    norm = (waves.shape[1] * nx * ny * nz * slots) ** -0.5
    args = (
        neighbors.reshape(12, 1, slots), positions.reshape(3, 1, slots), counts.reshape(1, 1),
        features.reshape(slots, -1), species.reshape(1, slots), waves, radial_in, radial_out, species_gain,
        mix_weight, readout.reshape(1, -1), charge_weight.T, ref_energy.reshape(1, -1),
    )
    site, forces = direct(sizes, norm, *args)
    crowded = jnp.isnan(site[0, 0])
    site, forces = lax.cond(
        crowded, lambda s, f, *a: tuple(general(sizes, norm, *a)), lambda s, f, *a: (s, f), site, forces, *args
    )
    return site.reshape(1, 1, 1, slots), forces.reshape(1, 1, 1, 3, slots)


def solution(mesh):
    sizes = tuple(mesh.shape[n] for n in AXES)
    cell = P("gx", "gy", "gz")
    placed = (cell,) * 5 + (P(),) * 8
    return jax.shard_map(
        functools.partial(per_device, sizes),
        mesh=mesh,
        in_specs=placed,
        out_specs=(cell, cell),
        check_vma=False,
    )
```
